32 devices in a mesh: data: 4 (over y, z), model: 8 (over x, core).
Axes of the slice: x: 4, y: 2, z: 2, core: 2. Of those that a mesh axis runs over, the one named last changes fastest.
The devices are a block of a 4x4x8 slice.
Arguments:
- tokens: bfloat16 [32, 512, 1024], P('data'), parts along dimension 0
- seg_ids: int32 [32, 512], P('data'), parts along dimension 0
- d_out: bfloat16 [32, 512, 1024], P('data'), parts along dimension 0
- gain_attn: bfloat16 [1024], replicated
- gain_mlp: bfloat16 [1024], replicated
- w_qkv: bfloat16 [1024, 16, 3, 64], P(None, 'model')
- w_out: bfloat16 [16, 64, 1024], P('model')
- w_up: bfloat16 [1024, 4096], P(None, 'model')
- w_down: bfloat16 [4096, 1024], P('model')
Outputs:
- output 1: bfloat16 [32, 512, 1024], P('data'), parts along dimension 0
- output 2: bfloat16 [32, 512, 1024], P('data'), parts along dimension 0
- output 3: bfloat16 [4096, 16, 3, 64], P('data', 'model'), parts along dimension 0
- output 4: bfloat16 [64, 64, 1024], P(('data', 'model')), parts along dimension 0
- output 5: bfloat16 [4096, 4096], P('data', 'model'), parts along dimension 0
- output 6: bfloat16 [16384, 1024], P(('data', 'model')), parts along dimension 0
- output 7: float32 [4096], P('data'), parts along dimension 0
- output 8: float32 [4096], P('data'), parts along dimension 0
There are 4 independent parts. The reference program is written for one: setup_inputs(seed, part) draws one part's arguments, and reference() takes and returns one part's arrays. A program takes and returns all parts, laid end to end along the dimension named above; an argument that names none is the same for every part.
All inputs are finite; a program needn't handle non-finite values.
Results may differ from the reference program's by a relative error of at most 0.02.
Values are sent between devices in bfloat16 or wider.
A program may use at most 768 MiB of HBM per device.

```python
import functools
import jax
import jax.numpy as jnp
from jax import lax

SEQ_COUNT = 8
SEQ_LEN = 512
HIDDEN = 1024
HEADS = 16
HEAD_DIM = 64
FFN_DIM = 4096
NORM_EPS = 1e-5


def setup_inputs(seed: int = 0, part: int = 0) -> dict:
    part_key = jax.random.fold_in(jax.random.key(seed), part)
    key_list = jax.random.split(part_key, 3)
    shared_keys = jax.random.split(jax.random.key(seed + 1), 6)
    tokens = jax.random.normal(key_list[0], (SEQ_COUNT, SEQ_LEN, HIDDEN), jnp.float32).astype(jnp.bfloat16)
    gap_draw = jax.random.randint(key_list[1], (SEQ_COUNT, SEQ_LEN), 0, max(SEQ_LEN // 2, 1))
    positions = jnp.arange(SEQ_LEN)[None, :]
    starts = jnp.where((gap_draw == 0) & (positions > 0), 1, 0)
    seg_ids = jnp.cumsum(starts, axis=1).astype(jnp.int32)
    d_out = jax.random.normal(key_list[2], (SEQ_COUNT, SEQ_LEN, HIDDEN), jnp.float32).astype(jnp.bfloat16)
    gain_attn = (1.0 + 0.2 * jax.random.normal(shared_keys[0], (HIDDEN,), jnp.float32)).astype(jnp.bfloat16)
    gain_mlp = (1.0 + 0.2 * jax.random.normal(shared_keys[1], (HIDDEN,), jnp.float32)).astype(jnp.bfloat16)
    w_qkv = (jax.random.normal(shared_keys[2], (HIDDEN, HEADS, 3, HEAD_DIM), jnp.float32) * (1.5 * HIDDEN ** -0.5)).astype(jnp.bfloat16)
    w_out = (jax.random.normal(shared_keys[3], (HEADS, HEAD_DIM, HIDDEN), jnp.float32) * (1.5 * (HEADS * HEAD_DIM) ** -0.5)).astype(jnp.bfloat16)
    w_up = (jax.random.normal(shared_keys[4], (HIDDEN, FFN_DIM), jnp.float32) * HIDDEN ** -0.5).astype(jnp.bfloat16)
    w_down = (jax.random.normal(shared_keys[5], (FFN_DIM, HIDDEN), jnp.float32) * (1.5 * FFN_DIM ** -0.5)).astype(jnp.bfloat16)
    return {'tokens': tokens, 'seg_ids': seg_ids, 'd_out': d_out, 'gain_attn': gain_attn, 'gain_mlp': gain_mlp, 'w_qkv': w_qkv, 'w_out': w_out, 'w_up': w_up, 'w_down': w_down}


def layer_norm(values, gain_vec):
    mean_val = jnp.mean(values, axis=-1, keepdims=True)
    centered = values - mean_val
    var_val = jnp.mean(centered * centered, axis=-1, keepdims=True)
    return centered * lax.rsqrt(var_val + NORM_EPS) * gain_vec


def attend_head(head_qkv, allowed):
    scores = jnp.einsum('bqd,bkd->bqk', head_qkv[0], head_qkv[1]) * (HEAD_DIM ** -0.5)
    scores = jnp.where(allowed, scores, -1e30)
    attn_probs = jax.nn.softmax(scores, axis=-1).astype(jnp.bfloat16)
    return jnp.einsum('bqk,bkd->bqd', attn_probs.astype(jnp.float32), head_qkv[2]).astype(jnp.bfloat16)


def layer_forward(tokens, gain_attn, gain_mlp, w_qkv, w_out, w_up, w_down, allowed):
    row_count = SEQ_COUNT * SEQ_LEN
    x_f32 = tokens.astype(jnp.float32).reshape(row_count, HIDDEN)
    normed = layer_norm(x_f32, gain_attn).astype(jnp.bfloat16)
    qkv_all = jnp.dot(normed.astype(jnp.float32), w_qkv.astype(jnp.float32).reshape(HIDDEN, HEADS * 3 * HEAD_DIM), preferred_element_type=jnp.float32).astype(jnp.bfloat16)
    qkv_heads = jnp.transpose(qkv_all.astype(jnp.float32).reshape(SEQ_COUNT, SEQ_LEN, HEADS, 3, HEAD_DIM), (2, 3, 0, 1, 4))
    head_out = lax.map(jax.checkpoint(functools.partial(attend_head, allowed=allowed)), qkv_heads)
    attn_rows = jnp.transpose(head_out, (1, 2, 0, 3)).reshape(row_count, HEADS * HEAD_DIM)
    attn_proj = jnp.dot(attn_rows.astype(jnp.float32), w_out.astype(jnp.float32).reshape(HEADS * HEAD_DIM, HIDDEN), preferred_element_type=jnp.float32).astype(jnp.bfloat16)
    resid_bf = (x_f32 + attn_proj.astype(jnp.float32)).astype(jnp.bfloat16)
    resid_f32 = resid_bf.astype(jnp.float32)
    normed_mlp = layer_norm(resid_f32, gain_mlp).astype(jnp.bfloat16)
    pre_act = jnp.dot(normed_mlp.astype(jnp.float32), w_up.astype(jnp.float32), preferred_element_type=jnp.float32)
    hidden = jax.nn.gelu(pre_act, approximate=True).astype(jnp.bfloat16)
    mlp_down = jnp.dot(hidden.astype(jnp.float32), w_down.astype(jnp.float32), preferred_element_type=jnp.float32).astype(jnp.bfloat16)
    layer_out = (resid_f32 + mlp_down.astype(jnp.float32)).astype(jnp.bfloat16)
    return layer_out.reshape(SEQ_COUNT, SEQ_LEN, HIDDEN)


def reference(tokens, seg_ids, d_out, gain_attn, gain_mlp, w_qkv, w_out, w_up, w_down):
    positions = jnp.arange(SEQ_LEN)
    allowed = (seg_ids[:, :, None] == seg_ids[:, None, :]) & (positions[:, None] >= positions[None, :])[None]
    layer_fn = functools.partial(layer_forward, allowed=allowed)
    layer_out, back_fn = jax.vjp(layer_fn, tokens, gain_attn.astype(jnp.float32), gain_mlp.astype(jnp.float32), w_qkv, w_out, w_up, w_down)
    grad_list = back_fn(d_out)
    return (layer_out, grad_list[0], grad_list[3], grad_list[4], grad_list[5], grad_list[6], grad_list[1], grad_list[2])
```

```python
import functools
import jax
import jax.numpy as jnp
from jax import lax
from jax.experimental import pallas as pl
from jax.experimental.pallas import tpu as pltpu
from jax.sharding import PartitionSpec as P

NORM_EPS = 1e-5
MESH = pl.DeviceIdType.MESH
F32 = jnp.float32
BF16 = jnp.bfloat16
SLOTS = 4
BLOCKS = 16
HALF = BLOCKS // 2
PIECE = 2
COPIES = 13
VMEM_LIMIT = 66 * 1000 * 1000


def mm(a, b):
    return lax.dot_general(a, b, (((1,), (0,)), ((), ())), preferred_element_type=F32)


def mt(a, b):
    return lax.dot_general(a, b, (((1,), (1,)), ((), ())), preferred_element_type=F32)


def tm(a, b):
    return lax.dot_general(a, b, (((0,), (0,)), ((), ())), preferred_element_type=F32)


def loop(count, body):
    def step(i, carry):
        body(i)
        return carry
    lax.fori_loop(0, count, step, 0)


class RingSum:
    def __init__(self, size, part, pair_in, relay_in, ring_in, whole, send, recv):
        me = lax.axis_index('model')
        self.core = lax.rem(me, 2)
        self.chips = size // 2
        self.chip = me // 2
        self.right = lax.rem(me + 2, size)
        self.left = lax.rem(me + size - 2, size)
        self.partner = me + 1 - 2 * self.core
        self.part, self.pair_in, self.relay_in, self.ring_in, self.whole = part, pair_in, relay_in, ring_in, whole
        self.send, self.recv = send, recv

    def base(self, core, step):
        return core * HALF + lax.rem(self.chip + step, self.chips) * PIECE

    def copy(self, n, s):
        slot = lax.rem(s, SLOTS)
        part, whole = self.part.at[slot], self.whole.at[slot]
        base = functools.partial(self.base, self.core)
        last = self.chips - 1
        if n == 0:
            src, dst, to = part.at[pl.ds((1 - self.core) * HALF, HALF)], self.pair_in.at[slot], self.partner
        elif n == 1:
            src, dst, to = part.at[pl.ds(base(2), 1)], self.relay_in.at[slot, pl.ds(0, 1)], self.right
        elif n == 2:
            src, dst, to = part.at[pl.ds(base(2) + 1, 1)], self.relay_in.at[slot, pl.ds(1, 1)], self.left
        elif n == 3:
            src, dst, to = part.at[pl.ds(base(1), PIECE)], self.ring_in.at[slot, 0], self.right
        elif n == 4:
            src, dst, to = part.at[pl.ds(base(last), PIECE)], self.ring_in.at[slot, 1], self.left
        else:
            start, length, to = {
                5: (base(0), PIECE, self.right),
                6: (base(0), PIECE, self.left),
                7: (base(0), PIECE, self.partner),
                8: (base(last), 1, self.right),
                9: (base(1) + 1, 1, self.left),
                10: (base(last), PIECE, self.partner),
                11: (base(1), PIECE, self.partner),
                12: (base(2), PIECE, self.partner),
            }[n]
            src = dst = whole.at[pl.ds(start, length)]
        return pltpu.make_async_remote_copy(
            src_ref=src, dst_ref=dst, send_sem=self.send.at[slot, n], recv_sem=self.recv.at[slot, n],
            device_id={'model': to}, device_id_type=MESH)

    def add(self, slot, block, others):
        total = self.part[slot, block].astype(F32)
        for ref in others:
            total = total + ref.astype(F32)
        return total.astype(BF16)

    def stage(self, j, s):
        slot = lax.rem(s, SLOTS)
        last = self.chips - 1
        if j == 0:
            self.copy(0, s).start()
        elif j == 1:
            self.copy(0, s).wait_recv()

            def pair(i):
                block = self.core * HALF + i
                self.part[slot, block] = self.add(slot, block, [self.pair_in[slot, i]])
            loop(HALF, pair)
            self.copy(1, s).start()
            self.copy(2, s).start()
        elif j == 2:
            self.copy(1, s).wait_recv()
            self.copy(2, s).wait_recv()
            first, second = self.base(self.core, 1), self.base(self.core, last) + 1
            self.part[slot, first] = self.add(slot, first, [self.relay_in[slot, 0]])
            self.part[slot, second] = self.add(slot, second, [self.relay_in[slot, 1]])
            self.copy(3, s).start()
            self.copy(4, s).start()
        elif j == 3:
            self.copy(3, s).wait_recv()
            self.copy(4, s).wait_recv()
            for i in range(PIECE):
                block = self.base(self.core, 0) + i
                self.whole[slot, block] = self.add(slot, block, [self.ring_in[slot, 0, i], self.ring_in[slot, 1, i]])
            for n in (5, 6, 7):
                self.copy(n, s).start()
        elif j == 4:
            self.copy(5, s).wait_recv()
            self.copy(6, s).wait_recv()
            for n in (8, 9, 10, 11):
                self.copy(n, s).start()
        elif j == 5:
            self.copy(8, s).wait_recv()
            self.copy(9, s).wait_recv()
            self.copy(12, s).start()
        else:
            for n in (7, 10, 11, 12):
                self.copy(n, s).wait_recv()
            for n in range(COPIES):
                self.copy(n, s).wait_send()


LAST = 6


def enter(size):
    me = lax.axis_index('model')
    barrier = pltpu.get_barrier_semaphore()
    for other in (lax.rem(me + 2, size), lax.rem(me + size - 2, size), me + 1 - 2 * lax.rem(me, 2)):
        pl.semaphore_signal(barrier, inc=1, device_id={'model': other}, device_id_type=MESH)
    pl.semaphore_wait(barrier, 3)


def drain_count(points, start):
    return (start + LAST) // points


def make_progress(count, points, sums):
    def progress(t, i):
        for ring, start, consume in sums:
            for j in range(LAST, 0, -1):
                if (start + j - i) % points:
                    continue
                s = t - (start + j - i) // points

                @pl.when(jnp.logical_and(s >= 0, s < count))
                def _(ring=ring, consume=consume, j=j, s=s):
                    ring.stage(j, s)
                    if j == LAST:
                        consume(s)
    return progress


def norm_stats(x):
    mean = jnp.mean(x, axis=-1, keepdims=True)
    centered = x - mean
    var = jnp.mean(centered * centered, axis=-1, keepdims=True)
    inv = lax.rsqrt(var + NORM_EPS)
    return centered * inv, inv


def norm_back(x, gain, d_normed):
    unit, inv = norm_stats(x)
    d_unit = d_normed * gain
    mean_d = jnp.mean(d_unit, axis=-1, keepdims=True)
    mean_du = jnp.mean(d_unit * unit, axis=-1, keepdims=True)
    return inv * (d_unit - mean_d - unit * mean_du), d_normed * unit


def probs_of(q, k, seg_col, seg_row, row0, scale):
    scores = mt(q, k) * scale
    q_pos = row0 + lax.broadcasted_iota(jnp.int32, scores.shape, 0)
    k_pos = lax.broadcasted_iota(jnp.int32, scores.shape, 1)
    allowed = jnp.logical_and(seg_col == seg_row, q_pos >= k_pos)
    scores = jnp.where(allowed, scores, -1e30)
    e = jnp.exp(scores - jnp.max(scores, axis=-1, keepdims=True))
    return e * (1.0 / jnp.sum(e, axis=-1, keepdims=True))


def head_masks(width, head_dim):
    lane = lax.broadcasted_iota(jnp.int32, (1, width), 1)
    return [jnp.logical_and(lane >= h * head_dim, lane < (h + 1) * head_dim) for h in range(width // head_dim)]


Q_ROWS = 128


def attn_forward_kernel(size, head_dim, tok_hbm, seg_row, seg_col, gain, w_qkv, w_out,
                        x1_hbm, a_hbm, saved_hbm,
                        x, a, saved, part, pair_in, relay_in, ring_in, whole,
                        in_sem, x1_sem, a_sem, saved_sem, send, recv):
    count = x.shape[0]
    rows, hidden = x.shape[1] * x.shape[2], x.shape[3]
    width = w_out.shape[0]
    scale = head_dim ** -0.5
    points, start = 3, 2
    steps = count + drain_count(points, start)

    def x_in(s):
        return pltpu.make_async_copy(tok_hbm.at[s], x.at[s], in_sem.at[s])

    def x_out(s):
        return pltpu.make_async_copy(x.at[s], x1_hbm.at[s], x1_sem.at[s])

    def a_out(s):
        slot = lax.rem(s, 2)
        return pltpu.make_async_copy(a.at[slot], a_hbm.at[s], a_sem.at[slot])

    def saved_out(s):
        slot = lax.rem(s, 2)
        return pltpu.make_async_copy(saved.at[slot], saved_hbm.at[s], saved_sem.at[slot])

    loop(count, lambda s: x_in(s).start())
    enter(size)
    ring = RingSum(size, part, pair_in, relay_in, ring_in, whole, send, recv)

    def consume(s):
        slot = lax.rem(s, SLOTS)

        def block(r):
            x[s, r] = (x[s, r].astype(F32) + whole[slot, r].astype(F32)).astype(BF16)
        loop(BLOCKS, block)
        x_out(s).start()

    progress = make_progress(count, points, [(ring, start, consume)])
    masks = head_masks(width, head_dim)

    def step(t):
        slot2 = lax.rem(t, 2)

        @pl.when(t < count)
        def _():
            x_in(t).wait()

            @pl.when(t >= 2)
            def _():
                a_out(t - 2).wait()
                saved_out(t - 2).wait()

            def block(r):
                unit, _ = norm_stats(x[t, r].astype(F32))
                a[slot2, r] = (unit * gain[...]).astype(BF16)
            loop(BLOCKS, block)
            a_out(t).start()

        progress(t, 0)

        @pl.when(t < count)
        def _():
            a_rows = a[slot2].reshape(rows, hidden)
            saved[slot2, :, :3 * width] = mm(a_rows, w_qkv[...]).astype(BF16)

            def q_block(i):
                row0 = pl.multiple_of(i * Q_ROWS, Q_ROWS)
                part_rows = pl.ds(row0, Q_ROWS)
                q = saved[slot2, part_rows, 0:width]
                k = saved[slot2, :, width:2 * width]
                v = saved[slot2, :, 2 * width:3 * width]
                out = None
                for mask in masks:
                    probs = probs_of(jnp.where(mask, q, 0).astype(BF16), k, seg_col[t, part_rows], seg_row[t], row0, scale)
                    head = mm(probs.astype(BF16), v)
                    out = head if out is None else jnp.where(mask, head, out)
                saved[slot2, part_rows, 3 * width:4 * width] = out.astype(BF16)
            loop(rows // Q_ROWS, q_block)

        progress(t, 1)

        @pl.when(t < count)
        def _():
            slot = lax.rem(t, SLOTS)
            half = rows // 2
            for h in range(2):
                proj = mm(saved[slot2, h * half:(h + 1) * half, 3 * width:4 * width], w_out[...])
                part[slot, h * HALF:(h + 1) * HALF] = proj.astype(BF16).reshape(HALF, rows // BLOCKS, hidden)
            saved_out(t).start()
            ring.stage(0, t)

        progress(t, 2)

    loop(steps, step)
    loop(count, lambda s: x_out(s).wait())
    for s in (count - 2, count - 1):
        a_out(s).wait()
        saved_out(s).wait()


def mlp_kernel(size, x1_hbm, dout_hbm, gain, w_up, w_down,
               out_hbm, db_hbm, dw_up_out, dw_down_out,
               x, d, b, pre, d_hid, u, d_pre, dw_up, dw_down,
               part1, pair_in1, relay_in1, ring_in1, whole1,
               part2, pair_in2, relay_in2, ring_in2, whole2,
               x_sem, d_sem, out_sem, db_sem, send1, recv1, send2, recv2):
    count = x.shape[0]
    block_rows, hidden = x.shape[2], x.shape[3]
    rows = BLOCKS * block_rows
    points, start = 4, 2
    steps = count + drain_count(points, start)

    def x_in(s):
        return pltpu.make_async_copy(x1_hbm.at[s], x.at[s], x_sem.at[s])

    def x_out(s):
        return pltpu.make_async_copy(x.at[s], out_hbm.at[s], out_sem.at[s])

    def d_in(s):
        slot = lax.rem(s, 2)
        return pltpu.make_async_copy(dout_hbm.at[s], d.at[slot], d_sem.at[slot])

    def db_out(s):
        slot = lax.rem(s, SLOTS)
        return pltpu.make_async_copy(whole1.at[slot], db_hbm.at[s], db_sem.at[slot])

    d_in(0).start()
    loop(count, lambda s: x_in(s).start())
    enter(size)
    ring1 = RingSum(size, part1, pair_in1, relay_in1, ring_in1, whole1, send1, recv1)
    ring2 = RingSum(size, part2, pair_in2, relay_in2, ring_in2, whole2, send2, recv2)
    dw_up[...] = jnp.zeros_like(dw_up)
    dw_down[...] = jnp.zeros_like(dw_down)

    def consume1(s):
        db_out(s).start()

    def consume2(s):
        slot = lax.rem(s, SLOTS)

        def block(r):
            x[s, r] = (x[s, r].astype(F32) + whole2[slot, r].astype(F32)).astype(BF16)
        loop(BLOCKS, block)
        x_out(s).start()

    progress = make_progress(count, points, [(ring1, start, consume1), (ring2, start, consume2)])

    def step(t):
        slot = lax.rem(t, SLOTS)
        slot2 = lax.rem(t, 2)

        @pl.when(t < count)
        def _():
            x_in(t).wait()
            d_in(t).wait()

            @pl.when(t + 1 < count)
            def _():
                d_in(t + 1).start()

            def block(r):
                unit, _ = norm_stats(x[t, r].astype(F32))
                b[r] = (unit * gain[...]).astype(BF16)
            loop(BLOCKS, block)
            pre[...] = mm(b[...].reshape(rows, hidden), w_up[...])

        progress(t, 0)

        @pl.when(t < count)
        def _():
            d_hid[...] = mt(d[slot2].reshape(rows, hidden), w_down[...])

            def block(r):
                part_rows = pl.ds(pl.multiple_of(r * block_rows, block_rows), block_rows)
                v = pre[part_rows]
                v2 = v * v
                c = 0.7978845608028654
                th = jnp.tanh(c * (v + 0.044715 * (v * v2)))
                u[part_rows] = (0.5 * v * (1.0 + th)).astype(BF16)
                slope = 0.5 * (1.0 + th) + 0.5 * v * (1.0 - th * th) * (c * (1.0 + 3.0 * 0.044715 * v2))
                d_pre[part_rows] = (d_hid[part_rows].astype(BF16).astype(F32) * slope).astype(BF16)
            loop(BLOCKS, block)

        progress(t, 1)

        @pl.when(t < count)
        def _():
            @pl.when(t >= SLOTS)
            def _():
                db_out(t - SLOTS).wait()
            half = rows // 2
            for h in range(2):
                d_b = mt(d_pre[h * half:(h + 1) * half], w_up[...])
                part1[slot, h * HALF:(h + 1) * HALF] = d_b.astype(BF16).reshape(HALF, block_rows, hidden)
            ring1.stage(0, t)
            for h in range(2):
                down = mm(u[h * half:(h + 1) * half], w_down[...])
                part2[slot, h * HALF:(h + 1) * HALF] = down.astype(BF16).reshape(HALF, block_rows, hidden)
            ring2.stage(0, t)

        progress(t, 2)

        @pl.when(t < count)
        def _():
            dw_up[...] += tm(b[...].reshape(rows, hidden), d_pre[...])
            dw_down[...] += tm(u[...], d[slot2].reshape(rows, hidden))

        progress(t, 3)

    loop(steps, step)
    dw_up_out[...] = dw_up[...].astype(BF16)
    dw_down_out[...] = dw_down[...].astype(BF16)
    loop(count, lambda s: x_out(s).wait())
    for s in range(count - SLOTS, count):
        db_out(s).wait()


def attn_backward_kernel(size, head_dim, tok_hbm, dout_hbm, x1_hbm, db_hbm, a_hbm, saved_hbm,
                         seg_row, seg_col, gain_attn, gain_mlp, w_qkv, w_out,
                         dtok_hbm, dw_qkv_out, dw_out_out, dg_attn_out, dg_mlp_out,
                         x, d, x1, db, a, saved, d_heads, probs, d_scores, d_qkv,
                         dw_qkv, dw_out, dg_attn, dg_mlp,
                         part, pair_in, relay_in, ring_in, whole,
                         x_sem, d_sem, x1_sem, db_sem, a_sem, saved_sem, out_sem, send, recv):
    count = x.shape[0]
    block_rows, hidden = x.shape[2], x.shape[3]
    rows = BLOCKS * block_rows
    width = w_out.shape[0]
    scale = head_dim ** -0.5
    points, start = 3, 2
    steps = count + drain_count(points, start)

    def whole_in(s):
        return [pltpu.make_async_copy(tok_hbm.at[s], x.at[s], x_sem.at[s]),
                pltpu.make_async_copy(dout_hbm.at[s], d.at[s], d_sem.at[s])]

    def slot_in(s):
        slot = lax.rem(s, 2)
        return [pltpu.make_async_copy(x1_hbm.at[s], x1.at[slot], x1_sem.at[slot]),
                pltpu.make_async_copy(db_hbm.at[s], db.at[slot], db_sem.at[slot]),
                pltpu.make_async_copy(a_hbm.at[s], a.at[slot], a_sem.at[slot]),
                pltpu.make_async_copy(saved_hbm.at[s], saved.at[slot], saved_sem.at[slot])]

    def x_out(s):
        return pltpu.make_async_copy(x.at[s], dtok_hbm.at[s], out_sem.at[s])

    for c in slot_in(0) + whole_in(0):
        c.start()
    enter(size)
    ring = RingSum(size, part, pair_in, relay_in, ring_in, whole, send, recv)
    for ref in (dw_qkv, dw_out, dg_attn, dg_mlp):
        ref[...] = jnp.zeros_like(ref)

    def rows_sum(v):
        return jnp.sum(v.reshape(v.shape[0] // 8, 8, hidden), axis=0)

    def consume(s):
        slot = lax.rem(s, SLOTS)

        def block(r):
            dx, dg = norm_back(x[s, r].astype(F32), gain_attn[...], whole[slot, r].astype(F32))
            dg_attn[...] += rows_sum(dg)
            x[s, r] = (d[s, r].astype(F32) + dx).astype(BF16)
        loop(BLOCKS, block)
        x_out(s).start()

    progress = make_progress(count, points, [(ring, start, consume)])
    masks = head_masks(width, head_dim)

    def step(t):
        slot = lax.rem(t, SLOTS)
        slot2 = lax.rem(t, 2)

        @pl.when(t < count)
        def _():
            for c in slot_in(t) + whole_in(t):
                c.wait()

            @pl.when(t + 1 < count)
            def _():
                for c in slot_in(t + 1) + whole_in(t + 1):
                    c.start()

            def block(r):
                dx, dg = norm_back(x1[slot2, r].astype(F32), gain_mlp[...], db[slot2, r].astype(F32))
                dg_mlp[...] += rows_sum(dg)
                d[t, r] = (d[t, r].astype(F32) + dx).astype(BF16)
            loop(BLOCKS, block)
            d_rows = d[t].reshape(rows, hidden)
            d_heads[...] = mt(d_rows, w_out[...]).astype(BF16)

        progress(t, 0)

        @pl.when(t < count)
        def _():
            q_all = saved[slot2, :, 0:width]
            k_all = saved[slot2, :, width:2 * width]
            v_all = saved[slot2, :, 2 * width:3 * width]
            for h, mask in enumerate(masks):
                def q_block(i):
                    row0 = pl.multiple_of(i * Q_ROWS, Q_ROWS)
                    part_rows = pl.ds(row0, Q_ROWS)
                    q = jnp.where(mask, saved[slot2, part_rows, 0:width], 0).astype(BF16)
                    d_head = jnp.where(mask, d_heads[part_rows], 0).astype(BF16)
                    p = probs_of(q, saved[slot2, :, width:2 * width], seg_col[t, part_rows], seg_row[t], row0, scale)
                    d_p = mt(d_head, saved[slot2, :, 2 * width:3 * width])
                    row_dot = jnp.sum(d_p * p, axis=-1, keepdims=True)
                    probs[part_rows] = p.astype(BF16)
                    d_scores[part_rows] = (p * (d_p - row_dot) * scale).astype(BF16)
                loop(rows // Q_ROWS, q_block)
                d_q = mm(d_scores[...], k_all).astype(BF16)
                d_k = tm(d_scores[...], q_all).astype(BF16)
                d_v = tm(probs[...], d_heads[...]).astype(BF16)
                for j, value in enumerate((d_q, d_k, d_v)):
                    cols = slice(j * width, (j + 1) * width)
                    d_qkv[:, cols] = value if h == 0 else jnp.where(mask, value, d_qkv[:, cols])

        progress(t, 1)

        @pl.when(t < count)
        def _():
            half = rows // 2
            for h in range(2):
                d_a = mt(d_qkv[h * half:(h + 1) * half], w_qkv[...])
                part[slot, h * HALF:(h + 1) * HALF] = d_a.astype(BF16).reshape(HALF, block_rows, hidden)
            ring.stage(0, t)
            dw_qkv[...] += tm(a[slot2].reshape(rows, hidden), d_qkv[...])
            dw_out[...] += tm(saved[slot2, :, 3 * width:4 * width], d[t].reshape(rows, hidden))

        progress(t, 2)

    loop(steps, step)
    dw_qkv_out[...] = dw_qkv[...].astype(BF16)
    dw_out_out[...] = dw_out[...].astype(BF16)
    dg_attn_out[...] = jnp.sum(dg_attn[...], axis=0, keepdims=True)
    dg_mlp_out[...] = jnp.sum(dg_mlp[...], axis=0, keepdims=True)
    loop(count, lambda s: x_out(s).wait())


def ring_buffers(block_rows, hidden):
    return [
        pltpu.VMEM((SLOTS, BLOCKS, block_rows, hidden), BF16),
        pltpu.VMEM((SLOTS, HALF, block_rows, hidden), BF16),
        pltpu.VMEM((SLOTS, 2, block_rows, hidden), BF16),
        pltpu.VMEM((SLOTS, 2, PIECE, block_rows, hidden), BF16),
        pltpu.VMEM((SLOTS, BLOCKS, block_rows, hidden), BF16),
    ]


def ring_sems():
    return [pltpu.SemaphoreType.DMA((SLOTS, COPIES)), pltpu.SemaphoreType.DMA((SLOTS, COPIES))]


def run_kernel(kernel, ident, outs, out_vmem, args, in_vmem, scratch):
    def spec(in_vmem):
        return pl.BlockSpec(memory_space=pltpu.VMEM if in_vmem else pl.ANY)
    return pl.pallas_call(
        kernel,
        out_shape=[jax.ShapeDtypeStruct(s, t) for s, t in outs],
        in_specs=[spec(v) for v in in_vmem],
        out_specs=[spec(v) for v in out_vmem],
        scratch_shapes=scratch,
        compiler_params=pltpu.CompilerParams(collective_id=ident, has_side_effects=True, vmem_limit_bytes=VMEM_LIMIT),
        name=f'layer_part_{ident}',
    )(*args)


def solution(mesh):
    size = mesh.shape['model']
    dma = pltpu.SemaphoreType.DMA

    def device_step(tokens, seg_ids, d_out, gain_attn, gain_mlp, w_qkv, w_out, w_up, w_down):
        count, seq_len, hidden = tokens.shape
        heads, head_dim = w_qkv.shape[1], w_qkv.shape[3]
        width = heads * head_dim
        inner = w_up.shape[1]
        block_rows = seq_len // BLOCKS
        act = (count, BLOCKS, block_rows, hidden)
        one = (BLOCKS, block_rows, hidden)
        x = tokens.reshape(act)
        d = d_out.reshape(act)
        seg_row = seg_ids.reshape(count, 1, seq_len)
        seg_col = seg_ids.reshape(count, seq_len, 1)
        g_attn = gain_attn.astype(F32).reshape(1, hidden)
        g_mlp = gain_mlp.astype(F32).reshape(1, hidden)
        wqkv = w_qkv.transpose(0, 2, 1, 3).reshape(hidden, 3 * width)
        wout = w_out.reshape(width, hidden)

        x1, a, saved = run_kernel(
            functools.partial(attn_forward_kernel, size, head_dim), 1,
            [(act, BF16), (act, BF16), ((count, seq_len, 4 * width), BF16)], [False] * 3,
            [x, seg_row, seg_col, g_attn, wqkv, wout], [False] + [True] * 5,
            [pltpu.VMEM(act, BF16), pltpu.VMEM((2,) + one, BF16), pltpu.VMEM((2, seq_len, 4 * width), BF16)]
            + ring_buffers(block_rows, hidden)
            + [dma((count,)), dma((count,)), dma((2,)), dma((2,))] + ring_sems())

        layer_out, d_b, d_w_up, d_w_down = run_kernel(
            functools.partial(mlp_kernel, size), 2,
            [(act, BF16), (act, BF16), ((hidden, inner), BF16), ((inner, hidden), BF16)], [False, False, True, True],
            [x1, d, g_mlp, w_up, w_down], [False, False, True, True, True],
            [pltpu.VMEM(act, BF16), pltpu.VMEM((2,) + one, BF16), pltpu.VMEM(one, BF16),
             pltpu.VMEM((seq_len, inner), F32), pltpu.VMEM((seq_len, inner), F32),
             pltpu.VMEM((seq_len, inner), BF16), pltpu.VMEM((seq_len, inner), BF16),
             pltpu.VMEM((hidden, inner), F32), pltpu.VMEM((inner, hidden), F32)]
            + ring_buffers(block_rows, hidden) + ring_buffers(block_rows, hidden)
            + [dma((count,)), dma((2,)), dma((count,)), dma((SLOTS,))] + ring_sems() + ring_sems())

        d_tokens, dw_qkv, dw_out, dg_attn, dg_mlp = run_kernel(
            functools.partial(attn_backward_kernel, size, head_dim), 3,
            [(act, BF16), ((hidden, 3 * width), BF16), ((width, hidden), BF16), ((1, hidden), F32), ((1, hidden), F32)],
            [False] + [True] * 4,
            [x, d, x1, d_b, a, saved, seg_row, seg_col, g_attn, g_mlp, wqkv, wout], [False] * 6 + [True] * 6,
            [pltpu.VMEM(act, BF16), pltpu.VMEM(act, BF16)] + [pltpu.VMEM((2,) + one, BF16)] * 3
            + [pltpu.VMEM((2, seq_len, 4 * width), BF16), pltpu.VMEM((seq_len, width), BF16),
               pltpu.VMEM((seq_len, seq_len), BF16), pltpu.VMEM((seq_len, seq_len), BF16),
               pltpu.VMEM((seq_len, 3 * width), BF16),
               pltpu.VMEM((hidden, 3 * width), F32), pltpu.VMEM((width, hidden), F32),
               pltpu.VMEM((8, hidden), F32), pltpu.VMEM((8, hidden), F32)]
            + ring_buffers(block_rows, hidden)
            + [dma((count,)), dma((count,))] + [dma((2,))] * 4 + [dma((count,))] + ring_sems())

        d_w_qkv = dw_qkv.reshape(hidden, 3, heads, head_dim).transpose(0, 2, 1, 3)
        return (layer_out.reshape(tokens.shape), d_tokens.reshape(tokens.shape), d_w_qkv,
                dw_out.reshape(w_out.shape), d_w_up, d_w_down, dg_attn.reshape(hidden), dg_mlp.reshape(hidden))

    in_specs = (P('data', None, None), P('data', None), P('data', None, None), P(), P(), P(None, 'model', None, None), P('model', None, None), P(None, 'model'), P('model', None))
    out_specs = (P('data', None, None), P('data', None, None), P('data', 'model', None, None), P(('data', 'model'), None, None), P('data', 'model'), P(('data', 'model'), None), P('data'), P('data'))
    return jax.shard_map(device_step, mesh=mesh, in_specs=in_specs, out_specs=out_specs, check_vma=False)
```

```python
import functools
import jax
import jax.numpy as jnp
from jax import lax
from jax.experimental import pallas as pl
from jax.experimental.pallas import tpu as pltpu
from jax.sharding import PartitionSpec as P

NORM_EPS = 1e-5
MESH = pl.DeviceIdType.MESH
F32 = jnp.float32
BF16 = jnp.bfloat16
SLOTS = 2
SPACING = 2
POINTS = 12
BLOCKS = 16
HALF = BLOCKS // 2
PIECE = 2
COPIES = 13
VMEM_LIMIT = 66 * 1000 * 1000


def mm(a, b):
    return lax.dot_general(a, b, (((1,), (0,)), ((), ())), preferred_element_type=F32)


def mt(a, b):
    return lax.dot_general(a, b, (((1,), (1,)), ((), ())), preferred_element_type=F32)


def tm(a, b):
    return lax.dot_general(a, b, (((0,), (0,)), ((), ())), preferred_element_type=F32)


def loop(count, body):
    def step(i, carry):
        body(i)
        return carry
    lax.fori_loop(0, count, step, 0)


class RingSum:
    def __init__(self, size, part, pair_in, relay_in, ring_in, whole, send, recv):
        me = lax.axis_index('model')
        self.core = lax.rem(me, 2)
        self.chips = size // 2
        self.chip = me // 2
        self.right = lax.rem(me + 2, size)
        self.left = lax.rem(me + size - 2, size)
        self.partner = me + 1 - 2 * self.core
        self.part, self.pair_in, self.relay_in, self.ring_in, self.whole = part, pair_in, relay_in, ring_in, whole
        self.send, self.recv = send, recv

    def base(self, core, step):
        return core * HALF + lax.rem(self.chip + step, self.chips) * PIECE

    def copy(self, n, s):
        slot = lax.rem(s, SLOTS)
        part, whole = self.part.at[slot], self.whole.at[slot]
        base = functools.partial(self.base, self.core)
        last = self.chips - 1
        if n == 0:
            src, dst, to = part.at[pl.ds((1 - self.core) * HALF, HALF)], self.pair_in.at[slot], self.partner
        elif n == 1:
            src, dst, to = part.at[pl.ds(base(2), 1)], self.relay_in.at[slot, pl.ds(0, 1)], self.right
        elif n == 2:
            src, dst, to = part.at[pl.ds(base(2) + 1, 1)], self.relay_in.at[slot, pl.ds(1, 1)], self.left
        elif n == 3:
            src, dst, to = part.at[pl.ds(base(1), PIECE)], self.ring_in.at[slot, 0], self.right
        elif n == 4:
            src, dst, to = part.at[pl.ds(base(last), PIECE)], self.ring_in.at[slot, 1], self.left
        else:
            start, length, to = {
                5: (base(0), PIECE, self.right),
                6: (base(0), PIECE, self.left),
                7: (base(0), PIECE, self.partner),
                8: (base(last), 1, self.right),
                9: (base(1) + 1, 1, self.left),
                10: (base(last), PIECE, self.partner),
                11: (base(1), PIECE, self.partner),
                12: (base(2), PIECE, self.partner),
            }[n]
            src = dst = whole.at[pl.ds(start, length)]
        return pltpu.make_async_remote_copy(
            src_ref=src, dst_ref=dst, send_sem=self.send.at[slot, n], recv_sem=self.recv.at[slot, n],
            device_id={'model': to}, device_id_type=MESH)

    def add(self, slot, block, others):
        total = self.part[slot, block].astype(F32)
        for ref in others:
            total = total + ref.astype(F32)
        return total.astype(BF16)

    def stage(self, j, s):
        slot = lax.rem(s, SLOTS)
        last = self.chips - 1
        if j == 0:
            self.copy(0, s).start()
        elif j == 1:
            self.copy(0, s).wait_recv()

            def pair(i):
                block = self.core * HALF + i
                self.part[slot, block] = self.add(slot, block, [self.pair_in[slot, i]])
            loop(HALF, pair)
            self.copy(1, s).start()
            self.copy(2, s).start()
        elif j == 2:
            self.copy(1, s).wait_recv()
            self.copy(2, s).wait_recv()
            first, second = self.base(self.core, 1), self.base(self.core, last) + 1
            self.part[slot, first] = self.add(slot, first, [self.relay_in[slot, 0]])
            self.part[slot, second] = self.add(slot, second, [self.relay_in[slot, 1]])
            self.copy(3, s).start()
            self.copy(4, s).start()
        elif j == 3:
            self.copy(3, s).wait_recv()
            self.copy(4, s).wait_recv()
            for i in range(PIECE):
                block = self.base(self.core, 0) + i
                self.whole[slot, block] = self.add(slot, block, [self.ring_in[slot, 0, i], self.ring_in[slot, 1, i]])
            for n in (5, 6, 7):
                self.copy(n, s).start()
        elif j == 4:
            self.copy(5, s).wait_recv()
            self.copy(6, s).wait_recv()
            for n in (8, 9, 10, 11):
                self.copy(n, s).start()
        elif j == 5:
            self.copy(8, s).wait_recv()
            self.copy(9, s).wait_recv()
            self.copy(12, s).start()
        else:
            for n in (7, 10, 11, 12):
                self.copy(n, s).wait_recv()
            for n in range(COPIES):
                self.copy(n, s).wait_send()


LAST = 6


def enter(size):
    me = lax.axis_index('model')
    barrier = pltpu.get_barrier_semaphore()
    for other in (lax.rem(me + 2, size), lax.rem(me + size - 2, size), me + 1 - 2 * lax.rem(me, 2)):
        pl.semaphore_signal(barrier, inc=1, device_id={'model': other}, device_id_type=MESH)
    pl.semaphore_wait(barrier, 3)


def make_progress(count, points, sums):
    def progress(t, i):
        for ring, lead, start, consume in sums:
            for j in range(LAST, 0, -1):
                ahead = start + SPACING * j - i
                if ahead % points:
                    continue
                s = t - lead - ahead // points

                @pl.when(jnp.logical_and(s >= 0, s < count))
                def _(ring=ring, consume=consume, j=j, s=s):
                    ring.stage(j, s)
                    if j == LAST and consume is not None:
                        consume(s)
    return progress


def norm_stats(x):
    mean = jnp.mean(x, axis=-1, keepdims=True)
    centered = x - mean
    var = jnp.mean(centered * centered, axis=-1, keepdims=True)
    inv = lax.rsqrt(var + NORM_EPS)
    return centered * inv, inv


def norm_back(x, gain, d_normed):
    unit, inv = norm_stats(x)
    d_unit = d_normed * gain
    mean_d = jnp.mean(d_unit, axis=-1, keepdims=True)
    mean_du = jnp.mean(d_unit * unit, axis=-1, keepdims=True)
    return inv * (d_unit - mean_d - unit * mean_du), d_normed * unit


def probs_of(q, k, seg_col, seg_row, row0, scale):
    scores = mt(q, k) * scale
    q_pos = row0 + lax.broadcasted_iota(jnp.int32, scores.shape, 0)
    k_pos = lax.broadcasted_iota(jnp.int32, scores.shape, 1)
    allowed = jnp.logical_and(seg_col == seg_row, q_pos >= k_pos)
    scores = jnp.where(allowed, scores, -1e30)
    e = jnp.exp(scores - jnp.max(scores, axis=-1, keepdims=True))
    return e * (1.0 / jnp.sum(e, axis=-1, keepdims=True))


def head_masks(width, head_dim):
    lane = lax.broadcasted_iota(jnp.int32, (1, width), 1)
    return [jnp.logical_and(lane >= h * head_dim, lane < (h + 1) * head_dim) for h in range(width // head_dim)]


Q_ROWS = 128
X_SLOTS = 5
D_SLOTS = 4
A_SLOTS = 3


def layer_kernel(size, head_dim, *refs):
    (tok_hbm, dout_hbm, seg_row, seg_col, gain_attn, gain_mlp, w_qkv, w_out, w_up, w_down,
     out_hbm, dtok_hbm, dw_qkv_out, dw_out_out, dw_up_out, dw_down_out, dg_attn_out, dg_mlp_out,
     x, d, x1, a, saved, b, pre, d_hid, u, d_pre, d_heads, probs, d_scores, d_qkv,
     dw_qkv, dw_out, dw_up, dw_down, dg_attn, dg_mlp,
     x_sem, d_sem, out_sem, dtok_sem) = refs[:42]
    rings = [RingSum(size, *refs[42 + 7 * n:49 + 7 * n]) for n in range(4)]
    ring_p1, ring_db, ring_p2, ring_da = rings
    count = tok_hbm.shape[0]
    block_rows, hidden = x.shape[2], x.shape[3]
    rows = BLOCKS * block_rows
    half = rows // 2
    width = w_out.shape[0]
    scale = head_dim ** -0.5
    masks = head_masks(width, head_dim)

    def x_in(s):
        slot = lax.rem(s, X_SLOTS)
        return pltpu.make_async_copy(tok_hbm.at[s], x.at[slot], x_sem.at[slot])

    def d_in(s):
        slot = lax.rem(s, D_SLOTS)
        return pltpu.make_async_copy(dout_hbm.at[s], d.at[slot], d_sem.at[slot])

    def out_copy(s):
        slot = lax.rem(s, SLOTS)
        return pltpu.make_async_copy(ring_p2.whole.at[slot], out_hbm.at[s], out_sem.at[slot])

    def dtok_copy(s):
        slot = lax.rem(s, SLOTS)
        return pltpu.make_async_copy(ring_da.whole.at[slot], dtok_hbm.at[s], dtok_sem.at[slot])

    def rows_sum(v):
        return jnp.sum(v.reshape(v.shape[0] // 8, 8, hidden), axis=0)

    def consume_p1(s):
        slot = lax.rem(s, SLOTS)

        def block(r):
            x1[slot, r] = (x[lax.rem(s, X_SLOTS), r].astype(F32) + ring_p1.whole[slot, r].astype(F32)).astype(BF16)
        loop(BLOCKS, block)

    def consume_p2(s):
        slot = lax.rem(s, SLOTS)

        def block(r):
            ring_p2.whole[slot, r] = (x1[slot, r].astype(F32) + ring_p2.whole[slot, r].astype(F32)).astype(BF16)
        loop(BLOCKS, block)
        out_copy(s).start()

    def consume_da(s):
        slot = lax.rem(s, SLOTS)

        def block(r):
            dx, dg = norm_back(x[lax.rem(s, X_SLOTS), r].astype(F32), gain_attn[...], ring_da.whole[slot, r].astype(F32))
            dg_attn[...] += rows_sum(dg)
            ring_da.whole[slot, r] = (d[lax.rem(s, D_SLOTS), r].astype(F32) + dx).astype(BF16)
        loop(BLOCKS, block)
        dtok_copy(s).start()

    def store_part(ring, slot, h, value):
        ring.part[slot, h * HALF:(h + 1) * HALF] = value.astype(BF16).reshape(HALF, block_rows, hidden)

    def norm_in(s):
        x_in(s).wait()

        def block(r):
            unit, _ = norm_stats(x[lax.rem(s, X_SLOTS), r].astype(F32))
            a[lax.rem(s, A_SLOTS), r] = (unit * gain_attn[...]).astype(BF16)
        loop(BLOCKS, block)
        slot = lax.rem(s, A_SLOTS)
        saved[slot, :, :3 * width] = mm(a[slot].reshape(rows, hidden), w_qkv[...]).astype(BF16)

    def attend(s):
        slot = lax.rem(s, A_SLOTS)

        def q_block(i):
            row0 = pl.multiple_of(i * Q_ROWS, Q_ROWS)
            part_rows = pl.ds(row0, Q_ROWS)
            q = saved[slot, part_rows, 0:width]
            k = saved[slot, :, width:2 * width]
            v = saved[slot, :, 2 * width:3 * width]
            out = None
            for mask in masks:
                p = probs_of(jnp.where(mask, q, 0).astype(BF16), k, seg_col[s, part_rows], seg_row[s], row0, scale)
                head = mm(p.astype(BF16), v)
                out = head if out is None else jnp.where(mask, head, out)
            saved[slot, part_rows, 3 * width:4 * width] = out.astype(BF16)
        loop(rows // Q_ROWS, q_block)

    def project(s):
        for h in range(2):
            proj = mm(saved[lax.rem(s, A_SLOTS), h * half:(h + 1) * half, 3 * width:4 * width], w_out[...])
            store_part(ring_p1, lax.rem(s, SLOTS), h, proj)
        ring_p1.stage(0, s)

    def norm_mid(s):
        def block(r):
            unit, _ = norm_stats(x1[lax.rem(s, SLOTS), r].astype(F32))
            b[r] = (unit * gain_mlp[...]).astype(BF16)
        loop(BLOCKS, block)
        d_in(s).wait()

    def up(s):
        pre[...] = mm(b[...].reshape(rows, hidden), w_up[...])
        d_hid[...] = mt(d[lax.rem(s, D_SLOTS)].reshape(rows, hidden), w_down[...])

    def gelu_both(s):
        def block(r):
            part_rows = pl.ds(pl.multiple_of(r * block_rows, block_rows), block_rows)
            v = pre[part_rows]
            v2 = v * v
            c = 0.7978845608028654
            th = jnp.tanh(c * (v + 0.044715 * (v * v2)))
            u[part_rows] = (0.5 * v * (1.0 + th)).astype(BF16)
            slope = 0.5 * (1.0 + th) + 0.5 * v * (1.0 - th * th) * (c * (1.0 + 3.0 * 0.044715 * v2))
            d_pre[part_rows] = (d_hid[part_rows].astype(BF16).astype(F32) * slope).astype(BF16)
        loop(BLOCKS, block)

    def grad_b(s):
        for h in range(2):
            store_part(ring_db, lax.rem(s, SLOTS), h, mt(d_pre[h * half:(h + 1) * half], w_up[...]))
        ring_db.stage(0, s)

    def down(s):
        @pl.when(s >= SLOTS)
        def _():
            out_copy(s - SLOTS).wait()
        for h in range(2):
            store_part(ring_p2, lax.rem(s, SLOTS), h, mm(u[h * half:(h + 1) * half], w_down[...]))
        ring_p2.stage(0, s)
        dw_up[...] += tm(b[...].reshape(rows, hidden), d_pre[...])
        dw_down[...] += tm(u[...], d[lax.rem(s, D_SLOTS)].reshape(rows, hidden))

    def grad_mid(s):
        slot = lax.rem(s, SLOTS)
        d_slot = lax.rem(s, D_SLOTS)

        def block(r):
            dx, dg = norm_back(x1[slot, r].astype(F32), gain_mlp[...], ring_db.whole[slot, r].astype(F32))
            dg_mlp[...] += rows_sum(dg)
            d[d_slot, r] = (d[d_slot, r].astype(F32) + dx).astype(BF16)
        loop(BLOCKS, block)
        d_rows = d[d_slot].reshape(rows, hidden)
        d_heads[...] = mt(d_rows, w_out[...]).astype(BF16)
        dw_out[...] += tm(saved[lax.rem(s, A_SLOTS), :, 3 * width:4 * width], d_rows)

    def attend_back(h, s):
        mask = masks[h]
        slot = lax.rem(s, A_SLOTS)

        def q_block(i):
            row0 = pl.multiple_of(i * Q_ROWS, Q_ROWS)
            part_rows = pl.ds(row0, Q_ROWS)
            q = jnp.where(mask, saved[slot, part_rows, 0:width], 0).astype(BF16)
            d_head = jnp.where(mask, d_heads[part_rows], 0).astype(BF16)
            p = probs_of(q, saved[slot, :, width:2 * width], seg_col[s, part_rows], seg_row[s], row0, scale)
            d_p = mt(d_head, saved[slot, :, 2 * width:3 * width])
            row_dot = jnp.sum(d_p * p, axis=-1, keepdims=True)
            probs[part_rows] = p.astype(BF16)
            d_scores[part_rows] = (p * (d_p - row_dot) * scale).astype(BF16)
        loop(rows // Q_ROWS, q_block)
        d_q = mm(d_scores[...], saved[slot, :, width:2 * width]).astype(BF16)
        d_k = tm(d_scores[...], saved[slot, :, 0:width]).astype(BF16)
        d_v = tm(probs[...], d_heads[...]).astype(BF16)
        for j, value in enumerate((d_q, d_k, d_v)):
            cols = slice(j * width, (j + 1) * width)
            d_qkv[:, cols] = value if h == 0 else jnp.where(mask, value, d_qkv[:, cols])

    def grad_a(s):
        @pl.when(s >= SLOTS)
        def _():
            dtok_copy(s - SLOTS).wait()
        for h in range(2):
            store_part(ring_da, lax.rem(s, SLOTS), h, mt(d_qkv[h * half:(h + 1) * half], w_qkv[...]))
        ring_da.stage(0, s)
        dw_qkv[...] += tm(a[lax.rem(s, A_SLOTS)].reshape(rows, hidden), d_qkv[...])

    work = [(0, norm_in), (0, attend), (0, project),
            (1, norm_mid), (1, up), (1, gelu_both), (1, grad_b), (1, down),
            (2, grad_mid), (2, functools.partial(attend_back, 0)), (2, functools.partial(attend_back, 1)), (2, grad_a)]
    assert len(work) == POINTS
    progress = make_progress(count, POINTS, [
        (ring_p1, 0, 2, consume_p1), (ring_db, 1, 6, None), (ring_p2, 1, 7, consume_p2), (ring_da, 2, 11, consume_da)])

    x_in(0).start()
    enter(size)
    for ref in (dw_qkv, dw_out, dw_up, dw_down, dg_attn, dg_mlp):
        ref[...] = jnp.zeros_like(ref)

    def step(t):
        @pl.when(t + 1 < count)
        def _():
            x_in(t + 1).start()

        @pl.when(t < count)
        def _():
            d_in(t).start()
        for i, (lead, fn) in enumerate(work):
            s = t - lead

            @pl.when(jnp.logical_and(s >= 0, s < count))
            def _(fn=fn, s=s):
                fn(s)
            progress(t, i)

    loop(count + 3, step)
    for acc, out in ((dw_qkv, dw_qkv_out), (dw_out, dw_out_out), (dw_up, dw_up_out), (dw_down, dw_down_out)):
        out[...] = acc[...].astype(BF16)
    dg_attn_out[...] = jnp.sum(dg_attn[...], axis=0, keepdims=True)
    dg_mlp_out[...] = jnp.sum(dg_mlp[...], axis=0, keepdims=True)
    for s in range(count - SLOTS, count):
        out_copy(s).wait()
        dtok_copy(s).wait()


def ring_buffers(block_rows, hidden):
    return [
        pltpu.VMEM((SLOTS, BLOCKS, block_rows, hidden), BF16),
        pltpu.VMEM((SLOTS, HALF, block_rows, hidden), BF16),
        pltpu.VMEM((SLOTS, 2, block_rows, hidden), BF16),
        pltpu.VMEM((SLOTS, 2, PIECE, block_rows, hidden), BF16),
        pltpu.VMEM((SLOTS, BLOCKS, block_rows, hidden), BF16),
    ]


def ring_sems():
    return [pltpu.SemaphoreType.DMA((SLOTS, COPIES)), pltpu.SemaphoreType.DMA((SLOTS, COPIES))]


def run_kernel(kernel, ident, outs, out_vmem, args, in_vmem, scratch):
    def spec(in_vmem):
        return pl.BlockSpec(memory_space=pltpu.VMEM if in_vmem else pl.ANY)
    return pl.pallas_call(
        kernel,
        out_shape=[jax.ShapeDtypeStruct(s, t) for s, t in outs],
        in_specs=[spec(v) for v in in_vmem],
        out_specs=[spec(v) for v in out_vmem],
        scratch_shapes=scratch,
        compiler_params=pltpu.CompilerParams(collective_id=ident, has_side_effects=True, vmem_limit_bytes=VMEM_LIMIT),
        name=f'layer_part_{ident}',
    )(*args)


def solution(mesh):
    size = mesh.shape['model']
    dma = pltpu.SemaphoreType.DMA

    def device_step(tokens, seg_ids, d_out, gain_attn, gain_mlp, w_qkv, w_out, w_up, w_down):
        count, seq_len, hidden = tokens.shape
        heads, head_dim = w_qkv.shape[1], w_qkv.shape[3]
        width = heads * head_dim
        inner = w_up.shape[1]
        block_rows = seq_len // BLOCKS
        act = (count, BLOCKS, block_rows, hidden)
        one = (BLOCKS, block_rows, hidden)
        x = tokens.reshape(act)
        d = d_out.reshape(act)
        seg_row = seg_ids.reshape(count, 1, seq_len)
        seg_col = seg_ids.reshape(count, seq_len, 1)
        g_attn = gain_attn.astype(F32).reshape(1, hidden)
        g_mlp = gain_mlp.astype(F32).reshape(1, hidden)
        wqkv = w_qkv.transpose(0, 2, 1, 3).reshape(hidden, 3 * width)
        wout = w_out.reshape(width, hidden)

        outs = [(act, BF16), (act, BF16), ((hidden, 3 * width), BF16), ((width, hidden), BF16),
                ((hidden, inner), BF16), ((inner, hidden), BF16), ((1, hidden), F32), ((1, hidden), F32)]
        scratch = [pltpu.VMEM(shape, kind) for shape, kind in (
            ((X_SLOTS,) + one, BF16), ((D_SLOTS,) + one, BF16), ((SLOTS,) + one, BF16), ((A_SLOTS,) + one, BF16),
            ((A_SLOTS, seq_len, 4 * width), BF16), (one, BF16), ((seq_len, inner), F32), ((seq_len, inner), F32),
            ((seq_len, inner), BF16), ((seq_len, inner), BF16), ((seq_len, width), BF16),
            ((seq_len, seq_len), BF16), ((seq_len, seq_len), BF16), ((seq_len, 3 * width), BF16),
            ((hidden, 3 * width), F32), ((width, hidden), F32), ((hidden, inner), F32), ((inner, hidden), F32),
            ((8, hidden), F32), ((8, hidden), F32))]
        scratch += [dma((X_SLOTS,)), dma((D_SLOTS,)), dma((SLOTS,)), dma((SLOTS,))]
        for _ in range(4):
            scratch += ring_buffers(block_rows, hidden) + ring_sems()
        layer_out, d_tokens, dw_qkv, dw_out, d_w_up, d_w_down, dg_attn, dg_mlp = run_kernel(
            functools.partial(layer_kernel, size, head_dim), 1, outs, [False] * 2 + [True] * 6,
            [x, d, seg_row, seg_col, g_attn, g_mlp, wqkv, wout, w_up, w_down], [False] * 2 + [True] * 8, scratch)

        d_w_qkv = dw_qkv.reshape(hidden, 3, heads, head_dim).transpose(0, 2, 1, 3)
        return (layer_out.reshape(tokens.shape), d_tokens.reshape(tokens.shape), d_w_qkv,
                dw_out.reshape(w_out.shape), d_w_up, d_w_down, dg_attn.reshape(hidden), dg_mlp.reshape(hidden))

    in_specs = (P('data', None, None), P('data', None), P('data', None, None), P(), P(), P(None, 'model', None, None), P('model', None, None), P(None, 'model'), P('model', None))
    out_specs = (P('data', None, None), P('data', None, None), P('data', 'model', None, None), P(('data', 'model'), None, None), P('data', 'model'), P(('data', 'model'), None), P('data'), P('data'))
    return jax.shard_map(device_step, mesh=mesh, in_specs=in_specs, out_specs=out_specs, check_vma=False)
```

```python
import functools
import jax
import jax.numpy as jnp
from jax import lax
from jax.experimental import pallas as pl
from jax.experimental.pallas import tpu as pltpu
from jax.sharding import PartitionSpec as P

NORM_EPS = 1e-5
MESH = pl.DeviceIdType.MESH
F32 = jnp.float32
BF16 = jnp.bfloat16
SLOTS = 2
BLOCKS = 16
HALF = BLOCKS // 2
PIECE = 2
COPIES = 13
VMEM_LIMIT = 66 * 1000 * 1000


def mm(a, b):
    return lax.dot_general(a, b, (((1,), (0,)), ((), ())), preferred_element_type=F32)


def mt(a, b):
    return lax.dot_general(a, b, (((1,), (1,)), ((), ())), preferred_element_type=F32)


def tm(a, b):
    return lax.dot_general(a, b, (((0,), (0,)), ((), ())), preferred_element_type=F32)


def loop(count, body):
    def step(i, carry):
        body(i)
        return carry
    lax.fori_loop(0, count, step, 0)


class Gather:
    first, last = 0, 3

    def __init__(self, size, slots, view, send, recv):
        me = lax.axis_index('model')
        self.core = lax.rem(me, 2)
        self.chips = size // 2
        self.chip = me // 2
        self.right = lax.rem(me + 2, size)
        self.left = lax.rem(me + size - 2, size)
        self.partner = me + 1 - 2 * self.core
        self.slots, self.view, self.send, self.recv = slots, view, send, recv

    def at(self, slot, step, part=None):
        return self.view(slot, self.core, lax.rem(self.chip + step, self.chips), part)

    def remote(self, slot, n, src, dst, to):
        return pltpu.make_async_remote_copy(
            src_ref=src, dst_ref=dst, send_sem=self.send.at[slot, n], recv_sem=self.recv.at[slot, n],
            device_id={'model': to}, device_id_type=MESH)

    def copy(self, n, s):
        slot = lax.rem(s, self.slots)
        behind = self.chips - 1
        step, part, to = [(0, None, self.right), (0, None, self.left), (0, None, self.partner),
                          (behind, 0, self.right), (1, 1, self.left), (behind, None, self.partner),
                          (1, None, self.partner), (2, None, self.partner)][n]
        ref = self.at(slot, step, part)
        return self.remote(slot, n, ref, ref, to)

    def gather_stage(self, j, s):
        if j == 0:
            starts, waits = (0, 1, 2), ()
        elif j == 1:
            starts, waits = (3, 4, 5, 6), (0, 1)
        elif j == 2:
            starts, waits = (7,), (3, 4)
        else:
            starts, waits = (), (2, 5, 6, 7)
        for n in waits:
            self.copy(n, s).wait_recv()
        for n in starts:
            self.copy(n, s).start()
        if j == 3:
            for n in range(8):
                self.copy(n, s).wait_send()

    def stage(self, j, s):
        self.gather_stage(j, s)


class RingSum(Gather):
    last = 6

    def __init__(self, size, part, pair_in, relay_in, ring_in, whole, send, recv):
        self.part, self.pair_in, self.relay_in, self.ring_in, self.whole = part, pair_in, relay_in, ring_in, whole
        super().__init__(size, SLOTS, self.block_view, send, recv)

    def block_view(self, slot, core, chip, part):
        start = core * HALF + chip * PIECE
        if part is None:
            return self.whole.at[slot, pl.ds(start, PIECE)]
        return self.whole.at[slot, pl.ds(start + part, 1)]

    def base(self, step):
        return self.core * HALF + lax.rem(self.chip + step, self.chips) * PIECE

    def sum_copy(self, n, s):
        slot = lax.rem(s, SLOTS)
        part = self.part.at[slot]
        if n == 8:
            src, dst, to = part.at[pl.ds((1 - self.core) * HALF, HALF)], self.pair_in.at[slot], self.partner
        elif n == 9:
            src, dst, to = part.at[pl.ds(self.base(2), 1)], self.relay_in.at[slot, pl.ds(0, 1)], self.right
        elif n == 10:
            src, dst, to = part.at[pl.ds(self.base(2) + 1, 1)], self.relay_in.at[slot, pl.ds(1, 1)], self.left
        elif n == 11:
            src, dst, to = part.at[pl.ds(self.base(1), PIECE)], self.ring_in.at[slot, 0], self.right
        else:
            src, dst, to = part.at[pl.ds(self.base(self.chips - 1), PIECE)], self.ring_in.at[slot, 1], self.left
        return self.remote(slot, n, src, dst, to)

    def add(self, slot, block, others):
        total = self.part[slot, block].astype(F32)
        for ref in others:
            total = total + ref.astype(F32)
        return total.astype(BF16)

    def stage(self, j, s):
        slot = lax.rem(s, SLOTS)
        if j == 0:
            self.sum_copy(8, s).start()
        elif j == 1:
            self.sum_copy(8, s).wait_recv()

            def pair(i):
                at = lax.rem(lax.rem(self.chip + 2, self.chips) * PIECE + i, HALF)
                block = self.core * HALF + at
                self.part[slot, block] = self.add(slot, block, [self.pair_in[slot, at]])
            loop(HALF, pair)
            self.sum_copy(9, s).start()
            self.sum_copy(10, s).start()
        elif j == 2:
            self.sum_copy(9, s).wait_recv()
            self.sum_copy(10, s).wait_recv()
            first, second = self.base(1), self.base(self.chips - 1) + 1
            self.part[slot, first] = self.add(slot, first, [self.relay_in[slot, 0]])
            self.part[slot, second] = self.add(slot, second, [self.relay_in[slot, 1]])
            self.sum_copy(11, s).start()
            self.sum_copy(12, s).start()
        elif j == 3:
            self.sum_copy(11, s).wait_recv()
            self.sum_copy(12, s).wait_recv()
            for i in range(PIECE):
                block = self.base(0) + i
                self.whole[slot, block] = self.add(slot, block, [self.ring_in[slot, 0, i], self.ring_in[slot, 1, i]])
            self.gather_stage(0, s)
        else:
            self.gather_stage(j - 3, s)
            if j == self.last:
                for n in range(8, COPIES):
                    self.sum_copy(n, s).wait_send()


def enter(size):
    me = lax.axis_index('model')
    barrier = pltpu.get_barrier_semaphore()
    for other in (lax.rem(me + 2, size), lax.rem(me + size - 2, size), me + 1 - 2 * lax.rem(me, 2)):
        pl.semaphore_signal(barrier, inc=1, device_id={'model': other}, device_id_type=MESH)
    pl.semaphore_wait(barrier, 3)


def make_progress(points, sums):
    def progress(t, i):
        for ring, count, lead, start, offsets, consume in sums:
            for j in range(ring.last, 0, -1):
                ahead = start + offsets[j - 1] - i
                if ahead % points:
                    continue
                s = t - lead - ahead // points

                @pl.when(jnp.logical_and(s >= 0, s < count))
                def _(ring=ring, consume=consume, j=j, s=s):
                    ring.stage(j, s)
                    if j == ring.last and consume is not None:
                        consume(s)
    return progress


def norm_stats(x):
    mean = jnp.mean(x, axis=-1, keepdims=True)
    centered = x - mean
    var = jnp.mean(centered * centered, axis=-1, keepdims=True)
    inv = lax.rsqrt(var + NORM_EPS)
    return centered * inv, inv


def norm_back(x, gain, d_normed):
    unit, inv = norm_stats(x)
    d_unit = d_normed * gain
    mean_d = jnp.mean(d_unit, axis=-1, keepdims=True)
    mean_du = jnp.mean(d_unit * unit, axis=-1, keepdims=True)
    return inv * (d_unit - mean_d - unit * mean_du), d_normed * unit


def probs_of(q, k, seg_ref, s, row0, scale):
    keys = k.shape[0]
    seg_q = seg_ref[s, :, pl.ds(row0, Q_ROWS)]
    seg_q = jnp.broadcast_to(seg_q, (Q_ROWS, Q_ROWS)).T[:, :1]
    seg_k = seg_ref[s, :, :keys]
    scores = mt(q, k) * scale
    q_pos = row0 + lax.broadcasted_iota(jnp.int32, scores.shape, 0)
    k_pos = lax.broadcasted_iota(jnp.int32, scores.shape, 1)
    allowed = jnp.logical_and(seg_q == seg_k, q_pos >= k_pos)
    scores = jnp.where(allowed, scores, -1e30)
    e = jnp.exp(scores - jnp.max(scores, axis=-1, keepdims=True))
    return e * (1.0 / jnp.sum(e, axis=-1, keepdims=True))


def head_masks(width, head_dim):
    lane = lax.broadcasted_iota(jnp.int32, (1, width), 1)
    return [jnp.logical_and(lane >= h * head_dim, lane < (h + 1) * head_dim) for h in range(width // head_dim)]


Q_ROWS = 128

ORDER = ['A0', 'A1', 'A2', 'B0', 'B1', 'A3', 'B2', 'B3', 'B4', 'B5', 'B6', 'C0', 'C1', 'C2', 'B7', 'C3', 'C4', 'C5',
         'C6', 'C7', 'B8', 'C8']
STAGES = {'p1': [7, 18, 19], 'db': [1, 6, 12, 16, 22, 23], 'p2': [7, 13, 20, 31, 34, 35], 'da': [1, 7, 17, 25, 31, 32]}
STARTS = {'p1': 'A3', 'db': 'B5', 'p2': 'B6', 'da': 'C7'}


class Plan:
    def __init__(self):
        self.points = n = len(ORDER)
        self.pos = {tag: i for i, tag in enumerate(ORDER)}
        self.start = {ring: self.pos[tag] for ring, tag in STARTS.items()}
        self.lead = {'A': 0}
        self.lead['B'] = self.after('p1', 'B0')
        self.lead['C'] = self.after('db', 'C0')
        end = {ring: self.end(ring) // n for ring in STAGES}
        self.steps = max(end.values())
        self.x_slots = end['da'] + 2
        self.d_slots = end['da'] - self.lead['B'] + 1
        self.x1_slots = max(self.lead['C'], end['p2']) - end['p1'] + 1
        self.a_slots = self.lead['C'] + 1
        self.head_slots = 2 if STAGES['p1'][-1] < n else 3
        assert all(o[-1] < 2 * n for o in STAGES.values())
        assert self.lead['C'] * n + self.pos['C1'] < (self.lead['B'] + 2) * n + self.start['db']

    def ring_lead(self, ring):
        return self.lead[STARTS[ring][0]]

    def end(self, ring):
        return self.ring_lead(ring) * self.points + self.start[ring] + STAGES[ring][-1]

    def after(self, ring, tag):
        end = self.end(ring)
        return end // self.points + (0 if self.pos[tag] > end % self.points else 1)


def layer_kernel(size, head_dim, plan, *refs):
    (tok_hbm, dout_hbm, seg_in, gains, w_qkv_in, w_out, w_up, w_down,
     out_hbm, dtok_hbm, dw_qkv_out, dw_out_out, dw_up_out, dw_down_out, dg_out,
     x, d, x1, a, saved, heads, w_qkv, w_out_all, b, pre, d_hid, u, d_pre, d_heads, probs, d_scores, d_qkv,
     dw_qkv, dw_out, dw_up, dw_down, dg_attn, dg_mlp,
     seg, x_sem, d_sem, out_sem, dtok_sem, heads_send, heads_recv, wout_send, wout_recv) = refs[:47]
    ring_db, ring_p2, ring_da = [RingSum(size, *refs[47 + 7 * n:54 + 7 * n]) for n in range(3)]
    count = tok_hbm.shape[0]
    block_rows, hidden = x.shape[2], x.shape[3]
    rows = BLOCKS * block_rows
    half = rows // 2
    width = w_out.shape[0]
    scale = head_dim ** -0.5
    masks = head_masks(width, head_dim)
    me = lax.axis_index('model')
    my_lanes = pl.ds(pl.multiple_of(me * width, width), width)
    gain_attn, gain_mlp = gains.at[0:1], gains.at[1:2]

    def heads_view(slot, core, chip, part):
        lanes = pl.ds(pl.multiple_of((2 * chip + core) * width, width), width)
        span = pl.ds(0, rows) if part is None else pl.ds(part * half, half)
        return heads.at[slot, span, lanes]

    def wout_view(slot, core, chip, part):
        first = (2 * chip + core) * width
        if part is None:
            return w_out_all.at[pl.ds(pl.multiple_of(first, width), width)]
        size_half = width // 2
        return w_out_all.at[pl.ds(pl.multiple_of(first + part * size_half, size_half), size_half)]

    gather_p1 = Gather(size, plan.head_slots, heads_view, heads_send, heads_recv)
    gather_wout = Gather(size, 1, wout_view, wout_send, wout_recv)

    def x_in(s):
        slot = lax.rem(s, plan.x_slots)
        return pltpu.make_async_copy(tok_hbm.at[s], x.at[slot], x_sem.at[slot])

    def d_in(s):
        slot = lax.rem(s, plan.d_slots)
        return pltpu.make_async_copy(dout_hbm.at[s], d.at[slot], d_sem.at[slot])

    def out_copy(s):
        slot = lax.rem(s, SLOTS)
        return pltpu.make_async_copy(ring_p2.whole.at[slot], out_hbm.at[s], out_sem.at[slot])

    def dtok_copy(s):
        slot = lax.rem(s, SLOTS)
        return pltpu.make_async_copy(ring_da.whole.at[slot], dtok_hbm.at[s], dtok_sem.at[slot])

    def rows_sum(v):
        return jnp.sum(v.reshape(v.shape[0] // 8, 8, hidden), axis=0)

    def consume_p1(s):
        x_slot, x1_slot, h_slot = lax.rem(s, plan.x_slots), lax.rem(s, plan.x1_slots), lax.rem(s, plan.head_slots)
        for h in range(2):
            blocks = slice(h * HALF, (h + 1) * HALF)
            proj = mm(heads[h_slot, h * half:(h + 1) * half], w_out_all[...]).astype(BF16).reshape(HALF, block_rows, hidden)
            x1[x1_slot, blocks] = (x[x_slot, blocks].astype(F32) + proj.astype(F32)).astype(BF16)

    def consume_p2(s):
        slot, x1_slot = lax.rem(s, SLOTS), lax.rem(s, plan.x1_slots)

        def block(r):
            ring_p2.whole[slot, r] = (x1[x1_slot, r].astype(F32) + ring_p2.whole[slot, r].astype(F32)).astype(BF16)
        loop(BLOCKS, block)
        out_copy(s).start()

    def consume_da(s):
        slot, x_slot, d_slot = lax.rem(s, SLOTS), lax.rem(s, plan.x_slots), lax.rem(s, plan.d_slots)

        def block(r):
            dx, dg = norm_back(x[x_slot, r].astype(F32), gain_attn[...], ring_da.whole[slot, r].astype(F32))
            dg_attn[...] += rows_sum(dg)
            ring_da.whole[slot, r] = (d[d_slot, r].astype(F32) + dx).astype(BF16)
        loop(BLOCKS, block)
        dtok_copy(s).start()

    def store_part(ring, slot, h, value):
        ring.part[slot, h * HALF:(h + 1) * HALF] = value.astype(BF16).reshape(HALF, block_rows, hidden)

    def norm_in(h, s):
        x_slot, slot = lax.rem(s, plan.x_slots), lax.rem(s, plan.a_slots)
        if h == 0:
            x_in(s).wait()

        def block(i):
            r = h * HALF + i
            unit, _ = norm_stats(x[x_slot, r].astype(F32))
            a[slot, r] = (unit * gain_attn[...]).astype(BF16)
        loop(HALF, block)
        if h == 1:
            saved[slot, :, :3 * width] = mt(a[slot].reshape(rows, hidden), w_qkv[...]).astype(BF16)

    def attend(h, s):
        slot, h_slot = lax.rem(s, plan.a_slots), lax.rem(s, plan.head_slots)
        keys = (h + 1) * half

        def q_block(i):
            row0 = pl.multiple_of(h * half + i * Q_ROWS, Q_ROWS)
            part_rows = pl.ds(row0, Q_ROWS)
            q = saved[slot, part_rows, 0:width]
            k = saved[slot, :keys, width:2 * width]
            v = saved[slot, :keys, 2 * width:3 * width]
            out = None
            for mask in masks:
                p = probs_of(jnp.where(mask, q, 0).astype(BF16), k, seg, s, row0, scale)
                head = mm(p.astype(BF16), v)
                out = head if out is None else jnp.where(mask, head, out)
            out = out.astype(BF16)
            saved[slot, part_rows, 3 * width:4 * width] = out
            heads[h_slot, part_rows, my_lanes] = out
        loop(half // Q_ROWS, q_block)
        if h == 1:
            gather_p1.stage(0, s)

    def norm_mid(h, s):
        x1_slot = lax.rem(s, plan.x1_slots)

        def block(i):
            r = h * HALF + i
            unit, _ = norm_stats(x1[x1_slot, r].astype(F32))
            b[r] = (unit * gain_mlp[...]).astype(BF16)
        loop(HALF, block)

    def up(s):
        pre[...] = mm(b[...].reshape(rows, hidden), w_up[...])

    def gelu_both(h, s):
        if h == 0:
            d_in(s).wait()
            d_hid[...] = mt(d[lax.rem(s, plan.d_slots)].reshape(rows, hidden), w_down[...]).astype(BF16)

        def block(i):
            part_rows = pl.ds(pl.multiple_of(h * half + i * block_rows, block_rows), block_rows)
            v = pre[part_rows]
            v2 = v * v
            c = 0.7978845608028654
            th = jnp.tanh(c * (v + 0.044715 * (v * v2)))
            u[part_rows] = (0.5 * v * (1.0 + th)).astype(BF16)
            slope = 0.5 * (1.0 + th) + 0.5 * v * (1.0 - th * th) * (c * (1.0 + 3.0 * 0.044715 * v2))
            d_pre[part_rows] = (d_hid[part_rows].astype(F32) * slope).astype(BF16)
        loop(HALF, block)

    def grad_b(s):
        for h in range(2):
            store_part(ring_db, lax.rem(s, SLOTS), h, mt(d_pre[h * half:(h + 1) * half], w_up[...]))
        ring_db.stage(0, s)

    def down(s):
        @pl.when(s >= SLOTS)
        def _():
            out_copy(s - SLOTS).wait()
        for h in range(2):
            store_part(ring_p2, lax.rem(s, SLOTS), h, mm(u[h * half:(h + 1) * half], w_down[...]))
        ring_p2.stage(0, s)

    def grad_up(s):
        dw_up[...] += tm(b[...].reshape(rows, hidden), d_pre[...])

    def grad_down(s):
        dw_down[...] += tm(u[...], d[lax.rem(s, plan.d_slots)].reshape(rows, hidden))

    def grad_mid(h, s):
        slot, x1_slot, d_slot = lax.rem(s, SLOTS), lax.rem(s, plan.x1_slots), lax.rem(s, plan.d_slots)

        def block(i):
            r = h * HALF + i
            dx, dg = norm_back(x1[x1_slot, r].astype(F32), gain_mlp[...], ring_db.whole[slot, r].astype(F32))
            dg_mlp[...] += rows_sum(dg)
            d[d_slot, r] = (d[d_slot, r].astype(F32) + dx).astype(BF16)
        loop(HALF, block)

    def grad_heads(s):
        d_rows = d[lax.rem(s, plan.d_slots)].reshape(rows, hidden)
        d_heads[...] = mt(d_rows, w_out[...]).astype(BF16)
        dw_out[...] += tm(saved[lax.rem(s, plan.a_slots), :, 3 * width:4 * width], d_rows)

    def attend_back(head, s):
        mask = masks[head]
        slot = lax.rem(s, plan.a_slots)
        for h in range(2):
            keys = (h + 1) * half

            def q_block(i):
                row0 = pl.multiple_of(h * half + i * Q_ROWS, Q_ROWS)
                part_rows = pl.ds(row0, Q_ROWS)
                q = jnp.where(mask, saved[slot, part_rows, 0:width], 0).astype(BF16)
                d_head = jnp.where(mask, d_heads[part_rows], 0).astype(BF16)
                p = probs_of(q, saved[slot, :keys, width:2 * width], seg, s, row0, scale)
                d_p = mt(d_head, saved[slot, :keys, 2 * width:3 * width])
                row_dot = jnp.sum(d_p * p, axis=-1, keepdims=True)
                probs[part_rows, :keys] = p.astype(BF16)
                d_scores[part_rows, :keys] = (p * (d_p - row_dot) * scale).astype(BF16)
            loop(half // Q_ROWS, q_block)

    def head_grads(head, s):
        mask = masks[head]
        slot = lax.rem(s, plan.a_slots)
        d_q = mm(d_scores[...], saved[slot, :, width:2 * width]).astype(BF16)
        d_k = tm(d_scores[...], saved[slot, :, 0:width]).astype(BF16)
        d_v = tm(probs[...], d_heads[...]).astype(BF16)
        for j, value in enumerate((d_q, d_k, d_v)):
            cols = slice(j * width, (j + 1) * width)
            d_qkv[:, cols] = value if head == 0 else jnp.where(mask, value, d_qkv[:, cols])

    def grad_a(s):
        @pl.when(s >= SLOTS)
        def _():
            dtok_copy(s - SLOTS).wait()
        for h in range(2):
            store_part(ring_da, lax.rem(s, SLOTS), h, mm(d_qkv[h * half:(h + 1) * half], w_qkv[...]))
        ring_da.stage(0, s)

    def grad_qkv(s):
        dw_qkv[...] += tm(d_qkv[...], a[lax.rem(s, plan.a_slots)].reshape(rows, hidden))

    def with_h(fn, h):
        return functools.partial(fn, h)

    work = {'A': [with_h(norm_in, 0), with_h(norm_in, 1), with_h(attend, 0), with_h(attend, 1)],
            'B': [with_h(norm_mid, 0), with_h(norm_mid, 1), up, with_h(gelu_both, 0), with_h(gelu_both, 1), grad_b, down,
                  grad_up, grad_down],
            'C': [with_h(grad_mid, 0), with_h(grad_mid, 1), grad_heads, with_h(attend_back, 0), with_h(head_grads, 0),
                  with_h(attend_back, 1), with_h(head_grads, 1), grad_a, grad_qkv]}
    assert sum(len(v) for v in work.values()) == plan.points
    first = plan.start['p1']
    progress = make_progress(plan.points, [(gather_wout, 1, 0, 0, [first + 1, first + 4, first + 7], None)] + [
        (ring, count, plan.ring_lead(name), plan.start[name], STAGES[name], consume) for name, ring, consume in (
            ('p1', gather_p1, consume_p1), ('db', ring_db, None), ('p2', ring_p2, consume_p2), ('da', ring_da, consume_da))])

    x_in(0).start()
    for s in range(count):
        seg[s] = seg_in[s:s + 1]
    w_out_all[my_rows(me, width)] = w_out[...]
    enter(size)
    gather_wout.stage(0, 0)
    for n in range(w_qkv_in.shape[0]):
        for j in range(3):
            at = (j * w_qkv_in.shape[0] + n) * head_dim
            w_qkv[at:at + head_dim] = w_qkv_in[n, j]
    for ref in (dw_qkv, dw_out, dw_up, dw_down, dg_attn, dg_mlp, probs, d_scores):
        ref[...] = jnp.zeros_like(ref)

    def step(t):
        @pl.when(t + 1 < count)
        def _():
            x_in(t + 1).start()
        s_mid = t - plan.lead['B']

        @pl.when(jnp.logical_and(s_mid >= 0, s_mid < count))
        def _():
            d_in(s_mid).start()
        for i, tag in enumerate(ORDER):
            s = t - plan.lead[tag[0]]

            @pl.when(jnp.logical_and(s >= 0, s < count))
            def _(fn=work[tag[0]][int(tag[1:])], s=s):
                fn(s)
            progress(t, i)

    loop(count + plan.steps, step)
    for acc, out in ((dw_out, dw_out_out), (dw_up, dw_up_out), (dw_down, dw_down_out)):
        out[...] = acc[...].astype(BF16)
    for n in range(w_qkv_in.shape[0]):
        for j in range(3):
            at = (j * w_qkv_in.shape[0] + n) * head_dim
            dw_qkv_out[n, j] = dw_qkv[at:at + head_dim].astype(BF16)
    dg_out[0:1] = jnp.sum(dg_attn[...], axis=0, keepdims=True)
    dg_out[1:2] = jnp.sum(dg_mlp[...], axis=0, keepdims=True)
    for s in range(count - SLOTS, count):
        out_copy(s).wait()
        dtok_copy(s).wait()


def my_rows(me, width):
    return pl.ds(pl.multiple_of(me * width, width), width)


def publish_kernel(count, *refs):
    n = len(refs) // 5
    ins, outs, held, in_sems, out_sems = (refs[k * n:(k + 1) * n] for k in range(5))

    def moves(i):
        if i >= count:
            yield (pltpu.make_async_copy(ins[i], held[i], in_sems[i].at[0]),
                   pltpu.make_async_copy(held[i], outs[i], out_sems[i].at[0]))
            return
        for r in range(ins[i].shape[0]):
            yield (pltpu.make_async_copy(ins[i].at[r], held[i].at[r], in_sems[i].at[r]),
                   pltpu.make_async_copy(held[i].at[r], outs[i].at[r], out_sems[i].at[r]))
    pairs = [pair for i in range(n) for pair in moves(i)]
    for into, _ in pairs:
        into.start()
    for into, out in pairs:
        into.wait()
        out.start()
    for _, out in pairs:
        out.wait()


def publish(values, split):
    sems = [pltpu.SemaphoreType.DMA((v.shape[0] if i < split else 1,)) for i, v in enumerate(values)]
    return pl.pallas_call(
        functools.partial(publish_kernel, split),
        out_shape=[jax.ShapeDtypeStruct(v.shape, v.dtype) for v in values],
        in_specs=[pl.BlockSpec(memory_space=pl.ANY)] * len(values),
        out_specs=[pl.BlockSpec(memory_space=pl.ANY)] * len(values),
        scratch_shapes=[pltpu.VMEM(v.shape, v.dtype) for v in values] + sems + sems,
        compiler_params=pltpu.CompilerParams(vmem_limit_bytes=VMEM_LIMIT),
        name='publish',
    )(*values)


def ring_buffers(block_rows, hidden):
    return [
        pltpu.VMEM((SLOTS, BLOCKS, block_rows, hidden), BF16),
        pltpu.VMEM((SLOTS, HALF, block_rows, hidden), BF16),
        pltpu.VMEM((SLOTS, 2, block_rows, hidden), BF16),
        pltpu.VMEM((SLOTS, 2, PIECE, block_rows, hidden), BF16),
        pltpu.VMEM((SLOTS, BLOCKS, block_rows, hidden), BF16),
    ]


def ring_sems():
    return [pltpu.SemaphoreType.DMA((SLOTS, COPIES)), pltpu.SemaphoreType.DMA((SLOTS, COPIES))]


def run_kernel(kernel, ident, outs, out_vmem, args, in_vmem, scratch):
    def spec(in_vmem):
        return pl.BlockSpec(memory_space=pltpu.VMEM if in_vmem else pl.ANY)
    return pl.pallas_call(
        kernel,
        out_shape=[jax.ShapeDtypeStruct(s, t) for s, t in outs],
        in_specs=[spec(v) for v in in_vmem],
        out_specs=[spec(v) for v in out_vmem],
        scratch_shapes=scratch,
        compiler_params=pltpu.CompilerParams(collective_id=ident, has_side_effects=True, vmem_limit_bytes=VMEM_LIMIT),
        name=f'layer_part_{ident}',
    )(*args)


def solution(mesh):
    size = mesh.shape['model']
    dma = pltpu.SemaphoreType.DMA

    def device_step(tokens, seg_ids, d_out, gain_attn, gain_mlp, w_qkv, w_out, w_up, w_down):
        count, seq_len, hidden = tokens.shape
        heads, head_dim = w_qkv.shape[1], w_qkv.shape[3]
        width = heads * head_dim
        inner = w_up.shape[1]
        block_rows = seq_len // BLOCKS
        act = (count, BLOCKS, block_rows, hidden)
        one = (BLOCKS, block_rows, hidden)
        x = tokens.reshape(act)
        d = d_out.reshape(act)
        gains = jnp.stack([gain_attn, gain_mlp]).astype(F32)
        wqkv = w_qkv.transpose(1, 2, 3, 0)
        wout = w_out.reshape(width, hidden)
        plan = Plan()

        outs = [(act, BF16), (act, BF16), (wqkv.shape, BF16), ((width, hidden), BF16),
                ((hidden, inner), BF16), ((inner, hidden), BF16), ((2, hidden), F32)]
        scratch = [pltpu.VMEM(shape, kind) for shape, kind in (
            ((plan.x_slots,) + one, BF16), ((plan.d_slots,) + one, BF16), ((plan.x1_slots,) + one, BF16),
            ((plan.a_slots,) + one, BF16), ((plan.a_slots, seq_len, 4 * width), BF16),
            ((plan.head_slots, seq_len, size * width), BF16), ((3 * width, hidden), BF16), ((size * width, hidden), BF16),
            (one, BF16), ((seq_len, inner), F32), ((seq_len, inner), BF16),
            ((seq_len, inner), BF16), ((seq_len, inner), BF16), ((seq_len, width), BF16),
            ((seq_len, seq_len), BF16), ((seq_len, seq_len), BF16), ((seq_len, 3 * width), BF16),
            ((3 * width, hidden), F32), ((width, hidden), F32), ((hidden, inner), F32), ((inner, hidden), F32),
            ((8, hidden), F32), ((8, hidden), F32), ((count, 1, seq_len), jnp.int32))]
        scratch += [dma((plan.x_slots,)), dma((plan.d_slots,)), dma((SLOTS,)), dma((SLOTS,))]
        scratch += [dma((plan.head_slots, 8))] * 2 + [dma((1, 8))] * 2
        for _ in range(3):
            scratch += ring_buffers(block_rows, hidden) + ring_sems()
        results = run_kernel(
            functools.partial(layer_kernel, size, head_dim, plan), 1, outs, [False] * 2 + [True] * 5,
            [x, d, seg_ids, gains, wqkv, wout, w_up, w_down], [False] * 2 + [True] * 6, scratch)
        layer_out, d_tokens, dw_qkv, dw_out, d_w_up, d_w_down, dg = publish(results, 2)

        return (layer_out.reshape(tokens.shape), d_tokens.reshape(tokens.shape), dw_qkv.transpose(3, 0, 1, 2),
                dw_out.reshape(w_out.shape), d_w_up, d_w_down, dg[0], dg[1])

    in_specs = (P('data', None, None), P('data', None), P('data', None, None), P(), P(), P(None, 'model', None, None), P('model', None, None), P(None, 'model'), P('model', None))
    out_specs = (P('data', None, None), P('data', None, None), P('data', 'model', None, None), P(('data', 'model'), None, None), P('data', 'model'), P(('data', 'model'), None), P('data'), P('data'))
    return jax.shard_map(device_step, mesh=mesh, in_specs=in_specs, out_specs=out_specs, check_vma=False)
```

```python
import functools
import jax
import jax.numpy as jnp
from jax import lax
from jax.experimental import pallas as pl
from jax.experimental.pallas import tpu as pltpu
from jax.sharding import PartitionSpec as P

NORM_EPS = 1e-5
MESH = pl.DeviceIdType.MESH
F32 = jnp.float32
BF16 = jnp.bfloat16
SLOTS = 2
BLOCKS = 16
HALF = BLOCKS // 2
PIECE = 2
COPIES = 13
VMEM_LIMIT = 66 * 1000 * 1000


def mm(a, b):
    return lax.dot_general(a, b, (((1,), (0,)), ((), ())), preferred_element_type=F32)


def mt(a, b):
    return lax.dot_general(a, b, (((1,), (1,)), ((), ())), preferred_element_type=F32)


def tm(a, b):
    return lax.dot_general(a, b, (((0,), (0,)), ((), ())), preferred_element_type=F32)


def loop(count, body):
    def step(i, carry):
        body(i)
        return carry
    lax.fori_loop(0, count, step, 0)


class Gather:
    first, last = 0, 3

    def __init__(self, size, slots, view, send, recv):
        me = lax.axis_index('model')
        self.core = lax.rem(me, 2)
        self.chips = size // 2
        self.chip = me // 2
        self.right = lax.rem(me + 2, size)
        self.left = lax.rem(me + size - 2, size)
        self.partner = me + 1 - 2 * self.core
        self.slots, self.view, self.send, self.recv = slots, view, send, recv

    def at(self, slot, step, part=None):
        return self.view(slot, self.core, lax.rem(self.chip + step, self.chips), part)

    def remote(self, slot, n, src, dst, to):
        return pltpu.make_async_remote_copy(
            src_ref=src, dst_ref=dst, send_sem=self.send.at[slot, n], recv_sem=self.recv.at[slot, n],
            device_id={'model': to}, device_id_type=MESH)

    def copy(self, n, s):
        slot = lax.rem(s, self.slots)
        behind = self.chips - 1
        step, part, to = [(0, None, self.right), (0, None, self.left), (0, None, self.partner),
                          (behind, 0, self.right), (1, 1, self.left), (behind, None, self.partner),
                          (1, None, self.partner), (2, None, self.partner)][n]
        ref = self.at(slot, step, part)
        return self.remote(slot, n, ref, ref, to)

    def gather_stage(self, j, s):
        if j == 0:
            starts, waits = (0, 1, 2), ()
        elif j == 1:
            starts, waits = (3, 4, 5, 6), (0, 1)
        elif j == 2:
            starts, waits = (7,), (3, 4)
        else:
            starts, waits = (), (2, 5, 6, 7)
        for n in waits:
            self.copy(n, s).wait_recv()
        for n in starts:
            self.copy(n, s).start()
        if j == 3:
            for n in range(8):
                self.copy(n, s).wait_send()

    def stage(self, j, s):
        self.gather_stage(j, s)


class RingSum(Gather):
    last = 6

    def __init__(self, size, part, pair_in, relay_in, ring_in, whole, send, recv):
        self.part, self.pair_in, self.relay_in, self.ring_in, self.whole = part, pair_in, relay_in, ring_in, whole
        super().__init__(size, SLOTS, self.block_view, send, recv)

    def block_view(self, slot, core, chip, part):
        start = core * HALF + chip * PIECE
        if part is None:
            return self.whole.at[slot, pl.ds(start, PIECE)]
        return self.whole.at[slot, pl.ds(start + part, 1)]

    def base(self, step):
        return self.core * HALF + lax.rem(self.chip + step, self.chips) * PIECE

    def sum_copy(self, n, s):
        slot = lax.rem(s, SLOTS)
        part = self.part.at[slot]
        if n == 8:
            src, dst, to = part.at[pl.ds((1 - self.core) * HALF, HALF)], self.pair_in.at[slot], self.partner
        elif n == 9:
            src, dst, to = part.at[pl.ds(self.base(2), 1)], self.relay_in.at[slot, pl.ds(0, 1)], self.right
        elif n == 10:
            src, dst, to = part.at[pl.ds(self.base(2) + 1, 1)], self.relay_in.at[slot, pl.ds(1, 1)], self.left
        elif n == 11:
            src, dst, to = part.at[pl.ds(self.base(1), PIECE)], self.ring_in.at[slot, 0], self.right
        else:
            src, dst, to = part.at[pl.ds(self.base(self.chips - 1), PIECE)], self.ring_in.at[slot, 1], self.left
        return self.remote(slot, n, src, dst, to)

    def add(self, slot, block, others):
        total = self.part[slot, block].astype(F32)
        for ref in others:
            total = total + ref.astype(F32)
        return total.astype(BF16)

    def stage(self, j, s):
        slot = lax.rem(s, SLOTS)
        if j == 0:
            self.sum_copy(8, s).start()
        elif j == 1:
            self.sum_copy(8, s).wait_recv()

            def pair(i):
                at = lax.rem(lax.rem(self.chip + 2, self.chips) * PIECE + i, HALF)
                block = self.core * HALF + at
                self.part[slot, block] = self.add(slot, block, [self.pair_in[slot, at]])
            loop(HALF, pair)
            self.sum_copy(9, s).start()
            self.sum_copy(10, s).start()
        elif j == 2:
            self.sum_copy(9, s).wait_recv()
            self.sum_copy(10, s).wait_recv()
            first, second = self.base(1), self.base(self.chips - 1) + 1
            self.part[slot, first] = self.add(slot, first, [self.relay_in[slot, 0]])
            self.part[slot, second] = self.add(slot, second, [self.relay_in[slot, 1]])
            self.sum_copy(11, s).start()
            self.sum_copy(12, s).start()
        elif j == 3:
            self.sum_copy(11, s).wait_recv()
            self.sum_copy(12, s).wait_recv()
            for i in range(PIECE):
                block = self.base(0) + i
                self.whole[slot, block] = self.add(slot, block, [self.ring_in[slot, 0, i], self.ring_in[slot, 1, i]])
            self.gather_stage(0, s)
        else:
            self.gather_stage(j - 3, s)
            if j == self.last:
                for n in range(8, COPIES):
                    self.sum_copy(n, s).wait_send()


def enter(size):
    me = lax.axis_index('model')
    barrier = pltpu.get_barrier_semaphore()
    for other in (lax.rem(me + 2, size), lax.rem(me + size - 2, size), me + 1 - 2 * lax.rem(me, 2)):
        pl.semaphore_signal(barrier, inc=1, device_id={'model': other}, device_id_type=MESH)
    pl.semaphore_wait(barrier, 3)


def make_progress(points, sums):
    def progress(t, i):
        for ring, count, lead, start, offsets, consume in sums:
            for j in range(ring.last, 0, -1):
                ahead = start + offsets[j - 1] - i
                if ahead % points:
                    continue
                s = t - lead - ahead // points

                @pl.when(jnp.logical_and(s >= 0, s < count))
                def _(ring=ring, consume=consume, j=j, s=s):
                    ring.stage(j, s)
                    if j == ring.last and consume is not None:
                        consume(s)
    return progress


def norm_stats(x):
    mean = jnp.mean(x, axis=-1, keepdims=True)
    centered = x - mean
    var = jnp.mean(centered * centered, axis=-1, keepdims=True)
    inv = lax.rsqrt(var + NORM_EPS)
    return centered * inv, inv


def norm_back(x, gain, d_normed):
    unit, inv = norm_stats(x)
    d_unit = d_normed * gain
    mean_d = jnp.mean(d_unit, axis=-1, keepdims=True)
    mean_du = jnp.mean(d_unit * unit, axis=-1, keepdims=True)
    return inv * (d_unit - mean_d - unit * mean_du), d_normed * unit


def probs_of(q, k, seg_ref, s, row0, scale):
    keys = k.shape[0]
    seg_q = seg_ref[s, :, pl.ds(row0, Q_ROWS)]
    seg_q = jnp.broadcast_to(seg_q, (Q_ROWS, Q_ROWS)).T[:, :1]
    seg_k = seg_ref[s, :, :keys]
    scores = mt(q, k) * scale
    q_pos = row0 + lax.broadcasted_iota(jnp.int32, scores.shape, 0)
    k_pos = lax.broadcasted_iota(jnp.int32, scores.shape, 1)
    allowed = jnp.logical_and(seg_q == seg_k, q_pos >= k_pos)
    scores = jnp.where(allowed, scores, -1e30)
    e = jnp.exp(scores - jnp.max(scores, axis=-1, keepdims=True))
    return e * (1.0 / jnp.sum(e, axis=-1, keepdims=True))


def head_masks(width, head_dim):
    lane = lax.broadcasted_iota(jnp.int32, (1, width), 1)
    return [jnp.logical_and(lane >= h * head_dim, lane < (h + 1) * head_dim) for h in range(width // head_dim)]


Q_ROWS = 128

ORDER = ['A0', 'A1', 'B0', 'B1', 'B2', 'B3', 'B4', 'B5', 'B6', 'B7', 'A2', 'B8', 'C0', 'A3', 'C1', 'C2', 'C3', 'C4',
         'C5', 'C6', 'C7', 'C8']
STAGES = {'p1': [14, 25, 32], 'mlp': [1, 4, 13, 22, 24, 25], 'da': [3, 10, 13, 21, 26, 34]}
STARTS = {'p1': 'A3', 'mlp': 'B6', 'da': 'C7'}


class Plan:
    def __init__(self):
        self.points = n = len(ORDER)
        self.pos = {tag: i for i, tag in enumerate(ORDER)}
        self.start = {ring: self.pos[tag] for ring, tag in STARTS.items()}
        self.lead = {'A': 0}
        self.lead['B'] = self.after('p1', 'B0')
        self.lead['C'] = self.after('mlp', 'C0')
        end = {ring: self.end(ring) // n for ring in STAGES}
        self.steps = max(end.values())
        self.x_slots = end['da'] + 2
        self.d_slots = end['da'] - self.lead['B'] + 1
        self.x1_slots = max(self.lead['C'], end['mlp']) - end['p1'] + 1
        self.a_slots = self.lead['C'] + 1
        self.head_slots = 2 if STAGES['p1'][-1] < n else 3
        assert all(o[-1] < 2 * n for o in STAGES.values())
        assert self.lead['C'] * n + self.pos['C1'] < (self.lead['B'] + 2) * n + self.start['mlp']

    def ring_lead(self, ring):
        return self.lead[STARTS[ring][0]]

    def end(self, ring):
        return self.ring_lead(ring) * self.points + self.start[ring] + STAGES[ring][-1]

    def after(self, ring, tag):
        end = self.end(ring)
        return end // self.points + (0 if self.pos[tag] > end % self.points else 1)


def layer_kernel(size, head_dim, plan, *refs):
    (tok_hbm, dout_hbm, seg_in, gains, w_qkv_in, w_out, w_up, w_down,
     out_hbm, dtok_hbm, dw_qkv_out, dw_out_out, dw_up_out, dw_down_out, dg_out,
     x, d, x1, a, saved, heads, w_qkv, w_out_all, b, pre, d_hid, u, d_pre, d_heads, probs, d_scores, d_qkv,
     dw_qkv, dw_out, dw_up, dw_down, dg_attn, dg_mlp,
     seg, x_sem, d_sem, out_sem, dtok_sem, heads_send, heads_recv, wout_send, wout_recv) = refs[:47]
    ring_mlp, ring_da = [RingSum(size, *refs[47 + 7 * n:54 + 7 * n]) for n in range(2)]
    count = tok_hbm.shape[0]
    block_rows, hidden = x.shape[2], x.shape[3]
    rows = BLOCKS * block_rows
    half = rows // 2
    width = w_out.shape[0]
    scale = head_dim ** -0.5
    masks = head_masks(width, head_dim)
    me = lax.axis_index('model')
    db_rows, p2_rows = slice(0, block_rows), slice(block_rows, 2 * block_rows)
    my_lanes = pl.ds(pl.multiple_of(me * width, width), width)
    gain_attn, gain_mlp = gains.at[0:1], gains.at[1:2]

    def heads_view(slot, core, chip, part):
        lanes = pl.ds(pl.multiple_of((2 * chip + core) * width, width), width)
        span = pl.ds(0, rows) if part is None else pl.ds(part * half, half)
        return heads.at[slot, span, lanes]

    def wout_view(slot, core, chip, part):
        first = (2 * chip + core) * width
        if part is None:
            return w_out_all.at[pl.ds(pl.multiple_of(first, width), width)]
        size_half = width // 2
        return w_out_all.at[pl.ds(pl.multiple_of(first + part * size_half, size_half), size_half)]

    gather_p1 = Gather(size, plan.head_slots, heads_view, heads_send, heads_recv)
    gather_wout = Gather(size, 1, wout_view, wout_send, wout_recv)

    def x_in(s):
        slot = lax.rem(s, plan.x_slots)
        return pltpu.make_async_copy(tok_hbm.at[s], x.at[slot], x_sem.at[slot])

    def d_in(s):
        slot = lax.rem(s, plan.d_slots)
        return pltpu.make_async_copy(dout_hbm.at[s], d.at[slot], d_sem.at[slot])

    def out_copy(s):
        slot = lax.rem(s, SLOTS)
        return pltpu.make_async_copy(ring_mlp.whole.at[slot, :, pl.ds(block_rows, block_rows)], out_hbm.at[s], out_sem.at[slot])

    def dtok_copy(s):
        slot = lax.rem(s, SLOTS)
        return pltpu.make_async_copy(ring_da.whole.at[slot], dtok_hbm.at[s], dtok_sem.at[slot])

    def rows_sum(v):
        return jnp.sum(v.reshape(v.shape[0] // 8, 8, hidden), axis=0)

    def consume_p1(s):
        x_slot, x1_slot, h_slot = lax.rem(s, plan.x_slots), lax.rem(s, plan.x1_slots), lax.rem(s, plan.head_slots)
        for h in range(2):
            blocks = slice(h * HALF, (h + 1) * HALF)
            proj = mm(heads[h_slot, h * half:(h + 1) * half], w_out_all[...]).astype(BF16).reshape(HALF, block_rows, hidden)
            x1[x1_slot, blocks] = (x[x_slot, blocks].astype(F32) + proj.astype(F32)).astype(BF16)

    def consume_p2(s):
        slot, x1_slot = lax.rem(s, SLOTS), lax.rem(s, plan.x1_slots)

        def block(r):
            total = x1[x1_slot, r].astype(F32) + ring_mlp.whole[slot, r, p2_rows].astype(F32)
            ring_mlp.whole[slot, r, p2_rows] = total.astype(BF16)
        loop(BLOCKS, block)
        out_copy(s).start()

    def consume_da(s):
        slot, x_slot, d_slot = lax.rem(s, SLOTS), lax.rem(s, plan.x_slots), lax.rem(s, plan.d_slots)

        def block(r):
            dx, dg = norm_back(x[x_slot, r].astype(F32), gain_attn[...], ring_da.whole[slot, r].astype(F32))
            dg_attn[...] += rows_sum(dg)
            ring_da.whole[slot, r] = (d[d_slot, r].astype(F32) + dx).astype(BF16)
        loop(BLOCKS, block)
        dtok_copy(s).start()

    def store_part(ring, slot, h, value, at=slice(None)):
        ring.part[slot, h * HALF:(h + 1) * HALF, at] = value.astype(BF16).reshape(HALF, block_rows, hidden)

    def norm_in(h, s):
        x_slot, slot = lax.rem(s, plan.x_slots), lax.rem(s, plan.a_slots)
        if h == 0:
            x_in(s).wait()

        def block(i):
            r = h * HALF + i
            unit, _ = norm_stats(x[x_slot, r].astype(F32))
            a[slot, r] = (unit * gain_attn[...]).astype(BF16)
        loop(HALF, block)
        if h == 1:
            saved[slot, :, :3 * width] = mt(a[slot].reshape(rows, hidden), w_qkv[...]).astype(BF16)

    def attend(h, s):
        slot, h_slot = lax.rem(s, plan.a_slots), lax.rem(s, plan.head_slots)
        keys = (h + 1) * half

        def q_block(i):
            row0 = pl.multiple_of(h * half + i * Q_ROWS, Q_ROWS)
            part_rows = pl.ds(row0, Q_ROWS)
            q = saved[slot, part_rows, 0:width]
            k = saved[slot, :keys, width:2 * width]
            v = saved[slot, :keys, 2 * width:3 * width]
            out = None
            for mask in masks:
                p = probs_of(jnp.where(mask, q, 0).astype(BF16), k, seg, s, row0, scale)
                head = mm(p.astype(BF16), v)
                out = head if out is None else jnp.where(mask, head, out)
            out = out.astype(BF16)
            saved[slot, part_rows, 3 * width:4 * width] = out
            heads[h_slot, part_rows, my_lanes] = out
        loop(half // Q_ROWS, q_block)
        if h == 1:
            gather_p1.stage(0, s)

    def norm_mid(h, s):
        x1_slot = lax.rem(s, plan.x1_slots)

        def block(i):
            r = h * HALF + i
            unit, _ = norm_stats(x1[x1_slot, r].astype(F32))
            b[r] = (unit * gain_mlp[...]).astype(BF16)
        loop(HALF, block)

    def up(s):
        pre[...] = mm(b[...].reshape(rows, hidden), w_up[...])

    def gelu_both(h, s):
        if h == 0:
            d_in(s).wait()
            d_hid[...] = mt(d[lax.rem(s, plan.d_slots)].reshape(rows, hidden), w_down[...]).astype(BF16)

        def block(i):
            part_rows = pl.ds(pl.multiple_of(h * half + i * block_rows, block_rows), block_rows)
            v = pre[part_rows]
            v2 = v * v
            c = 0.7978845608028654
            th = jnp.tanh(c * (v + 0.044715 * (v * v2)))
            u[part_rows] = (0.5 * v * (1.0 + th)).astype(BF16)
            slope = 0.5 * (1.0 + th) + 0.5 * v * (1.0 - th * th) * (c * (1.0 + 3.0 * 0.044715 * v2))
            d_pre[part_rows] = (d_hid[part_rows].astype(F32) * slope).astype(BF16)
        loop(HALF, block)

    def grad_b(s):
        for h in range(2):
            store_part(ring_mlp, lax.rem(s, SLOTS), h, mt(d_pre[h * half:(h + 1) * half], w_up[...]), db_rows)

    def down(s):
        @pl.when(s >= SLOTS)
        def _():
            out_copy(s - SLOTS).wait()
        for h in range(2):
            store_part(ring_mlp, lax.rem(s, SLOTS), h, mm(u[h * half:(h + 1) * half], w_down[...]), p2_rows)
        ring_mlp.stage(0, s)

    def grad_up(s):
        dw_up[...] += tm(b[...].reshape(rows, hidden), d_pre[...])

    def grad_down(s):
        dw_down[...] += tm(u[...], d[lax.rem(s, plan.d_slots)].reshape(rows, hidden))

    def grad_mid(h, s):
        slot, x1_slot, d_slot = lax.rem(s, SLOTS), lax.rem(s, plan.x1_slots), lax.rem(s, plan.d_slots)

        def block(i):
            r = h * HALF + i
            dx, dg = norm_back(x1[x1_slot, r].astype(F32), gain_mlp[...], ring_mlp.whole[slot, r, db_rows].astype(F32))
            dg_mlp[...] += rows_sum(dg)
            d[d_slot, r] = (d[d_slot, r].astype(F32) + dx).astype(BF16)
        loop(HALF, block)

    def grad_heads(s):
        d_rows = d[lax.rem(s, plan.d_slots)].reshape(rows, hidden)
        d_heads[...] = mt(d_rows, w_out[...]).astype(BF16)
        dw_out[...] += tm(saved[lax.rem(s, plan.a_slots), :, 3 * width:4 * width], d_rows)

    def attend_back(head, s):
        mask = masks[head]
        slot = lax.rem(s, plan.a_slots)
        for h in range(2):
            keys = (h + 1) * half

            def q_block(i):
                row0 = pl.multiple_of(h * half + i * Q_ROWS, Q_ROWS)
                part_rows = pl.ds(row0, Q_ROWS)
                q = jnp.where(mask, saved[slot, part_rows, 0:width], 0).astype(BF16)
                d_head = jnp.where(mask, d_heads[part_rows], 0).astype(BF16)
                p = probs_of(q, saved[slot, :keys, width:2 * width], seg, s, row0, scale)
                d_p = mt(d_head, saved[slot, :keys, 2 * width:3 * width])
                row_dot = jnp.sum(d_p * p, axis=-1, keepdims=True)
                probs[part_rows, :keys] = p.astype(BF16)
                d_scores[part_rows, :keys] = (p * (d_p - row_dot) * scale).astype(BF16)
            loop(half // Q_ROWS, q_block)

    def head_grads(head, s):
        mask = masks[head]
        slot = lax.rem(s, plan.a_slots)
        d_q = mm(d_scores[...], saved[slot, :, width:2 * width]).astype(BF16)
        d_k = tm(d_scores[...], saved[slot, :, 0:width]).astype(BF16)
        d_v = tm(probs[...], d_heads[...]).astype(BF16)
        for j, value in enumerate((d_q, d_k, d_v)):
            cols = slice(j * width, (j + 1) * width)
            d_qkv[:, cols] = value if head == 0 else jnp.where(mask, value, d_qkv[:, cols])

    def grad_a(s):
        @pl.when(s >= SLOTS)
        def _():
            dtok_copy(s - SLOTS).wait()
        for h in range(2):
            store_part(ring_da, lax.rem(s, SLOTS), h, mm(d_qkv[h * half:(h + 1) * half], w_qkv[...]))
        ring_da.stage(0, s)

    def grad_qkv(s):
        dw_qkv[...] += tm(d_qkv[...], a[lax.rem(s, plan.a_slots)].reshape(rows, hidden))

    def with_h(fn, h):
        return functools.partial(fn, h)

    work = {'A': [with_h(norm_in, 0), with_h(norm_in, 1), with_h(attend, 0), with_h(attend, 1)],
            'B': [with_h(norm_mid, 0), with_h(norm_mid, 1), up, with_h(gelu_both, 0), with_h(gelu_both, 1), grad_b, down,
                  grad_up, grad_down],
            'C': [with_h(grad_mid, 0), with_h(grad_mid, 1), grad_heads, with_h(attend_back, 0), with_h(head_grads, 0),
                  with_h(attend_back, 1), with_h(head_grads, 1), grad_a, grad_qkv]}
    assert sum(len(v) for v in work.values()) == plan.points
    first = plan.start['p1']
    progress = make_progress(plan.points, [(gather_wout, 1, 0, 0, [first + 1, first + 4, first + 7], None)] + [
        (ring, count, plan.ring_lead(name), plan.start[name], STAGES[name], consume) for name, ring, consume in (
            ('p1', gather_p1, consume_p1), ('mlp', ring_mlp, consume_p2), ('da', ring_da, consume_da))])

    x_in(0).start()
    for s in range(count):
        seg[s] = seg_in[s:s + 1]
    w_out_all[my_rows(me, width)] = w_out[...]
    enter(size)
    gather_wout.stage(0, 0)
    for n in range(w_qkv_in.shape[0]):
        for j in range(3):
            at = (j * w_qkv_in.shape[0] + n) * head_dim
            w_qkv[at:at + head_dim] = w_qkv_in[n, j]
    for ref in (dw_qkv, dw_out, dw_up, dw_down, dg_attn, dg_mlp, probs, d_scores):
        ref[...] = jnp.zeros_like(ref)

    def step(t):
        @pl.when(t + 1 < count)
        def _():
            x_in(t + 1).start()
        s_mid = t - plan.lead['B']

        @pl.when(jnp.logical_and(s_mid >= 0, s_mid < count))
        def _():
            d_in(s_mid).start()
        for i, tag in enumerate(ORDER):
            s = t - plan.lead[tag[0]]

            @pl.when(jnp.logical_and(s >= 0, s < count))
            def _(fn=work[tag[0]][int(tag[1:])], s=s):
                fn(s)
            progress(t, i)

    loop(count + plan.steps, step)
    for acc, out in ((dw_out, dw_out_out), (dw_up, dw_up_out), (dw_down, dw_down_out)):
        out[...] = acc[...].astype(BF16)
    for n in range(w_qkv_in.shape[0]):
        for j in range(3):
            at = (j * w_qkv_in.shape[0] + n) * head_dim
            dw_qkv_out[n, j] = dw_qkv[at:at + head_dim].astype(BF16)
    dg_out[0:1] = jnp.sum(dg_attn[...], axis=0, keepdims=True)
    dg_out[1:2] = jnp.sum(dg_mlp[...], axis=0, keepdims=True)
    for s in range(count - SLOTS, count):
        out_copy(s).wait()
        dtok_copy(s).wait()


def my_rows(me, width):
    return pl.ds(pl.multiple_of(me * width, width), width)


def publish_kernel(count, *refs):
    n = len(refs) // 5
    ins, outs, held, in_sems, out_sems = (refs[k * n:(k + 1) * n] for k in range(5))

    def moves(i):
        if i >= count:
            yield (pltpu.make_async_copy(ins[i], held[i], in_sems[i].at[0]),
                   pltpu.make_async_copy(held[i], outs[i], out_sems[i].at[0]))
            return
        for r in range(ins[i].shape[0]):
            yield (pltpu.make_async_copy(ins[i].at[r], held[i].at[r], in_sems[i].at[r]),
                   pltpu.make_async_copy(held[i].at[r], outs[i].at[r], out_sems[i].at[r]))
    pairs = [pair for i in range(n) for pair in moves(i)]
    for into, _ in pairs:
        into.start()
    for into, out in pairs:
        into.wait()
        out.start()
    for _, out in pairs:
        out.wait()


def publish(values, split):
    sems = [pltpu.SemaphoreType.DMA((v.shape[0] if i < split else 1,)) for i, v in enumerate(values)]
    return pl.pallas_call(
        functools.partial(publish_kernel, split),
        out_shape=[jax.ShapeDtypeStruct(v.shape, v.dtype) for v in values],
        in_specs=[pl.BlockSpec(memory_space=pl.ANY)] * len(values),
        out_specs=[pl.BlockSpec(memory_space=pl.ANY)] * len(values),
        scratch_shapes=[pltpu.VMEM(v.shape, v.dtype) for v in values] + sems + sems,
        compiler_params=pltpu.CompilerParams(vmem_limit_bytes=VMEM_LIMIT),
        name='publish',
    )(*values)


def ring_buffers(block_rows, hidden):
    return [
        pltpu.VMEM((SLOTS, BLOCKS, block_rows, hidden), BF16),
        pltpu.VMEM((SLOTS, HALF, block_rows, hidden), BF16),
        pltpu.VMEM((SLOTS, 2, block_rows, hidden), BF16),
        pltpu.VMEM((SLOTS, 2, PIECE, block_rows, hidden), BF16),
        pltpu.VMEM((SLOTS, BLOCKS, block_rows, hidden), BF16),
    ]


def ring_sems():
    return [pltpu.SemaphoreType.DMA((SLOTS, COPIES)), pltpu.SemaphoreType.DMA((SLOTS, COPIES))]


def run_kernel(kernel, ident, outs, out_vmem, args, in_vmem, scratch):
    def spec(in_vmem):
        return pl.BlockSpec(memory_space=pltpu.VMEM if in_vmem else pl.ANY)
    return pl.pallas_call(
        kernel,
        out_shape=[jax.ShapeDtypeStruct(s, t) for s, t in outs],
        in_specs=[spec(v) for v in in_vmem],
        out_specs=[spec(v) for v in out_vmem],
        scratch_shapes=scratch,
        compiler_params=pltpu.CompilerParams(collective_id=ident, has_side_effects=True, vmem_limit_bytes=VMEM_LIMIT),
        name=f'layer_part_{ident}',
    )(*args)


def solution(mesh):
    size = mesh.shape['model']
    dma = pltpu.SemaphoreType.DMA

    def device_step(tokens, seg_ids, d_out, gain_attn, gain_mlp, w_qkv, w_out, w_up, w_down):
        count, seq_len, hidden = tokens.shape
        heads, head_dim = w_qkv.shape[1], w_qkv.shape[3]
        width = heads * head_dim
        inner = w_up.shape[1]
        block_rows = seq_len // BLOCKS
        act = (count, BLOCKS, block_rows, hidden)
        one = (BLOCKS, block_rows, hidden)
        x = tokens.reshape(act)
        d = d_out.reshape(act)
        gains = jnp.stack([gain_attn, gain_mlp]).astype(F32)
        wqkv = w_qkv.transpose(1, 2, 3, 0)
        wout = w_out.reshape(width, hidden)
        plan = Plan()

        outs = [(act, BF16), (act, BF16), (wqkv.shape, BF16), ((width, hidden), BF16),
                ((hidden, inner), BF16), ((inner, hidden), BF16), ((2, hidden), F32)]
        scratch = [pltpu.VMEM(shape, kind) for shape, kind in (
            ((plan.x_slots,) + one, BF16), ((plan.d_slots,) + one, BF16), ((plan.x1_slots,) + one, BF16),
            ((plan.a_slots,) + one, BF16), ((plan.a_slots, seq_len, 4 * width), BF16),
            ((plan.head_slots, seq_len, size * width), BF16), ((3 * width, hidden), BF16), ((size * width, hidden), BF16),
            (one, BF16), ((seq_len, inner), F32), ((seq_len, inner), BF16),
            ((seq_len, inner), BF16), ((seq_len, inner), BF16), ((seq_len, width), BF16),
            ((seq_len, seq_len), BF16), ((seq_len, seq_len), BF16), ((seq_len, 3 * width), BF16),
            ((3 * width, hidden), F32), ((width, hidden), F32), ((hidden, inner), F32), ((inner, hidden), F32),
            ((8, hidden), F32), ((8, hidden), F32), ((count, 1, seq_len), jnp.int32))]
        scratch += [dma((plan.x_slots,)), dma((plan.d_slots,)), dma((SLOTS,)), dma((SLOTS,))]
        scratch += [dma((plan.head_slots, 8))] * 2 + [dma((1, 8))] * 2
        for ring_rows in (2 * block_rows, block_rows):
            scratch += ring_buffers(ring_rows, hidden) + ring_sems()
        results = run_kernel(
            functools.partial(layer_kernel, size, head_dim, plan), 1, outs, [False] * 2 + [True] * 5,
            [x, d, seg_ids, gains, wqkv, wout, w_up, w_down], [False] * 2 + [True] * 6, scratch)
        layer_out, d_tokens, dw_qkv, dw_out, d_w_up, d_w_down, dg = publish(results, 2)

        return (layer_out.reshape(tokens.shape), d_tokens.reshape(tokens.shape), dw_qkv.transpose(3, 0, 1, 2),
                dw_out.reshape(w_out.shape), d_w_up, d_w_down, dg[0], dg[1])

    in_specs = (P('data', None, None), P('data', None), P('data', None, None), P(), P(), P(None, 'model', None, None), P('model', None, None), P(None, 'model'), P('model', None))
    out_specs = (P('data', None, None), P('data', None, None), P('data', 'model', None, None), P(('data', 'model'), None, None), P('data', 'model'), P(('data', 'model'), None), P('data'), P('data'))
    return jax.shard_map(device_step, mesh=mesh, in_specs=in_specs, out_specs=out_specs, check_vma=False)
```

```python
import functools
import jax
import jax.numpy as jnp
from jax import lax
from jax.experimental import pallas as pl
from jax.experimental.pallas import tpu as pltpu
from jax.sharding import PartitionSpec as P

NORM_EPS = 1e-5
MESH = pl.DeviceIdType.MESH
F32 = jnp.float32
BF16 = jnp.bfloat16
SLOTS = 2
BLOCKS = 16
HALF = BLOCKS // 2
PIECE = 2
COPIES = 13
VMEM_LIMIT = 66 * 1000 * 1000


def mm(a, b):
    return lax.dot_general(a, b, (((1,), (0,)), ((), ())), preferred_element_type=F32)


def mt(a, b):
    return lax.dot_general(a, b, (((1,), (1,)), ((), ())), preferred_element_type=F32)


def tm(a, b):
    return lax.dot_general(a, b, (((0,), (0,)), ((), ())), preferred_element_type=F32)


def loop(count, body):
    def step(i, carry):
        body(i)
        return carry
    lax.fori_loop(0, count, step, 0)


class Gather:
    first, last = 0, 3

    def __init__(self, size, slots, view, send, recv):
        me = lax.axis_index('model')
        self.core = lax.rem(me, 2)
        self.chips = size // 2
        self.chip = me // 2
        self.right = lax.rem(me + 2, size)
        self.left = lax.rem(me + size - 2, size)
        self.partner = me + 1 - 2 * self.core
        self.slots, self.view, self.send, self.recv = slots, view, send, recv

    def at(self, slot, step, part=None):
        return self.view(slot, self.core, lax.rem(self.chip + step, self.chips), part)

    def remote(self, slot, n, src, dst, to):
        return pltpu.make_async_remote_copy(
            src_ref=src, dst_ref=dst, send_sem=self.send.at[slot, n], recv_sem=self.recv.at[slot, n],
            device_id={'model': to}, device_id_type=MESH)

    def copy(self, n, s):
        slot = lax.rem(s, self.slots)
        behind = self.chips - 1
        step, part, to = [(0, None, self.right), (0, None, self.left), (0, None, self.partner),
                          (behind, 0, self.right), (1, 1, self.left), (behind, None, self.partner),
                          (1, None, self.partner), (2, None, self.partner)][n]
        ref = self.at(slot, step, part)
        return self.remote(slot, n, ref, ref, to)

    def gather_stage(self, j, s):
        if j == 0:
            starts, waits = (0, 1, 2), ()
        elif j == 1:
            starts, waits = (3, 4, 5, 6), (0, 1)
        elif j == 2:
            starts, waits = (7,), (3, 4)
        else:
            starts, waits = (), (2, 5, 6, 7)
        for n in waits:
            self.copy(n, s).wait_recv()
        for n in starts:
            self.copy(n, s).start()
        if j == 3:
            for n in range(8):
                self.copy(n, s).wait_send()

    def stage(self, j, s):
        self.gather_stage(j, s)


class RingSum(Gather):
    last = 6

    def __init__(self, size, part, pair_in, relay_in, ring_in, whole, send, recv):
        self.part, self.pair_in, self.relay_in, self.ring_in, self.whole = part, pair_in, relay_in, ring_in, whole
        self.finish = None
        super().__init__(size, SLOTS, self.block_view, send, recv)

    def block_view(self, slot, core, chip, part):
        start = core * HALF + chip * PIECE
        if part is None:
            return self.whole.at[slot, pl.ds(start, PIECE)]
        return self.whole.at[slot, pl.ds(start + part, 1)]

    def base(self, step):
        return self.core * HALF + lax.rem(self.chip + step, self.chips) * PIECE

    def sum_copy(self, n, s):
        slot = lax.rem(s, SLOTS)
        part = self.part.at[slot]
        if n == 8:
            src, dst, to = part.at[pl.ds((1 - self.core) * HALF, HALF)], self.pair_in.at[slot], self.partner
        elif n == 9:
            src, dst, to = part.at[pl.ds(self.base(2), 1)], self.relay_in.at[slot, pl.ds(0, 1)], self.right
        elif n == 10:
            src, dst, to = part.at[pl.ds(self.base(2) + 1, 1)], self.relay_in.at[slot, pl.ds(1, 1)], self.left
        elif n == 11:
            src, dst, to = part.at[pl.ds(self.base(1), PIECE)], self.ring_in.at[slot, 0], self.right
        else:
            src, dst, to = part.at[pl.ds(self.base(self.chips - 1), PIECE)], self.ring_in.at[slot, 1], self.left
        return self.remote(slot, n, src, dst, to)

    def add(self, slot, block, others):
        total = self.part[slot, block].astype(F32)
        for ref in others:
            total = total + ref.astype(F32)
        return total.astype(BF16)

    def stage(self, j, s):
        slot = lax.rem(s, SLOTS)
        if j == 0:
            self.sum_copy(8, s).start()
        elif j == 1:
            self.sum_copy(8, s).wait_recv()

            def pair(i):
                at = lax.rem(lax.rem(self.chip + 2, self.chips) * PIECE + i, HALF)
                block = self.core * HALF + at
                self.part[slot, block] = self.add(slot, block, [self.pair_in[slot, at]])
            loop(HALF, pair)
            self.sum_copy(9, s).start()
            self.sum_copy(10, s).start()
        elif j == 2:
            self.sum_copy(9, s).wait_recv()
            self.sum_copy(10, s).wait_recv()
            first, second = self.base(1), self.base(self.chips - 1) + 1
            self.part[slot, first] = self.add(slot, first, [self.relay_in[slot, 0]])
            self.part[slot, second] = self.add(slot, second, [self.relay_in[slot, 1]])
            self.sum_copy(11, s).start()
            self.sum_copy(12, s).start()
        elif j == 3:
            self.sum_copy(11, s).wait_recv()
            self.sum_copy(12, s).wait_recv()
            for i in range(PIECE):
                block = self.base(0) + i
                total = self.part[slot, block].astype(F32)
                total = total + self.ring_in[slot, 0, i].astype(F32) + self.ring_in[slot, 1, i].astype(F32)
                self.whole[slot, block] = self.finish(s, block, i, total).astype(BF16)
            self.gather_stage(0, s)
        else:
            self.gather_stage(j - 3, s)
            if j == self.last:
                for n in range(8, COPIES):
                    self.sum_copy(n, s).wait_send()


def enter(size):
    me = lax.axis_index('model')
    barrier = pltpu.get_barrier_semaphore()
    for step in range(1, size):
        pl.semaphore_signal(barrier, inc=1, device_id={'model': lax.rem(me + step, size)}, device_id_type=MESH)
    pl.semaphore_wait(barrier, size - 1)


def make_progress(points, sums):
    def progress(t, i):
        for ring, count, lead, start, offsets, consume in sums:
            for j in range(ring.last, 0, -1):
                ahead = start + offsets[j - 1] - i
                if ahead % points:
                    continue
                s = t - lead - ahead // points

                @pl.when(jnp.logical_and(s >= 0, s < count))
                def _(ring=ring, consume=consume, j=j, s=s):
                    ring.stage(j, s)
                    if j == ring.last and consume is not None:
                        consume(s)
    return progress


def norm_stats(x):
    mean = jnp.mean(x, axis=-1, keepdims=True)
    centered = x - mean
    var = jnp.mean(centered * centered, axis=-1, keepdims=True)
    inv = lax.rsqrt(var + NORM_EPS)
    return centered * inv, inv


def norm_back(x, gain, d_normed):
    unit, inv = norm_stats(x)
    d_unit = d_normed * gain
    mean_d = jnp.mean(d_unit, axis=-1, keepdims=True)
    mean_du = jnp.mean(d_unit * unit, axis=-1, keepdims=True)
    return inv * (d_unit - mean_d - unit * mean_du), d_normed * unit


def probs_of(q, k, seg_ref, s, row0, scale):
    keys = k.shape[0]
    seg_q = seg_ref[s, :, pl.ds(row0, Q_ROWS)]
    seg_q = jnp.broadcast_to(seg_q, (Q_ROWS, Q_ROWS)).T[:, :1]
    seg_k = seg_ref[s, :, :keys]
    scores = mt(q, k) * scale
    q_pos = row0 + lax.broadcasted_iota(jnp.int32, scores.shape, 0)
    k_pos = lax.broadcasted_iota(jnp.int32, scores.shape, 1)
    allowed = jnp.logical_and(seg_q == seg_k, q_pos >= k_pos)
    scores = jnp.where(allowed, scores, -1e30)
    e = jnp.exp(scores - jnp.max(scores, axis=-1, keepdims=True))
    return e * (1.0 / jnp.sum(e, axis=-1, keepdims=True))


def head_masks(width, head_dim):
    lane = lax.broadcasted_iota(jnp.int32, (1, width), 1)
    return [jnp.logical_and(lane >= h * head_dim, lane < (h + 1) * head_dim) for h in range(width // head_dim)]


Q_ROWS = 128

ORDER = ['B0', 'B1', 'B2', 'B3', 'B4', 'B5', 'B6', 'C0', 'A0', 'C1', 'A1', 'C2', 'A2', 'C3', 'C4', 'A3', 'B7', 'C5',
         'B8', 'C6']
STAGES = {'p1': [10, 17, 23], 'db': [2, 5, 9, 13, 19, 21], 'p2': [2, 6, 14, 23, 33, 35], 'da': [2, 7, 19, 23, 35, 36]}
STARTS = {'p1': 'A3', 'db': 'B5', 'p2': 'B6', 'da': 'C5'}


class Plan:
    def __init__(self):
        self.points = n = len(ORDER)
        self.pos = {tag: i for i, tag in enumerate(ORDER)}
        self.start = {ring: self.pos[tag] for ring, tag in STARTS.items()}
        self.lead = {'A': 0}
        self.lead['B'] = self.after('p1', 'B0')
        self.lead['C'] = self.after('db', 'C0')
        end = {ring: self.step_of(ring, -1) for ring in STAGES}
        own = {ring: self.step_of(ring, 2) for ring in STAGES}
        self.steps = max(end.values())
        self.x_slots = own['da'] + 2
        self.d_slots = max(own['db'], self.lead['B']) - self.lead['B'] + 1
        self.x1_slots = max(own['db'], own['p2']) - end['p1'] + 1
        self.own_slots = own['da'] - own['db'] + 1
        self.a_slots = self.lead['C'] + 1
        self.head_slots = 2 if STAGES['p1'][-1] < n else 3
        assert all(o[-1] < 2 * n for o in STAGES.values())
        assert self.lead['C'] * n + self.pos['C0'] < (self.lead['B'] + 2) * n + self.start['db']

    def ring_lead(self, ring):
        return self.lead[STARTS[ring][0]]

    def end(self, ring, stage=-1):
        return self.ring_lead(ring) * self.points + self.start[ring] + STAGES[ring][stage]

    def step_of(self, ring, stage):
        return self.end(ring, stage) // self.points

    def after(self, ring, tag):
        end = self.end(ring)
        return end // self.points + (0 if self.pos[tag] > end % self.points else 1)


def layer_kernel(size, head_dim, plan, *refs):
    (tok_hbm, dout_hbm, seg_in, gains, w_qkv_in, w_out, w_up, w_down,
     out_hbm, dtok_hbm, dw_qkv_out, dw_out_out, dw_up_out, dw_down_out, dg_out,
     x, d, x1, a, saved, heads, w_qkv, w_out_all, b, pre, d_hid, u, d_pre, d_heads, probs, d_scores, d_qkv,
     dw_qkv, dw_out, dw_up, dw_down, dg_attn, dg_mlp,
     seg, own, dg_parts, x_sem, d_sem, out_sem, dtok_sem, heads_send, heads_recv, wout_send, wout_recv,
     dg_send, dg_recv) = refs[:51]
    ring_db, ring_p2, ring_da = [RingSum(size, *refs[51 + 7 * n:58 + 7 * n]) for n in range(3)]
    count = tok_hbm.shape[0]
    block_rows, hidden = x.shape[2], x.shape[3]
    rows = BLOCKS * block_rows
    half = rows // 2
    width = w_out.shape[0]
    scale = head_dim ** -0.5
    masks = head_masks(width, head_dim)
    me = lax.axis_index('model')
    my_lanes = pl.ds(pl.multiple_of(me * width, width), width)
    gain_attn, gain_mlp = gains.at[0:1], gains.at[1:2]

    def heads_view(slot, core, chip, part):
        lanes = pl.ds(pl.multiple_of((2 * chip + core) * width, width), width)
        span = pl.ds(0, rows) if part is None else pl.ds(part * half, half)
        return heads.at[slot, span, lanes]

    def wout_view(slot, core, chip, part):
        first = (2 * chip + core) * width
        if part is None:
            return w_out_all.at[pl.ds(pl.multiple_of(first, width), width)]
        size_half = width // 2
        return w_out_all.at[pl.ds(pl.multiple_of(first + part * size_half, size_half), size_half)]

    gather_p1 = Gather(size, plan.head_slots, heads_view, heads_send, heads_recv)
    gather_wout = Gather(size, 1, wout_view, wout_send, wout_recv)

    def x_in(s):
        slot = lax.rem(s, plan.x_slots)
        return pltpu.make_async_copy(tok_hbm.at[s], x.at[slot], x_sem.at[slot])

    def d_in(s):
        slot = lax.rem(s, plan.d_slots)
        return pltpu.make_async_copy(dout_hbm.at[s], d.at[slot], d_sem.at[slot])

    def out_copy(s):
        slot = lax.rem(s, SLOTS)
        return pltpu.make_async_copy(ring_p2.whole.at[slot], out_hbm.at[s], out_sem.at[slot])

    def dtok_copy(s):
        slot = lax.rem(s, SLOTS)
        return pltpu.make_async_copy(ring_da.whole.at[slot], dtok_hbm.at[s], dtok_sem.at[slot])

    def rows_sum(v):
        return jnp.sum(v.reshape(v.shape[0] // 8, 8, hidden), axis=0)

    def consume_p1(s):
        x_slot, x1_slot, h_slot = lax.rem(s, plan.x_slots), lax.rem(s, plan.x1_slots), lax.rem(s, plan.head_slots)
        for h in range(2):
            blocks = slice(h * HALF, (h + 1) * HALF)
            proj = mm(heads[h_slot, h * half:(h + 1) * half], w_out_all[...]).astype(BF16).reshape(HALF, block_rows, hidden)
            x1[x1_slot, blocks] = (x[x_slot, blocks].astype(F32) + proj.astype(F32)).astype(BF16)

    def finish_db(s, block, i, total):
        x1_slot, d_slot = lax.rem(s, plan.x1_slots), lax.rem(s, plan.d_slots)
        dx, dg = norm_back(x1[x1_slot, block].astype(F32), gain_mlp[...], total)
        dg_mlp[...] += rows_sum(dg)
        d_resid = (d[d_slot, block].astype(F32) + dx).astype(BF16)
        own[lax.rem(s, plan.own_slots), i] = d_resid
        return d_resid

    def finish_p2(s, block, i, total):
        return x1[lax.rem(s, plan.x1_slots), block].astype(F32) + total.astype(BF16).astype(F32)

    def finish_da(s, block, i, total):
        dx, dg = norm_back(x[lax.rem(s, plan.x_slots), block].astype(F32), gain_attn[...], total)
        dg_attn[...] += rows_sum(dg)
        return own[lax.rem(s, plan.own_slots), i].astype(F32) + dx

    ring_db.finish, ring_p2.finish, ring_da.finish = finish_db, finish_p2, finish_da

    def consume_p2(s):
        out_copy(s).start()

    def consume_da(s):
        dtok_copy(s).start()

    def store_part(ring, slot, h, value):
        ring.part[slot, h * HALF:(h + 1) * HALF] = value.astype(BF16).reshape(HALF, block_rows, hidden)

    def norm_in(h, s):
        x_slot, slot = lax.rem(s, plan.x_slots), lax.rem(s, plan.a_slots)
        if h == 0:
            x_in(s).wait()

        def block(i):
            r = h * HALF + i
            unit, _ = norm_stats(x[x_slot, r].astype(F32))
            a[slot, r] = (unit * gain_attn[...]).astype(BF16)
        loop(HALF, block)
        if h == 1:
            saved[slot, :, :3 * width] = mt(a[slot].reshape(rows, hidden), w_qkv[...]).astype(BF16)

    def attend(h, s):
        slot, h_slot = lax.rem(s, plan.a_slots), lax.rem(s, plan.head_slots)
        keys = (h + 1) * half

        def q_block(i):
            row0 = pl.multiple_of(h * half + i * Q_ROWS, Q_ROWS)
            part_rows = pl.ds(row0, Q_ROWS)
            q = saved[slot, part_rows, 0:width]
            k = saved[slot, :keys, width:2 * width]
            v = saved[slot, :keys, 2 * width:3 * width]
            out = None
            for mask in masks:
                p = probs_of(jnp.where(mask, q, 0).astype(BF16), k, seg, s, row0, scale)
                head = mm(p.astype(BF16), v)
                out = head if out is None else jnp.where(mask, head, out)
            out = out.astype(BF16)
            saved[slot, part_rows, 3 * width:4 * width] = out
            heads[h_slot, part_rows, my_lanes] = out
        loop(half // Q_ROWS, q_block)
        if h == 1:
            gather_p1.stage(0, s)

    def norm_mid(h, s):
        x1_slot = lax.rem(s, plan.x1_slots)

        def block(i):
            r = h * HALF + i
            unit, _ = norm_stats(x1[x1_slot, r].astype(F32))
            b[r] = (unit * gain_mlp[...]).astype(BF16)
        loop(HALF, block)

    def up(s):
        pre[...] = mm(b[...].reshape(rows, hidden), w_up[...])

    def gelu_both(h, s):
        if h == 0:
            d_in(s).wait()
            d_hid[...] = mt(d[lax.rem(s, plan.d_slots)].reshape(rows, hidden), w_down[...]).astype(BF16)

        def block(i):
            part_rows = pl.ds(pl.multiple_of(h * half + i * block_rows, block_rows), block_rows)
            v = pre[part_rows]
            v2 = v * v
            c = 0.7978845608028654
            th = jnp.tanh(c * (v + 0.044715 * (v * v2)))
            u[part_rows] = (0.5 * v * (1.0 + th)).astype(BF16)
            slope = 0.5 * (1.0 + th) + 0.5 * v * (1.0 - th * th) * (c * (1.0 + 3.0 * 0.044715 * v2))
            d_pre[part_rows] = (d_hid[part_rows].astype(F32) * slope).astype(BF16)
        loop(HALF, block)

    def grad_b(s):
        for h in range(2):
            store_part(ring_db, lax.rem(s, SLOTS), h, mt(d_pre[h * half:(h + 1) * half], w_up[...]))
        ring_db.stage(0, s)

    def down(s):
        @pl.when(s >= SLOTS)
        def _():
            out_copy(s - SLOTS).wait()
        for h in range(2):
            store_part(ring_p2, lax.rem(s, SLOTS), h, mm(u[h * half:(h + 1) * half], w_down[...]))
        ring_p2.stage(0, s)

    def grad_up(s):
        dw_up[...] += tm(b[...].reshape(rows, hidden), d_pre[...])

    def grad_down(s):
        dw_down[...] += tm(u[...], d[lax.rem(s, plan.d_slots)].reshape(rows, hidden))

    def grad_heads(s):
        d_rows = ring_db.whole[lax.rem(s, SLOTS)].reshape(rows, hidden)
        d_heads[...] = mt(d_rows, w_out[...]).astype(BF16)
        dw_out[...] += tm(saved[lax.rem(s, plan.a_slots), :, 3 * width:4 * width], d_rows)

    def attend_back(head, s):
        mask = masks[head]
        slot = lax.rem(s, plan.a_slots)
        for h in range(2):
            keys = (h + 1) * half

            def q_block(i):
                row0 = pl.multiple_of(h * half + i * Q_ROWS, Q_ROWS)
                part_rows = pl.ds(row0, Q_ROWS)
                q = jnp.where(mask, saved[slot, part_rows, 0:width], 0).astype(BF16)
                d_head = jnp.where(mask, d_heads[part_rows], 0).astype(BF16)
                p = probs_of(q, saved[slot, :keys, width:2 * width], seg, s, row0, scale)
                d_p = mt(d_head, saved[slot, :keys, 2 * width:3 * width])
                row_dot = jnp.sum(d_p * p, axis=-1, keepdims=True)
                probs[part_rows, :keys] = p.astype(BF16)
                d_scores[part_rows, :keys] = (p * (d_p - row_dot) * scale).astype(BF16)
            loop(half // Q_ROWS, q_block)

    def head_grads(head, s):
        mask = masks[head]
        slot = lax.rem(s, plan.a_slots)
        d_q = mm(d_scores[...], saved[slot, :, width:2 * width]).astype(BF16)
        d_k = tm(d_scores[...], saved[slot, :, 0:width]).astype(BF16)
        d_v = tm(probs[...], d_heads[...]).astype(BF16)
        for j, value in enumerate((d_q, d_k, d_v)):
            cols = slice(j * width, (j + 1) * width)
            d_qkv[:, cols] = value if head == 0 else jnp.where(mask, value, d_qkv[:, cols])

    def grad_a(s):
        @pl.when(s >= SLOTS)
        def _():
            dtok_copy(s - SLOTS).wait()
        for h in range(2):
            store_part(ring_da, lax.rem(s, SLOTS), h, mm(d_qkv[h * half:(h + 1) * half], w_qkv[...]))
        ring_da.stage(0, s)

    def grad_qkv(s):
        dw_qkv[...] += tm(d_qkv[...], a[lax.rem(s, plan.a_slots)].reshape(rows, hidden))

    def with_h(fn, h):
        return functools.partial(fn, h)

    work = {'A': [with_h(norm_in, 0), with_h(norm_in, 1), with_h(attend, 0), with_h(attend, 1)],
            'B': [with_h(norm_mid, 0), with_h(norm_mid, 1), up, with_h(gelu_both, 0), with_h(gelu_both, 1), grad_b, down,
                  grad_up, grad_down],
            'C': [grad_heads, with_h(attend_back, 0), with_h(head_grads, 0),
                  with_h(attend_back, 1), with_h(head_grads, 1), grad_a, grad_qkv]}
    assert sum(len(v) for v in work.values()) == plan.points
    first = plan.start['p1']
    progress = make_progress(plan.points, [(gather_wout, 1, 0, 0, [first + 1, first + 4, first + 7], None)] + [
        (ring, count, plan.ring_lead(name), plan.start[name], STAGES[name], consume) for name, ring, consume in (
            ('p1', gather_p1, consume_p1), ('db', ring_db, None), ('p2', ring_p2, consume_p2), ('da', ring_da, consume_da))])

    x_in(0).start()
    for s in range(count):
        seg[s] = seg_in[s:s + 1]
    w_out_all[my_rows(me, width)] = w_out[...]
    enter(size)
    gather_wout.stage(0, 0)
    for n in range(w_qkv_in.shape[0]):
        for j in range(3):
            at = (j * w_qkv_in.shape[0] + n) * head_dim
            w_qkv[at:at + head_dim] = w_qkv_in[n, j]
    for ref in (dw_qkv, dw_out, dw_up, dw_down, dg_attn, dg_mlp, probs, d_scores):
        ref[...] = jnp.zeros_like(ref)

    def step(t):
        @pl.when(t + 1 < count)
        def _():
            x_in(t + 1).start()
        s_mid = t - plan.lead['B']

        @pl.when(jnp.logical_and(s_mid >= 0, s_mid < count))
        def _():
            d_in(s_mid).start()
        for i, tag in enumerate(ORDER):
            s = t - plan.lead[tag[0]]

            @pl.when(jnp.logical_and(s >= 0, s < count))
            def _(fn=work[tag[0]][int(tag[1:])], s=s):
                fn(s)
            progress(t, i)

    loop(count + plan.steps, step)
    dg_parts[me, 0:1] = jnp.sum(dg_attn[...], axis=0, keepdims=True)
    dg_parts[me, 1:2] = jnp.sum(dg_mlp[...], axis=0, keepdims=True)

    def dg_copy(step, owner):
        return pltpu.make_async_remote_copy(
            src_ref=dg_parts.at[owner], dst_ref=dg_parts.at[owner], send_sem=dg_send.at[step], recv_sem=dg_recv.at[step],
            device_id={'model': lax.rem(me + step, size)}, device_id_type=MESH)

    for step_ahead in range(1, size):
        dg_copy(step_ahead, me).start()
    for acc, out in ((dw_out, dw_out_out), (dw_up, dw_up_out), (dw_down, dw_down_out)):
        out[...] = acc[...].astype(BF16)
    for n in range(w_qkv_in.shape[0]):
        for j in range(3):
            at = (j * w_qkv_in.shape[0] + n) * head_dim
            dw_qkv_out[n, j] = dw_qkv[at:at + head_dim].astype(BF16)
    for step_ahead in range(1, size):
        dg_copy(step_ahead, lax.rem(me + size - step_ahead, size)).wait_recv()
    dg_out[...] = sum(dg_parts[owner] for owner in range(size))
    for step_ahead in range(1, size):
        dg_copy(step_ahead, me).wait_send()
    for s in range(count - SLOTS, count):
        out_copy(s).wait()
        dtok_copy(s).wait()


def my_rows(me, width):
    return pl.ds(pl.multiple_of(me * width, width), width)


def publish_kernel(count, *refs):
    n = len(refs) // 5
    ins, outs, held, in_sems, out_sems = (refs[k * n:(k + 1) * n] for k in range(5))

    def moves(i):
        if i >= count:
            yield (pltpu.make_async_copy(ins[i], held[i], in_sems[i].at[0]),
                   pltpu.make_async_copy(held[i], outs[i], out_sems[i].at[0]))
            return
        for r in range(ins[i].shape[0]):
            yield (pltpu.make_async_copy(ins[i].at[r], held[i].at[r], in_sems[i].at[r]),
                   pltpu.make_async_copy(held[i].at[r], outs[i].at[r], out_sems[i].at[r]))
    pairs = [pair for i in range(n) for pair in moves(i)]
    for into, _ in pairs:
        into.start()
    for into, out in pairs:
        into.wait()
        out.start()
    for _, out in pairs:
        out.wait()


def publish(values, split):
    sems = [pltpu.SemaphoreType.DMA((v.shape[0] if i < split else 1,)) for i, v in enumerate(values)]
    return pl.pallas_call(
        functools.partial(publish_kernel, split),
        out_shape=[jax.ShapeDtypeStruct(v.shape, v.dtype) for v in values],
        in_specs=[pl.BlockSpec(memory_space=pl.ANY)] * len(values),
        out_specs=[pl.BlockSpec(memory_space=pl.ANY)] * len(values),
        scratch_shapes=[pltpu.VMEM(v.shape, v.dtype) for v in values] + sems + sems,
        compiler_params=pltpu.CompilerParams(vmem_limit_bytes=VMEM_LIMIT),
        name='publish',
    )(*values)


def ring_buffers(block_rows, hidden):
    return [
        pltpu.VMEM((SLOTS, BLOCKS, block_rows, hidden), BF16),
        pltpu.VMEM((SLOTS, HALF, block_rows, hidden), BF16),
        pltpu.VMEM((SLOTS, 2, block_rows, hidden), BF16),
        pltpu.VMEM((SLOTS, 2, PIECE, block_rows, hidden), BF16),
        pltpu.VMEM((SLOTS, BLOCKS, block_rows, hidden), BF16),
    ]


def ring_sems():
    return [pltpu.SemaphoreType.DMA((SLOTS, COPIES)), pltpu.SemaphoreType.DMA((SLOTS, COPIES))]


def run_kernel(kernel, ident, outs, out_vmem, args, in_vmem, scratch):
    def spec(in_vmem):
        return pl.BlockSpec(memory_space=pltpu.VMEM if in_vmem else pl.ANY)
    return pl.pallas_call(
        kernel,
        out_shape=[jax.ShapeDtypeStruct(s, t) for s, t in outs],
        in_specs=[spec(v) for v in in_vmem],
        out_specs=[spec(v) for v in out_vmem],
        scratch_shapes=scratch,
        compiler_params=pltpu.CompilerParams(collective_id=ident, has_side_effects=True, vmem_limit_bytes=VMEM_LIMIT),
        name=f'layer_part_{ident}',
    )(*args)


def solution(mesh):
    size = mesh.shape['model']
    dma = pltpu.SemaphoreType.DMA

    def device_step(tokens, seg_ids, d_out, gain_attn, gain_mlp, w_qkv, w_out, w_up, w_down):
        count, seq_len, hidden = tokens.shape
        heads, head_dim = w_qkv.shape[1], w_qkv.shape[3]
        width = heads * head_dim
        inner = w_up.shape[1]
        block_rows = seq_len // BLOCKS
        act = (count, BLOCKS, block_rows, hidden)
        one = (BLOCKS, block_rows, hidden)
        x = tokens.reshape(act)
        d = d_out.reshape(act)
        gains = jnp.stack([gain_attn, gain_mlp]).astype(F32)
        wqkv = w_qkv.transpose(1, 2, 3, 0)
        wout = w_out.reshape(width, hidden)
        plan = Plan()

        outs = [(act, BF16), (act, BF16), (wqkv.shape, BF16), ((width, hidden), BF16),
                ((hidden, inner), BF16), ((inner, hidden), BF16), ((2, hidden), F32)]
        scratch = [pltpu.VMEM(shape, kind) for shape, kind in (
            ((plan.x_slots,) + one, BF16), ((plan.d_slots,) + one, BF16), ((plan.x1_slots,) + one, BF16),
            ((plan.a_slots,) + one, BF16), ((plan.a_slots, seq_len, 4 * width), BF16),
            ((plan.head_slots, seq_len, size * width), BF16), ((3 * width, hidden), BF16), ((size * width, hidden), BF16),
            (one, BF16), ((seq_len, inner), F32), ((seq_len, inner), BF16),
            ((seq_len, inner), BF16), ((seq_len, inner), BF16), ((seq_len, width), BF16),
            ((seq_len, seq_len), BF16), ((seq_len, seq_len), BF16), ((seq_len, 3 * width), BF16),
            ((3 * width, hidden), F32), ((width, hidden), F32), ((hidden, inner), F32), ((inner, hidden), F32),
            ((8, hidden), F32), ((8, hidden), F32), ((count, 1, seq_len), jnp.int32),
            ((plan.own_slots, PIECE, block_rows, hidden), BF16), ((size, 2, hidden), F32))]
        scratch += [dma((plan.x_slots,)), dma((plan.d_slots,)), dma((SLOTS,)), dma((SLOTS,))]
        scratch += [dma((plan.head_slots, 8))] * 2 + [dma((1, 8))] * 2 + [dma((size,))] * 2
        for _ in range(3):
            scratch += ring_buffers(block_rows, hidden) + ring_sems()
        results = run_kernel(
            functools.partial(layer_kernel, size, head_dim, plan), 1, outs, [False] * 2 + [True] * 5,
            [x, d, seg_ids, gains, wqkv, wout, w_up, w_down], [False] * 2 + [True] * 6, scratch)
        layer_out, d_tokens, dw_qkv, dw_out, d_w_up, d_w_down, dg = publish(results, 2)

        return (layer_out.reshape(tokens.shape), d_tokens.reshape(tokens.shape), dw_qkv.transpose(3, 0, 1, 2),
                dw_out.reshape(w_out.shape), d_w_up, d_w_down, dg[0], dg[1])

    in_specs = (P('data', None, None), P('data', None), P('data', None, None), P(), P(), P(None, 'model', None, None), P('model', None, None), P(None, 'model'), P('model', None))
    out_specs = (P('data', None, None), P('data', None, None), P('data', 'model', None, None), P(('data', 'model'), None, None), P('data', 'model'), P(('data', 'model'), None), P('data'), P('data'))
    return jax.shard_map(device_step, mesh=mesh, in_specs=in_specs, out_specs=out_specs, check_vma=False)
```

```python
import functools
import jax
import jax.numpy as jnp
from jax import lax
from jax.experimental import pallas as pl
from jax.experimental.pallas import tpu as pltpu
from jax.sharding import PartitionSpec as P

NORM_EPS = 1e-5
MESH = pl.DeviceIdType.MESH
F32 = jnp.float32
BF16 = jnp.bfloat16
SLOTS = 2
BLOCKS = 16
HALF = BLOCKS // 2
PIECE = 2
COPIES = 13
VMEM_LIMIT = 66 * 1000 * 1000


def mm(a, b):
    return lax.dot_general(a, b, (((1,), (0,)), ((), ())), preferred_element_type=F32)


def mt(a, b):
    return lax.dot_general(a, b, (((1,), (1,)), ((), ())), preferred_element_type=F32)


def tm(a, b):
    return lax.dot_general(a, b, (((0,), (0,)), ((), ())), preferred_element_type=F32)


def loop(count, body, unroll=1):
    def step(i, carry):
        body(i)
        return carry
    lax.fori_loop(0, count, step, 0, unroll=unroll)


class Gather:
    first, last = 0, 3

    def __init__(self, size, slots, view, send, recv):
        me = lax.axis_index('model')
        self.core = lax.rem(me, 2)
        self.chips = size // 2
        self.chip = me // 2
        self.right = lax.rem(me + 2, size)
        self.left = lax.rem(me + size - 2, size)
        self.partner = me + 1 - 2 * self.core
        self.slots, self.view, self.send, self.recv = slots, view, send, recv

    def at(self, slot, step, part=None):
        return self.view(slot, self.core, lax.rem(self.chip + step, self.chips), part)

    def remote(self, slot, n, src, dst, to):
        return pltpu.make_async_remote_copy(
            src_ref=src, dst_ref=dst, send_sem=self.send.at[slot, n], recv_sem=self.recv.at[slot, n],
            device_id={'model': to}, device_id_type=MESH)

    def copy(self, n, s):
        slot = lax.rem(s, self.slots)
        behind = self.chips - 1
        step, part, to = [(0, None, self.right), (0, None, self.left), (0, None, self.partner),
                          (behind, 0, self.right), (1, 1, self.left), (behind, None, self.partner),
                          (1, None, self.partner), (2, None, self.partner)][n]
        ref = self.at(slot, step, part)
        return self.remote(slot, n, ref, ref, to)

    def gather_stage(self, j, s):
        if j == 0:
            starts, waits = (0, 1, 2), ()
        elif j == 1:
            starts, waits = (3, 4, 5, 6), (0, 1)
        elif j == 2:
            starts, waits = (7,), (3, 4)
        else:
            starts, waits = (), (2, 5, 6, 7)
        for n in waits:
            self.copy(n, s).wait_recv()
        for n in starts:
            self.copy(n, s).start()
        if j == 3:
            for n in range(8):
                self.copy(n, s).wait_send()

    def stage(self, j, s):
        self.gather_stage(j, s)


class RingSum(Gather):
    last = 6

    def __init__(self, size, part, pair_in, relay_in, ring_in, whole, send, recv):
        self.part, self.pair_in, self.relay_in, self.ring_in, self.whole = part, pair_in, relay_in, ring_in, whole
        self.finish = None
        super().__init__(size, SLOTS, self.block_view, send, recv)

    def block_view(self, slot, core, chip, part):
        start = core * HALF + chip * PIECE
        if part is None:
            return self.whole.at[slot, pl.ds(start, PIECE)]
        return self.whole.at[slot, pl.ds(start + part, 1)]

    def base(self, step):
        return self.core * HALF + lax.rem(self.chip + step, self.chips) * PIECE

    def sum_copy(self, n, s):
        slot = lax.rem(s, SLOTS)
        part = self.part.at[slot]
        if n == 8:
            src, dst, to = part.at[pl.ds((1 - self.core) * HALF, HALF)], self.pair_in.at[slot], self.partner
        elif n == 9:
            src, dst, to = part.at[pl.ds(self.base(2), 1)], self.relay_in.at[slot, pl.ds(0, 1)], self.right
        elif n == 10:
            src, dst, to = part.at[pl.ds(self.base(2) + 1, 1)], self.relay_in.at[slot, pl.ds(1, 1)], self.left
        elif n == 11:
            src, dst, to = part.at[pl.ds(self.base(1), PIECE)], self.ring_in.at[slot, 0], self.right
        else:
            src, dst, to = part.at[pl.ds(self.base(self.chips - 1), PIECE)], self.ring_in.at[slot, 1], self.left
        return self.remote(slot, n, src, dst, to)

    def add(self, slot, block, others):
        total = self.part[slot, block].astype(F32)
        for ref in others:
            total = total + ref.astype(F32)
        return total.astype(BF16)

    def stage(self, j, s):
        slot = lax.rem(s, SLOTS)
        if j == 0:
            self.sum_copy(8, s).start()
        elif j == 1:
            self.sum_copy(8, s).wait_recv()

            def pair(i):
                at = lax.rem(lax.rem(self.chip + 2, self.chips) * PIECE + i, HALF)
                block = self.core * HALF + at
                self.part[slot, block] = self.add(slot, block, [self.pair_in[slot, at]])
            loop(HALF, pair)
            self.sum_copy(9, s).start()
            self.sum_copy(10, s).start()
        elif j == 2:
            self.sum_copy(9, s).wait_recv()
            self.sum_copy(10, s).wait_recv()
            first, second = self.base(1), self.base(self.chips - 1) + 1
            self.part[slot, first] = self.add(slot, first, [self.relay_in[slot, 0]])
            self.part[slot, second] = self.add(slot, second, [self.relay_in[slot, 1]])
            self.sum_copy(11, s).start()
            self.sum_copy(12, s).start()
        elif j == 3:
            self.sum_copy(11, s).wait_recv()
            self.sum_copy(12, s).wait_recv()
            for i in range(PIECE):
                block = self.base(0) + i
                total = self.part[slot, block].astype(F32)
                total = total + self.ring_in[slot, 0, i].astype(F32) + self.ring_in[slot, 1, i].astype(F32)
                self.whole[slot, block] = self.finish(s, block, i, total).astype(BF16)
            self.gather_stage(0, s)
        else:
            self.gather_stage(j - 3, s)
            if j == self.last:
                for n in range(8, COPIES):
                    self.sum_copy(n, s).wait_send()


def enter(size):
    me = lax.axis_index('model')
    barrier = pltpu.get_barrier_semaphore()
    for step in range(1, size):
        pl.semaphore_signal(barrier, inc=1, device_id={'model': lax.rem(me + step, size)}, device_id_type=MESH)
    pl.semaphore_wait(barrier, size - 1)


def make_progress(points, sums):
    def progress(t, i):
        for ring, count, lead, start, offsets, consume in sums:
            for j in range(ring.last, 0, -1):
                ahead = start + offsets[j - 1] - i
                if ahead % points:
                    continue
                s = t - lead - ahead // points

                @pl.when(jnp.logical_and(s >= 0, s < count))
                def _(ring=ring, consume=consume, j=j, s=s):
                    ring.stage(j, s)
                    if j == ring.last and consume is not None:
                        consume(s)
    return progress


def norm_stats(x):
    mean = jnp.mean(x, axis=-1, keepdims=True)
    centered = x - mean
    var = jnp.mean(centered * centered, axis=-1, keepdims=True)
    inv = lax.rsqrt(var + NORM_EPS)
    return centered * inv, inv


def norm_back(x, gain, d_normed):
    unit, inv = norm_stats(x)
    d_unit = d_normed * gain
    mean_d = jnp.mean(d_unit, axis=-1, keepdims=True)
    mean_du = jnp.mean(d_unit * unit, axis=-1, keepdims=True)
    return inv * (d_unit - mean_d - unit * mean_du), d_normed * unit


def probs_of(q, k, seg_ref, s, row0, scale):
    keys = k.shape[0]
    seg_q = seg_ref[s, :, pl.ds(row0, Q_ROWS)]
    seg_q = jnp.broadcast_to(seg_q, (Q_ROWS, Q_ROWS)).T[:, :1]
    seg_k = seg_ref[s, :, :keys]
    scores = mt(q, k) * scale
    q_pos = row0 + lax.broadcasted_iota(jnp.int32, scores.shape, 0)
    k_pos = lax.broadcasted_iota(jnp.int32, scores.shape, 1)
    allowed = jnp.logical_and(seg_q == seg_k, q_pos >= k_pos)
    scores = jnp.where(allowed, scores, -1e30)
    e = jnp.exp(scores - jnp.max(scores, axis=-1, keepdims=True))
    return e * (1.0 / jnp.sum(e, axis=-1, keepdims=True))


def head_masks(width, head_dim):
    lane = lax.broadcasted_iota(jnp.int32, (1, width), 1)
    return [jnp.logical_and(lane >= h * head_dim, lane < (h + 1) * head_dim) for h in range(width // head_dim)]


Q_ROWS = 128
OUT_COLS = 256

ORDER = ['B0', 'B1', 'B2', 'B3', 'B4', 'B5', 'B6', 'C0', 'A0', 'C1', 'A1', 'C2', 'A2', 'C3', 'C4', 'A3', 'B7', 'C5',
         'B8', 'C6']
STAGES = {'p1': [10, 17, 23], 'db': [2, 5, 9, 13, 19, 21], 'p2': [2, 6, 14, 23, 33, 35], 'da': [2, 7, 19, 23, 35, 36]}
STARTS = {'p1': 'A3', 'db': 'B5', 'p2': 'B6', 'da': 'C5'}


class Plan:
    def __init__(self):
        self.points = n = len(ORDER)
        self.pos = {tag: i for i, tag in enumerate(ORDER)}
        self.start = {ring: self.pos[tag] for ring, tag in STARTS.items()}
        self.lead = {'A': 0}
        self.lead['B'] = self.after('p1', 'B0')
        self.lead['C'] = self.after('db', 'C0')
        end = {ring: self.step_of(ring, -1) for ring in STAGES}
        own = {ring: self.step_of(ring, 2) for ring in STAGES}
        self.steps = max(end.values())
        self.x_slots = own['da'] + 2
        self.d_slots = max(own['db'], self.lead['B']) - self.lead['B'] + 1
        self.x1_slots = max(own['db'], own['p2']) - end['p1'] + 1
        self.own_slots = own['da'] - own['db'] + 1
        self.a_slots = self.lead['C'] + 1
        self.head_slots = 2 if STAGES['p1'][-1] < n else 3
        assert all(o[-1] < 2 * n for o in STAGES.values())
        assert self.lead['C'] * n + self.pos['C0'] < (self.lead['B'] + 2) * n + self.start['db']

    def ring_lead(self, ring):
        return self.lead[STARTS[ring][0]]

    def end(self, ring, stage=-1):
        return self.ring_lead(ring) * self.points + self.start[ring] + STAGES[ring][stage]

    def step_of(self, ring, stage):
        return self.end(ring, stage) // self.points

    def after(self, ring, tag):
        end = self.end(ring)
        return end // self.points + (0 if self.pos[tag] > end % self.points else 1)


def layer_kernel(size, head_dim, plan, *refs):
    (tok_hbm, dout_hbm, seg_in, gains, w_qkv_in, w_out, w_up, w_down,
     out_hbm, dtok_hbm, dw_qkv_out, dw_out_out, dw_up_out, dw_down_out, dg_out,
     x, d, x1, a, saved, heads, w_qkv, w_out_all, b, pre, d_hid, u, d_pre, d_heads, probs, d_scores, d_qkv,
     dw_qkv, dw_out, dw_up, dw_down, dg_attn, dg_mlp,
     seg, own, dg_parts, x_sem, d_sem, out_sem, dtok_sem, heads_send, heads_recv, wout_send, wout_recv,
     dg_send, dg_recv) = refs[:51]
    ring_db, ring_p2, ring_da = [RingSum(size, *refs[51 + 7 * n:58 + 7 * n]) for n in range(3)]
    count = tok_hbm.shape[0]
    block_rows, hidden = x.shape[2], x.shape[3]
    rows = BLOCKS * block_rows
    half = rows // 2
    width = w_out.shape[0]
    scale = head_dim ** -0.5
    masks = head_masks(width, head_dim)
    me = lax.axis_index('model')
    my_lanes = pl.ds(pl.multiple_of(me * width, width), width)
    gain_attn, gain_mlp = gains.at[0:1], gains.at[1:2]

    def heads_view(slot, core, chip, part):
        lanes = pl.ds(pl.multiple_of((2 * chip + core) * width, width), width)
        span = pl.ds(0, rows) if part is None else pl.ds(part * half, half)
        return heads.at[slot, span, lanes]

    def wout_view(slot, core, chip, part):
        first = (2 * chip + core) * width
        if part is None:
            return w_out_all.at[pl.ds(pl.multiple_of(first, width), width)]
        size_half = width // 2
        return w_out_all.at[pl.ds(pl.multiple_of(first + part * size_half, size_half), size_half)]

    gather_p1 = Gather(size, plan.head_slots, heads_view, heads_send, heads_recv)
    gather_wout = Gather(size, 1, wout_view, wout_send, wout_recv)

    def x_in(s):
        slot = lax.rem(s, plan.x_slots)
        return pltpu.make_async_copy(tok_hbm.at[s], x.at[slot], x_sem.at[slot])

    def d_in(s):
        slot = lax.rem(s, plan.d_slots)
        return pltpu.make_async_copy(dout_hbm.at[s], d.at[slot], d_sem.at[slot])

    def out_copy(s):
        slot = lax.rem(s, SLOTS)
        return pltpu.make_async_copy(ring_p2.whole.at[slot], out_hbm.at[s], out_sem.at[slot])

    def dtok_copy(s):
        slot = lax.rem(s, SLOTS)
        return pltpu.make_async_copy(ring_da.whole.at[slot], dtok_hbm.at[s], dtok_sem.at[slot])

    def rows_sum(v):
        return jnp.sum(v.reshape(v.shape[0] // 8, 8, hidden), axis=0)

    def consume_p1(s):
        x_slot, x1_slot, h_slot = lax.rem(s, plan.x_slots), lax.rem(s, plan.x1_slots), lax.rem(s, plan.head_slots)
        for h in range(2):
            blocks = slice(h * HALF, (h + 1) * HALF)
            for first in range(0, hidden, OUT_COLS):
                cols = slice(first, first + OUT_COLS)
                proj = mm(heads[h_slot, h * half:(h + 1) * half], w_out_all[:, cols]).astype(BF16)
                proj = proj.reshape(HALF, block_rows, OUT_COLS).astype(F32)
                x1[x1_slot, blocks, :, cols] = (x[x_slot, blocks, :, cols].astype(F32) + proj).astype(BF16)

    def finish_db(s, block, i, total):
        x1_slot, d_slot = lax.rem(s, plan.x1_slots), lax.rem(s, plan.d_slots)
        dx, dg = norm_back(x1[x1_slot, block].astype(F32), gain_mlp[...], total)
        dg_mlp[...] += rows_sum(dg)
        d_resid = (d[d_slot, block].astype(F32) + dx).astype(BF16)
        own[lax.rem(s, plan.own_slots), i] = d_resid
        return d_resid

    def finish_p2(s, block, i, total):
        return x1[lax.rem(s, plan.x1_slots), block].astype(F32) + total.astype(BF16).astype(F32)

    def finish_da(s, block, i, total):
        dx, dg = norm_back(x[lax.rem(s, plan.x_slots), block].astype(F32), gain_attn[...], total)
        dg_attn[...] += rows_sum(dg)
        return own[lax.rem(s, plan.own_slots), i].astype(F32) + dx

    ring_db.finish, ring_p2.finish, ring_da.finish = finish_db, finish_p2, finish_da

    def consume_p2(s):
        out_copy(s).start()

    def consume_da(s):
        dtok_copy(s).start()

    def store_part(ring, slot, h, value):
        ring.part[slot, h * HALF:(h + 1) * HALF] = value.astype(BF16).reshape(HALF, block_rows, hidden)

    def norm_in(h, s):
        x_slot, slot = lax.rem(s, plan.x_slots), lax.rem(s, plan.a_slots)
        if h == 0:
            x_in(s).wait()

        def block(i):
            r = h * HALF + i
            unit, _ = norm_stats(x[x_slot, r].astype(F32))
            a[slot, r] = (unit * gain_attn[...]).astype(BF16)
        loop(HALF, block, unroll=2)
        if h == 1:
            saved[slot, :, :3 * width] = mt(a[slot].reshape(rows, hidden), w_qkv[...]).astype(BF16)

    def attend(h, s):
        slot, h_slot = lax.rem(s, plan.a_slots), lax.rem(s, plan.head_slots)
        keys = (h + 1) * half

        def q_block(i):
            row0 = pl.multiple_of(h * half + i * Q_ROWS, Q_ROWS)
            part_rows = pl.ds(row0, Q_ROWS)
            q = saved[slot, part_rows, 0:width]
            k = saved[slot, :keys, width:2 * width]
            v = saved[slot, :keys, 2 * width:3 * width]
            out = None
            for mask in masks:
                p = probs_of(jnp.where(mask, q, 0).astype(BF16), k, seg, s, row0, scale)
                head = mm(p.astype(BF16), v)
                out = head if out is None else jnp.where(mask, head, out)
            out = out.astype(BF16)
            saved[slot, part_rows, 3 * width:4 * width] = out
            heads[h_slot, part_rows, my_lanes] = out
        loop(half // Q_ROWS, q_block, unroll=2)
        if h == 1:
            gather_p1.stage(0, s)

    def norm_mid(h, s):
        x1_slot = lax.rem(s, plan.x1_slots)

        def block(i):
            r = h * HALF + i
            unit, _ = norm_stats(x1[x1_slot, r].astype(F32))
            b[r] = (unit * gain_mlp[...]).astype(BF16)
        loop(HALF, block, unroll=2)

    def up(s):
        pre[...] = mm(b[...].reshape(rows, hidden), w_up[...])

    def gelu_both(h, s):
        if h == 0:
            d_in(s).wait()
            d_hid[...] = mt(d[lax.rem(s, plan.d_slots)].reshape(rows, hidden), w_down[...]).astype(BF16)

        def block(i):
            part_rows = pl.ds(pl.multiple_of(h * half + i * block_rows, block_rows), block_rows)
            v = pre[part_rows]
            v2 = v * v
            c = 0.7978845608028654
            th = jnp.tanh(c * (v + 0.044715 * (v * v2)))
            u[part_rows] = (0.5 * v * (1.0 + th)).astype(BF16)
            slope = 0.5 * (1.0 + th) + 0.5 * v * (1.0 - th * th) * (c * (1.0 + 3.0 * 0.044715 * v2))
            d_pre[part_rows] = (d_hid[part_rows].astype(F32) * slope).astype(BF16)
        loop(HALF, block, unroll=2)

    def grad_b(s):
        for h in range(2):
            store_part(ring_db, lax.rem(s, SLOTS), h, mt(d_pre[h * half:(h + 1) * half], w_up[...]))
        ring_db.stage(0, s)

    def down(s):
        @pl.when(s >= SLOTS)
        def _():
            out_copy(s - SLOTS).wait()
        for h in range(2):
            store_part(ring_p2, lax.rem(s, SLOTS), h, mm(u[h * half:(h + 1) * half], w_down[...]))
        ring_p2.stage(0, s)

    def grad_up(s):
        dw_up[...] += tm(b[...].reshape(rows, hidden), d_pre[...])

    def grad_down(s):
        dw_down[...] += tm(u[...], d[lax.rem(s, plan.d_slots)].reshape(rows, hidden))

    def grad_heads(s):
        d_rows = ring_db.whole[lax.rem(s, SLOTS)].reshape(rows, hidden)
        d_heads[...] = mt(d_rows, w_out[...]).astype(BF16)
        dw_out[...] += tm(saved[lax.rem(s, plan.a_slots), :, 3 * width:4 * width], d_rows)

    def attend_back(head, s):
        mask = masks[head]
        slot = lax.rem(s, plan.a_slots)
        for h in range(2):
            keys = (h + 1) * half

            def q_block(i):
                row0 = pl.multiple_of(h * half + i * Q_ROWS, Q_ROWS)
                part_rows = pl.ds(row0, Q_ROWS)
                q = jnp.where(mask, saved[slot, part_rows, 0:width], 0).astype(BF16)
                d_head = jnp.where(mask, d_heads[part_rows], 0).astype(BF16)
                p = probs_of(q, saved[slot, :keys, width:2 * width], seg, s, row0, scale)
                d_p = mt(d_head, saved[slot, :keys, 2 * width:3 * width])
                row_dot = jnp.sum(d_p * p, axis=-1, keepdims=True)
                probs[part_rows, :keys] = p.astype(BF16)
                d_scores[part_rows, :keys] = (p * (d_p - row_dot) * scale).astype(BF16)
            loop(half // Q_ROWS, q_block, unroll=2)

    def head_grads(head, s):
        mask = masks[head]
        slot = lax.rem(s, plan.a_slots)
        d_q = mm(d_scores[...], saved[slot, :, width:2 * width]).astype(BF16)
        d_k = tm(d_scores[...], saved[slot, :, 0:width]).astype(BF16)
        d_v = tm(probs[...], d_heads[...]).astype(BF16)
        for j, value in enumerate((d_q, d_k, d_v)):
            cols = slice(j * width, (j + 1) * width)
            d_qkv[:, cols] = value if head == 0 else jnp.where(mask, value, d_qkv[:, cols])

    def grad_a(s):
        @pl.when(s >= SLOTS)
        def _():
            dtok_copy(s - SLOTS).wait()
        for h in range(2):
            store_part(ring_da, lax.rem(s, SLOTS), h, mm(d_qkv[h * half:(h + 1) * half], w_qkv[...]))
        ring_da.stage(0, s)

    def grad_qkv(s):
        dw_qkv[...] += tm(d_qkv[...], a[lax.rem(s, plan.a_slots)].reshape(rows, hidden))

    def with_h(fn, h):
        return functools.partial(fn, h)

    work = {'A': [with_h(norm_in, 0), with_h(norm_in, 1), with_h(attend, 0), with_h(attend, 1)],
            'B': [with_h(norm_mid, 0), with_h(norm_mid, 1), up, with_h(gelu_both, 0), with_h(gelu_both, 1), grad_b, down,
                  grad_up, grad_down],
            'C': [grad_heads, with_h(attend_back, 0), with_h(head_grads, 0),
                  with_h(attend_back, 1), with_h(head_grads, 1), grad_a, grad_qkv]}
    assert sum(len(v) for v in work.values()) == plan.points
    first = plan.start['p1']
    progress = make_progress(plan.points, [(gather_wout, 1, 0, 0, [first + 1, first + 4, first + 7], None)] + [
        (ring, count, plan.ring_lead(name), plan.start[name], STAGES[name], consume) for name, ring, consume in (
            ('p1', gather_p1, consume_p1), ('db', ring_db, None), ('p2', ring_p2, consume_p2), ('da', ring_da, consume_da))])

    x_in(0).start()
    for s in range(count):
        seg[s] = seg_in[s:s + 1]
    w_out_all[my_rows(me, width)] = w_out[...]
    enter(size)
    gather_wout.stage(0, 0)
    for n in range(w_qkv_in.shape[0]):
        for j in range(3):
            at = (j * w_qkv_in.shape[0] + n) * head_dim
            w_qkv[at:at + head_dim] = w_qkv_in[n, j]
    for ref in (dw_qkv, dw_out, dw_up, dw_down, dg_attn, dg_mlp, probs, d_scores):
        ref[...] = jnp.zeros_like(ref)

    def step(t):
        @pl.when(t + 1 < count)
        def _():
            x_in(t + 1).start()
        s_mid = t - plan.lead['B']

        @pl.when(jnp.logical_and(s_mid >= 0, s_mid < count))
        def _():
            d_in(s_mid).start()
        for i, tag in enumerate(ORDER):
            s = t - plan.lead[tag[0]]

            @pl.when(jnp.logical_and(s >= 0, s < count))
            def _(fn=work[tag[0]][int(tag[1:])], s=s):
                fn(s)
            progress(t, i)

    loop(count + plan.steps, step)
    dg_parts[me, 0:1] = jnp.sum(dg_attn[...], axis=0, keepdims=True)
    dg_parts[me, 1:2] = jnp.sum(dg_mlp[...], axis=0, keepdims=True)

    def dg_copy(step, owner):
        return pltpu.make_async_remote_copy(
            src_ref=dg_parts.at[owner], dst_ref=dg_parts.at[owner], send_sem=dg_send.at[step], recv_sem=dg_recv.at[step],
            device_id={'model': lax.rem(me + step, size)}, device_id_type=MESH)

    for step_ahead in range(1, size):
        dg_copy(step_ahead, me).start()
    for acc, out in ((dw_out, dw_out_out), (dw_up, dw_up_out), (dw_down, dw_down_out)):
        out[...] = acc[...].astype(BF16)
    for n in range(w_qkv_in.shape[0]):
        for j in range(3):
            at = (j * w_qkv_in.shape[0] + n) * head_dim
            dw_qkv_out[n, j] = dw_qkv[at:at + head_dim].astype(BF16)
    for step_ahead in range(1, size):
        dg_copy(step_ahead, lax.rem(me + size - step_ahead, size)).wait_recv()
    dg_out[...] = sum(dg_parts[owner] for owner in range(size))
    for step_ahead in range(1, size):
        dg_copy(step_ahead, me).wait_send()
    for s in range(count - SLOTS, count):
        out_copy(s).wait()
        dtok_copy(s).wait()


def my_rows(me, width):
    return pl.ds(pl.multiple_of(me * width, width), width)


def publish_kernel(count, *refs):
    n = len(refs) // 5
    ins, outs, held, in_sems, out_sems = (refs[k * n:(k + 1) * n] for k in range(5))

    def moves(i):
        if i >= count:
            yield (pltpu.make_async_copy(ins[i], held[i], in_sems[i].at[0]),
                   pltpu.make_async_copy(held[i], outs[i], out_sems[i].at[0]))
            return
        for r in range(ins[i].shape[0]):
            yield (pltpu.make_async_copy(ins[i].at[r], held[i].at[r], in_sems[i].at[r]),
                   pltpu.make_async_copy(held[i].at[r], outs[i].at[r], out_sems[i].at[r]))
    pairs = [pair for i in range(n) for pair in moves(i)]
    for into, _ in pairs:
        into.start()
    for into, out in pairs:
        into.wait()
        out.start()
    for _, out in pairs:
        out.wait()


def publish(values, split):
    sems = [pltpu.SemaphoreType.DMA((v.shape[0] if i < split else 1,)) for i, v in enumerate(values)]
    return pl.pallas_call(
        functools.partial(publish_kernel, split),
        out_shape=[jax.ShapeDtypeStruct(v.shape, v.dtype) for v in values],
        in_specs=[pl.BlockSpec(memory_space=pl.ANY)] * len(values),
        out_specs=[pl.BlockSpec(memory_space=pl.ANY)] * len(values),
        scratch_shapes=[pltpu.VMEM(v.shape, v.dtype) for v in values] + sems + sems,
        compiler_params=pltpu.CompilerParams(vmem_limit_bytes=VMEM_LIMIT),
        name='publish',
    )(*values)


def ring_buffers(block_rows, hidden):
    return [
        pltpu.VMEM((SLOTS, BLOCKS, block_rows, hidden), BF16),
        pltpu.VMEM((SLOTS, HALF, block_rows, hidden), BF16),
        pltpu.VMEM((SLOTS, 2, block_rows, hidden), BF16),
        pltpu.VMEM((SLOTS, 2, PIECE, block_rows, hidden), BF16),
        pltpu.VMEM((SLOTS, BLOCKS, block_rows, hidden), BF16),
    ]


def ring_sems():
    return [pltpu.SemaphoreType.DMA((SLOTS, COPIES)), pltpu.SemaphoreType.DMA((SLOTS, COPIES))]


def run_kernel(kernel, ident, outs, out_vmem, args, in_vmem, scratch):
    def spec(in_vmem):
        return pl.BlockSpec(memory_space=pltpu.VMEM if in_vmem else pl.ANY)
    return pl.pallas_call(
        kernel,
        out_shape=[jax.ShapeDtypeStruct(s, t) for s, t in outs],
        in_specs=[spec(v) for v in in_vmem],
        out_specs=[spec(v) for v in out_vmem],
        scratch_shapes=scratch,
        compiler_params=pltpu.CompilerParams(collective_id=ident, has_side_effects=True, vmem_limit_bytes=VMEM_LIMIT),
        name=f'layer_part_{ident}',
    )(*args)


def solution(mesh):
    size = mesh.shape['model']
    dma = pltpu.SemaphoreType.DMA

    def device_step(tokens, seg_ids, d_out, gain_attn, gain_mlp, w_qkv, w_out, w_up, w_down):
        count, seq_len, hidden = tokens.shape
        heads, head_dim = w_qkv.shape[1], w_qkv.shape[3]
        width = heads * head_dim
        inner = w_up.shape[1]
        block_rows = seq_len // BLOCKS
        act = (count, BLOCKS, block_rows, hidden)
        one = (BLOCKS, block_rows, hidden)
        x = tokens.reshape(act)
        d = d_out.reshape(act)
        gains = jnp.stack([gain_attn, gain_mlp]).astype(F32)
        wqkv = w_qkv.transpose(1, 2, 3, 0)
        wout = w_out.reshape(width, hidden)
        plan = Plan()

        outs = [(act, BF16), (act, BF16), (wqkv.shape, BF16), ((width, hidden), BF16),
                ((hidden, inner), BF16), ((inner, hidden), BF16), ((2, hidden), F32)]
        scratch = [pltpu.VMEM(shape, kind) for shape, kind in (
            ((plan.x_slots,) + one, BF16), ((plan.d_slots,) + one, BF16), ((plan.x1_slots,) + one, BF16),
            ((plan.a_slots,) + one, BF16), ((plan.a_slots, seq_len, 4 * width), BF16),
            ((plan.head_slots, seq_len, size * width), BF16), ((3 * width, hidden), BF16), ((size * width, hidden), BF16),
            (one, BF16), ((seq_len, inner), F32), ((seq_len, inner), BF16),
            ((seq_len, inner), BF16), ((seq_len, inner), BF16), ((seq_len, width), BF16),
            ((seq_len, seq_len), BF16), ((seq_len, seq_len), BF16), ((seq_len, 3 * width), BF16),
            ((3 * width, hidden), F32), ((width, hidden), F32), ((hidden, inner), F32), ((inner, hidden), F32),
            ((8, hidden), F32), ((8, hidden), F32), ((count, 1, seq_len), jnp.int32),
            ((plan.own_slots, PIECE, block_rows, hidden), BF16), ((size, 2, hidden), F32))]
        scratch += [dma((plan.x_slots,)), dma((plan.d_slots,)), dma((SLOTS,)), dma((SLOTS,))]
        scratch += [dma((plan.head_slots, 8))] * 2 + [dma((1, 8))] * 2 + [dma((size,))] * 2
        for _ in range(3):
            scratch += ring_buffers(block_rows, hidden) + ring_sems()
        results = run_kernel(
            functools.partial(layer_kernel, size, head_dim, plan), 1, outs, [False] * 2 + [True] * 5,
            [x, d, seg_ids, gains, wqkv, wout, w_up, w_down], [False] * 2 + [True] * 6, scratch)
        layer_out, d_tokens, dw_qkv, dw_out, d_w_up, d_w_down, dg = publish(results, 2)

        return (layer_out.reshape(tokens.shape), d_tokens.reshape(tokens.shape), dw_qkv.transpose(3, 0, 1, 2),
                dw_out.reshape(w_out.shape), d_w_up, d_w_down, dg[0], dg[1])

    in_specs = (P('data', None, None), P('data', None), P('data', None, None), P(), P(), P(None, 'model', None, None), P('model', None, None), P(None, 'model'), P('model', None))
    out_specs = (P('data', None, None), P('data', None, None), P('data', 'model', None, None), P(('data', 'model'), None, None), P('data', 'model'), P(('data', 'model'), None), P('data'), P('data'))
    return jax.shard_map(device_step, mesh=mesh, in_specs=in_specs, out_specs=out_specs, check_vma=False)
```

```python
import functools
import jax
import jax.numpy as jnp
from jax import lax
from jax.experimental import pallas as pl
from jax.experimental.pallas import tpu as pltpu
from jax.sharding import PartitionSpec as P

NORM_EPS = 1e-5
MESH = pl.DeviceIdType.MESH
F32 = jnp.float32
BF16 = jnp.bfloat16
SLOTS = 2
BLOCKS = 16
HALF = BLOCKS // 2
PIECE = 2
COPIES = 13
VMEM_LIMIT = 66 * 1000 * 1000


def mm(a, b):
    return lax.dot_general(a, b, (((1,), (0,)), ((), ())), preferred_element_type=F32)


def mt(a, b):
    return lax.dot_general(a, b, (((1,), (1,)), ((), ())), preferred_element_type=F32)


def tm(a, b):
    return lax.dot_general(a, b, (((0,), (0,)), ((), ())), preferred_element_type=F32)


def loop(count, body, unroll=1):
    def step(i, carry):
        body(i)
        return carry
    lax.fori_loop(0, count, step, 0, unroll=unroll)


class Gather:
    first, last = 0, 3

    def __init__(self, size, slots, view, send, recv):
        me = lax.axis_index('model')
        self.core = lax.rem(me, 2)
        self.chips = size // 2
        self.chip = me // 2
        self.right = lax.rem(me + 2, size)
        self.left = lax.rem(me + size - 2, size)
        self.partner = me + 1 - 2 * self.core
        self.slots, self.view, self.send, self.recv = slots, view, send, recv

    def at(self, slot, step, part=None):
        return self.view(slot, self.core, lax.rem(self.chip + step, self.chips), part)

    def remote(self, slot, n, src, dst, to):
        return pltpu.make_async_remote_copy(
            src_ref=src, dst_ref=dst, send_sem=self.send.at[slot, n], recv_sem=self.recv.at[slot, n],
            device_id={'model': to}, device_id_type=MESH)

    def copy(self, n, s):
        slot = lax.rem(s, self.slots)
        behind = self.chips - 1
        step, part, to = [(0, None, self.right), (0, None, self.left), (0, None, self.partner),
                          (behind, 0, self.right), (1, 1, self.left), (behind, None, self.partner),
                          (1, None, self.partner), (2, None, self.partner)][n]
        ref = self.at(slot, step, part)
        return self.remote(slot, n, ref, ref, to)

    def gather_stage(self, j, s):
        if j == 0:
            starts, waits = (0, 1, 2), ()
        elif j == 1:
            starts, waits = (3, 4, 5, 6), (0, 1)
        elif j == 2:
            starts, waits = (7,), (3, 4)
        else:
            starts, waits = (), (2, 5, 6, 7)
        for n in waits:
            self.copy(n, s).wait_recv()
        for n in starts:
            self.copy(n, s).start()
        if j == 3:
            for n in range(8):
                self.copy(n, s).wait_send()

    def stage(self, j, s):
        self.gather_stage(j, s)


class RingSum(Gather):
    last = 6

    def __init__(self, size, part, pair_in, relay_in, ring_in, whole, send, recv):
        self.part, self.pair_in, self.relay_in, self.ring_in, self.whole = part, pair_in, relay_in, ring_in, whole
        self.finish = None
        super().__init__(size, SLOTS, self.block_view, send, recv)

    def block_view(self, slot, core, chip, part):
        start = core * HALF + chip * PIECE
        if part is None:
            return self.whole.at[slot, pl.ds(start, PIECE)]
        return self.whole.at[slot, pl.ds(start + part, 1)]

    def base(self, step):
        return self.core * HALF + lax.rem(self.chip + step, self.chips) * PIECE

    def sum_copy(self, n, s):
        slot = lax.rem(s, SLOTS)
        part = self.part.at[slot]
        if n == 8:
            src, dst, to = part.at[pl.ds((1 - self.core) * HALF, HALF)], self.pair_in.at[slot], self.partner
        elif n == 9:
            src, dst, to = part.at[pl.ds(self.base(2), 1)], self.relay_in.at[slot, pl.ds(0, 1)], self.right
        elif n == 10:
            src, dst, to = part.at[pl.ds(self.base(2) + 1, 1)], self.relay_in.at[slot, pl.ds(1, 1)], self.left
        elif n == 11:
            src, dst, to = part.at[pl.ds(self.base(1), PIECE)], self.ring_in.at[slot, 0], self.right
        else:
            src, dst, to = part.at[pl.ds(self.base(self.chips - 1), PIECE)], self.ring_in.at[slot, 1], self.left
        return self.remote(slot, n, src, dst, to)

    def add(self, slot, block, others):
        total = self.part[slot, block].astype(F32)
        for ref in others:
            total = total + ref.astype(F32)
        return total.astype(BF16)

    def stage(self, j, s):
        slot = lax.rem(s, SLOTS)
        if j == 0:
            self.sum_copy(8, s).start()
        elif j == 1:
            self.sum_copy(8, s).wait_recv()

            def pair(i):
                at = lax.rem(lax.rem(self.chip + 2, self.chips) * PIECE + i, HALF)
                block = self.core * HALF + at
                self.part[slot, block] = self.add(slot, block, [self.pair_in[slot, at]])
            loop(HALF, pair, unroll=4)
            self.sum_copy(9, s).start()
            self.sum_copy(10, s).start()
        elif j == 2:
            self.sum_copy(9, s).wait_recv()
            self.sum_copy(10, s).wait_recv()
            first, second = self.base(1), self.base(self.chips - 1) + 1
            self.part[slot, first] = self.add(slot, first, [self.relay_in[slot, 0]])
            self.part[slot, second] = self.add(slot, second, [self.relay_in[slot, 1]])
            self.sum_copy(11, s).start()
            self.sum_copy(12, s).start()
        elif j == 3:
            self.sum_copy(11, s).wait_recv()
            self.sum_copy(12, s).wait_recv()
            for i in range(PIECE):
                block = self.base(0) + i
                total = self.part[slot, block].astype(F32)
                total = total + self.ring_in[slot, 0, i].astype(F32) + self.ring_in[slot, 1, i].astype(F32)
                self.whole[slot, block] = self.finish(s, block, i, total).astype(BF16)
            self.gather_stage(0, s)
        else:
            self.gather_stage(j - 3, s)
            if j == self.last:
                for n in range(8, COPIES):
                    self.sum_copy(n, s).wait_send()


def enter(size):
    me = lax.axis_index('model')
    barrier = pltpu.get_barrier_semaphore()
    for step in range(1, size):
        pl.semaphore_signal(barrier, inc=1, device_id={'model': lax.rem(me + step, size)}, device_id_type=MESH)
    pl.semaphore_wait(barrier, size - 1)


def make_progress(points, sums):
    def progress(t, i):
        for ring, count, lead, start, offsets, consume in sums:
            for j in range(ring.last, 0, -1):
                ahead = start + offsets[j - 1] - i
                if ahead % points:
                    continue
                s = t - lead - ahead // points

                @pl.when(jnp.logical_and(s >= 0, s < count))
                def _(ring=ring, consume=consume, j=j, s=s):
                    ring.stage(j, s)
                    if j == ring.last and consume is not None:
                        consume(s)
    return progress


def norm_stats(x):
    mean = jnp.mean(x, axis=-1, keepdims=True)
    centered = x - mean
    var = jnp.mean(centered * centered, axis=-1, keepdims=True)
    inv = lax.rsqrt(var + NORM_EPS)
    return centered * inv, inv


def norm_back(x, gain, d_normed):
    unit, inv = norm_stats(x)
    d_unit = d_normed * gain
    mean_d = jnp.mean(d_unit, axis=-1, keepdims=True)
    mean_du = jnp.mean(d_unit * unit, axis=-1, keepdims=True)
    return inv * (d_unit - mean_d - unit * mean_du), d_normed * unit


def probs_of(q, k, seg_ref, s, row0, scale):
    keys = k.shape[0]
    seg_q = seg_ref[s, :, pl.ds(row0, Q_ROWS)]
    seg_q = jnp.broadcast_to(seg_q, (Q_ROWS, Q_ROWS)).T[:, :1]
    seg_k = seg_ref[s, :, :keys]
    scores = mt(q, k) * scale
    q_pos = row0 + lax.broadcasted_iota(jnp.int32, scores.shape, 0)
    k_pos = lax.broadcasted_iota(jnp.int32, scores.shape, 1)
    allowed = jnp.logical_and(seg_q == seg_k, q_pos >= k_pos)
    scores = jnp.where(allowed, scores, -1e30)
    e = jnp.exp(scores - jnp.max(scores, axis=-1, keepdims=True))
    return e * (1.0 / jnp.sum(e, axis=-1, keepdims=True))


def head_masks(width, head_dim):
    lane = lax.broadcasted_iota(jnp.int32, (1, width), 1)
    return [jnp.logical_and(lane >= h * head_dim, lane < (h + 1) * head_dim) for h in range(width // head_dim)]


Q_ROWS = 128
OUT_COLS = 256

ORDER = ['B0', 'B1', 'B2', 'B3', 'B4', 'B5', 'B6', 'C0', 'A0', 'C1', 'A1', 'C2', 'A2', 'C3', 'C4', 'A3', 'B7', 'C5',
         'B8', 'C6']
STAGES = {'p1': [10, 17, 23], 'db': [2, 5, 9, 13, 19, 21], 'p2': [2, 6, 14, 23, 33, 35], 'da': [2, 7, 19, 23, 35, 36]}
STARTS = {'p1': 'A3', 'db': 'B5', 'p2': 'B6', 'da': 'C5'}


class Plan:
    def __init__(self):
        self.points = n = len(ORDER)
        self.pos = {tag: i for i, tag in enumerate(ORDER)}
        self.start = {ring: self.pos[tag] for ring, tag in STARTS.items()}
        self.lead = {'A': 0}
        self.lead['B'] = self.after('p1', 'B0')
        self.lead['C'] = self.after('db', 'C0')
        end = {ring: self.step_of(ring, -1) for ring in STAGES}
        own = {ring: self.step_of(ring, 2) for ring in STAGES}
        self.steps = max(end.values())
        self.x_slots = own['da'] + 2
        self.d_slots = max(own['db'], self.lead['B']) - self.lead['B'] + 1
        self.x1_slots = max(own['db'], own['p2']) - end['p1'] + 1
        self.own_slots = own['da'] - own['db'] + 1
        self.a_slots = self.lead['C'] + 1
        self.head_slots = 2 if STAGES['p1'][-1] < n else 3
        assert all(o[-1] < 2 * n for o in STAGES.values())
        assert self.lead['C'] * n + self.pos['C0'] < (self.lead['B'] + 2) * n + self.start['db']

    def ring_lead(self, ring):
        return self.lead[STARTS[ring][0]]

    def end(self, ring, stage=-1):
        return self.ring_lead(ring) * self.points + self.start[ring] + STAGES[ring][stage]

    def step_of(self, ring, stage):
        return self.end(ring, stage) // self.points

    def after(self, ring, tag):
        end = self.end(ring)
        return end // self.points + (0 if self.pos[tag] > end % self.points else 1)


def layer_kernel(size, head_dim, plan, *refs):
    (tok_hbm, dout_hbm, seg_in, gains, w_qkv_in, w_out, w_up, w_down,
     out_hbm, dtok_hbm, dw_qkv_out, dw_out_out, dw_up_out, dw_down_out, dg_out,
     x, d, x1, a, saved, heads, w_qkv, w_out_all, b, pre, d_hid, u, d_pre, d_heads, probs, d_scores, d_qkv,
     dw_qkv, dw_out, dw_up, dw_down, dg_attn, dg_mlp,
     seg, own, dg_parts, x_sem, d_sem, out_sem, dtok_sem, heads_send, heads_recv, wout_send, wout_recv,
     dg_send, dg_recv) = refs[:51]
    ring_db, ring_p2, ring_da = [RingSum(size, *refs[51 + 7 * n:58 + 7 * n]) for n in range(3)]
    count = tok_hbm.shape[0]
    block_rows, hidden = x.shape[2], x.shape[3]
    rows = BLOCKS * block_rows
    half = rows // 2
    width = w_out.shape[0]
    scale = head_dim ** -0.5
    masks = head_masks(width, head_dim)
    me = lax.axis_index('model')
    my_lanes = pl.ds(pl.multiple_of(me * width, width), width)
    gain_attn, gain_mlp = gains.at[0:1], gains.at[1:2]

    def heads_view(slot, core, chip, part):
        lanes = pl.ds(pl.multiple_of((2 * chip + core) * width, width), width)
        span = pl.ds(0, rows) if part is None else pl.ds(part * half, half)
        return heads.at[slot, span, lanes]

    def wout_view(slot, core, chip, part):
        first = (2 * chip + core) * width
        if part is None:
            return w_out_all.at[pl.ds(pl.multiple_of(first, width), width)]
        size_half = width // 2
        return w_out_all.at[pl.ds(pl.multiple_of(first + part * size_half, size_half), size_half)]

    gather_p1 = Gather(size, plan.head_slots, heads_view, heads_send, heads_recv)
    gather_wout = Gather(size, 1, wout_view, wout_send, wout_recv)

    def x_in(s):
        slot = lax.rem(s, plan.x_slots)
        return pltpu.make_async_copy(tok_hbm.at[s], x.at[slot], x_sem.at[slot])

    def d_in(s):
        slot = lax.rem(s, plan.d_slots)
        return pltpu.make_async_copy(dout_hbm.at[s], d.at[slot], d_sem.at[slot])

    def out_copy(s):
        slot = lax.rem(s, SLOTS)
        return pltpu.make_async_copy(ring_p2.whole.at[slot], out_hbm.at[s], out_sem.at[slot])

    def dtok_copy(s):
        slot = lax.rem(s, SLOTS)
        return pltpu.make_async_copy(ring_da.whole.at[slot], dtok_hbm.at[s], dtok_sem.at[slot])

    def rows_sum(v):
        return jnp.sum(v.reshape(v.shape[0] // 8, 8, hidden), axis=0)

    def consume_p1(s):
        x_slot, x1_slot, h_slot = lax.rem(s, plan.x_slots), lax.rem(s, plan.x1_slots), lax.rem(s, plan.head_slots)
        for h in range(2):
            blocks = slice(h * HALF, (h + 1) * HALF)
            for first in range(0, hidden, OUT_COLS):
                cols = slice(first, first + OUT_COLS)
                proj = mm(heads[h_slot, h * half:(h + 1) * half], w_out_all[:, cols]).astype(BF16)
                proj = proj.reshape(HALF, block_rows, OUT_COLS).astype(F32)
                x1[x1_slot, blocks, :, cols] = (x[x_slot, blocks, :, cols].astype(F32) + proj).astype(BF16)

    def finish_db(s, block, i, total):
        x1_slot, d_slot = lax.rem(s, plan.x1_slots), lax.rem(s, plan.d_slots)
        dx, dg = norm_back(x1[x1_slot, block].astype(F32), gain_mlp[...], total)
        dg_mlp[...] += rows_sum(dg)
        d_resid = (d[d_slot, block].astype(F32) + dx).astype(BF16)
        own[lax.rem(s, plan.own_slots), i] = d_resid
        return d_resid

    def finish_p2(s, block, i, total):
        return x1[lax.rem(s, plan.x1_slots), block].astype(F32) + total.astype(BF16).astype(F32)

    def finish_da(s, block, i, total):
        dx, dg = norm_back(x[lax.rem(s, plan.x_slots), block].astype(F32), gain_attn[...], total)
        dg_attn[...] += rows_sum(dg)
        return own[lax.rem(s, plan.own_slots), i].astype(F32) + dx

    ring_db.finish, ring_p2.finish, ring_da.finish = finish_db, finish_p2, finish_da

    def consume_p2(s):
        out_copy(s).start()

    def consume_da(s):
        dtok_copy(s).start()

    def store_part(ring, slot, h, value):
        ring.part[slot, h * HALF:(h + 1) * HALF] = value.astype(BF16).reshape(HALF, block_rows, hidden)

    def norm_in(h, s):
        x_slot, slot = lax.rem(s, plan.x_slots), lax.rem(s, plan.a_slots)
        if h == 0:
            x_in(s).wait()

        def block(i):
            r = h * HALF + i
            unit, _ = norm_stats(x[x_slot, r].astype(F32))
            a[slot, r] = (unit * gain_attn[...]).astype(BF16)
        loop(HALF, block, unroll=8)
        if h == 1:
            saved[slot, :, :3 * width] = mt(a[slot].reshape(rows, hidden), w_qkv[...]).astype(BF16)

    def attend(h, s):
        slot, h_slot = lax.rem(s, plan.a_slots), lax.rem(s, plan.head_slots)
        keys = (h + 1) * half

        def q_block(i):
            row0 = pl.multiple_of(h * half + i * Q_ROWS, Q_ROWS)
            part_rows = pl.ds(row0, Q_ROWS)
            q = saved[slot, part_rows, 0:width]
            k = saved[slot, :keys, width:2 * width]
            v = saved[slot, :keys, 2 * width:3 * width]
            out = None
            for mask in masks:
                p = probs_of(jnp.where(mask, q, 0).astype(BF16), k, seg, s, row0, scale)
                head = mm(p.astype(BF16), v)
                out = head if out is None else jnp.where(mask, head, out)
            out = out.astype(BF16)
            saved[slot, part_rows, 3 * width:4 * width] = out
            heads[h_slot, part_rows, my_lanes] = out
        loop(half // Q_ROWS, q_block, unroll=2)
        if h == 1:
            gather_p1.stage(0, s)

    def norm_mid(h, s):
        x1_slot = lax.rem(s, plan.x1_slots)

        def block(i):
            r = h * HALF + i
            unit, _ = norm_stats(x1[x1_slot, r].astype(F32))
            b[r] = (unit * gain_mlp[...]).astype(BF16)
        loop(HALF, block, unroll=8)

    def up(s):
        pre[...] = mm(b[...].reshape(rows, hidden), w_up[...])

    def gelu_both(h, s):
        if h == 0:
            d_in(s).wait()
            d_hid[...] = mt(d[lax.rem(s, plan.d_slots)].reshape(rows, hidden), w_down[...]).astype(BF16)

        def block(i):
            part_rows = pl.ds(pl.multiple_of(h * half + i * block_rows, block_rows), block_rows)
            v = pre[part_rows]
            v2 = v * v
            c = 0.7978845608028654
            th = jnp.tanh(c * (v + 0.044715 * (v * v2)))
            u[part_rows] = (0.5 * v * (1.0 + th)).astype(BF16)
            slope = 0.5 * (1.0 + th) + 0.5 * v * (1.0 - th * th) * (c * (1.0 + 3.0 * 0.044715 * v2))
            d_pre[part_rows] = (d_hid[part_rows].astype(F32) * slope).astype(BF16)
        loop(HALF, block, unroll=8)

    def grad_b(s):
        for h in range(2):
            store_part(ring_db, lax.rem(s, SLOTS), h, mt(d_pre[h * half:(h + 1) * half], w_up[...]))
        ring_db.stage(0, s)

    def down(s):
        @pl.when(s >= SLOTS)
        def _():
            out_copy(s - SLOTS).wait()
        for h in range(2):
            store_part(ring_p2, lax.rem(s, SLOTS), h, mm(u[h * half:(h + 1) * half], w_down[...]))
        ring_p2.stage(0, s)

    def grad_up(s):
        dw_up[...] += tm(b[...].reshape(rows, hidden), d_pre[...])

    def grad_down(s):
        dw_down[...] += tm(u[...], d[lax.rem(s, plan.d_slots)].reshape(rows, hidden))

    def grad_heads(s):
        d_rows = ring_db.whole[lax.rem(s, SLOTS)].reshape(rows, hidden)
        d_heads[...] = mt(d_rows, w_out[...]).astype(BF16)
        dw_out[...] += tm(saved[lax.rem(s, plan.a_slots), :, 3 * width:4 * width], d_rows)

    def attend_back(head, s):
        mask = masks[head]
        slot = lax.rem(s, plan.a_slots)
        for h in range(2):
            keys = (h + 1) * half

            def q_block(i):
                row0 = pl.multiple_of(h * half + i * Q_ROWS, Q_ROWS)
                part_rows = pl.ds(row0, Q_ROWS)
                q = jnp.where(mask, saved[slot, part_rows, 0:width], 0).astype(BF16)
                d_head = jnp.where(mask, d_heads[part_rows], 0).astype(BF16)
                p = probs_of(q, saved[slot, :keys, width:2 * width], seg, s, row0, scale)
                d_p = mt(d_head, saved[slot, :keys, 2 * width:3 * width])
                row_dot = jnp.sum(d_p * p, axis=-1, keepdims=True)
                probs[part_rows, :keys] = p.astype(BF16)
                d_scores[part_rows, :keys] = (p * (d_p - row_dot) * scale).astype(BF16)
            loop(half // Q_ROWS, q_block, unroll=2)

    def head_grads(head, s):
        mask = masks[head]
        slot = lax.rem(s, plan.a_slots)
        d_q = mm(d_scores[...], saved[slot, :, width:2 * width]).astype(BF16)
        d_k = tm(d_scores[...], saved[slot, :, 0:width]).astype(BF16)
        d_v = tm(probs[...], d_heads[...]).astype(BF16)
        for j, value in enumerate((d_q, d_k, d_v)):
            cols = slice(j * width, (j + 1) * width)
            d_qkv[:, cols] = value if head == 0 else jnp.where(mask, value, d_qkv[:, cols])

    def grad_a(s):
        @pl.when(s >= SLOTS)
        def _():
            dtok_copy(s - SLOTS).wait()
        for h in range(2):
            store_part(ring_da, lax.rem(s, SLOTS), h, mm(d_qkv[h * half:(h + 1) * half], w_qkv[...]))
        ring_da.stage(0, s)

    def grad_qkv(s):
        dw_qkv[...] += tm(d_qkv[...], a[lax.rem(s, plan.a_slots)].reshape(rows, hidden))

    def with_h(fn, h):
        return functools.partial(fn, h)

    work = {'A': [with_h(norm_in, 0), with_h(norm_in, 1), with_h(attend, 0), with_h(attend, 1)],
            'B': [with_h(norm_mid, 0), with_h(norm_mid, 1), up, with_h(gelu_both, 0), with_h(gelu_both, 1), grad_b, down,
                  grad_up, grad_down],
            'C': [grad_heads, with_h(attend_back, 0), with_h(head_grads, 0),
                  with_h(attend_back, 1), with_h(head_grads, 1), grad_a, grad_qkv]}
    assert sum(len(v) for v in work.values()) == plan.points
    first = plan.start['p1']
    progress = make_progress(plan.points, [(gather_wout, 1, 0, 0, [first + 1, first + 4, first + 7], None)] + [
        (ring, count, plan.ring_lead(name), plan.start[name], STAGES[name], consume) for name, ring, consume in (
            ('p1', gather_p1, consume_p1), ('db', ring_db, None), ('p2', ring_p2, consume_p2), ('da', ring_da, consume_da))])

    x_in(0).start()
    for s in range(count):
        seg[s] = seg_in[s:s + 1]
    w_out_all[my_rows(me, width)] = w_out[...]
    enter(size)
    gather_wout.stage(0, 0)
    for n in range(w_qkv_in.shape[0]):
        for j in range(3):
            at = (j * w_qkv_in.shape[0] + n) * head_dim
            w_qkv[at:at + head_dim] = w_qkv_in[n, j]
    for ref in (dw_qkv, dw_out, dw_up, dw_down, dg_attn, dg_mlp, probs, d_scores):
        ref[...] = jnp.zeros_like(ref)

    def step(t):
        @pl.when(t + 1 < count)
        def _():
            x_in(t + 1).start()
        s_mid = t - plan.lead['B']

        @pl.when(jnp.logical_and(s_mid >= 0, s_mid < count))
        def _():
            d_in(s_mid).start()
        for i, tag in enumerate(ORDER):
            s = t - plan.lead[tag[0]]

            @pl.when(jnp.logical_and(s >= 0, s < count))
            def _(fn=work[tag[0]][int(tag[1:])], s=s):
                fn(s)
            progress(t, i)

    loop(count + plan.steps, step)
    dg_parts[me, 0:1] = jnp.sum(dg_attn[...], axis=0, keepdims=True)
    dg_parts[me, 1:2] = jnp.sum(dg_mlp[...], axis=0, keepdims=True)

    def dg_copy(step, owner):
        return pltpu.make_async_remote_copy(
            src_ref=dg_parts.at[owner], dst_ref=dg_parts.at[owner], send_sem=dg_send.at[step], recv_sem=dg_recv.at[step],
            device_id={'model': lax.rem(me + step, size)}, device_id_type=MESH)

    for step_ahead in range(1, size):
        dg_copy(step_ahead, me).start()
    for acc, out in ((dw_out, dw_out_out), (dw_up, dw_up_out), (dw_down, dw_down_out)):
        out[...] = acc[...].astype(BF16)
    for n in range(w_qkv_in.shape[0]):
        for j in range(3):
            at = (j * w_qkv_in.shape[0] + n) * head_dim
            dw_qkv_out[n, j] = dw_qkv[at:at + head_dim].astype(BF16)
    for step_ahead in range(1, size):
        dg_copy(step_ahead, lax.rem(me + size - step_ahead, size)).wait_recv()
    dg_out[...] = sum(dg_parts[owner] for owner in range(size))
    for step_ahead in range(1, size):
        dg_copy(step_ahead, me).wait_send()
    for s in range(count - SLOTS, count):
        out_copy(s).wait()
        dtok_copy(s).wait()


def my_rows(me, width):
    return pl.ds(pl.multiple_of(me * width, width), width)


def publish_kernel(count, *refs):
    n = len(refs) // 5
    ins, outs, held, in_sems, out_sems = (refs[k * n:(k + 1) * n] for k in range(5))

    def moves(i):
        if i >= count:
            yield (pltpu.make_async_copy(ins[i], held[i], in_sems[i].at[0]),
                   pltpu.make_async_copy(held[i], outs[i], out_sems[i].at[0]))
            return
        for r in range(ins[i].shape[0]):
            yield (pltpu.make_async_copy(ins[i].at[r], held[i].at[r], in_sems[i].at[r]),
                   pltpu.make_async_copy(held[i].at[r], outs[i].at[r], out_sems[i].at[r]))
    pairs = [pair for i in range(n) for pair in moves(i)]
    for into, _ in pairs:
        into.start()
    for into, out in pairs:
        into.wait()
        out.start()
    for _, out in pairs:
        out.wait()


def publish(values, split):
    sems = [pltpu.SemaphoreType.DMA((v.shape[0] if i < split else 1,)) for i, v in enumerate(values)]
    return pl.pallas_call(
        functools.partial(publish_kernel, split),
        out_shape=[jax.ShapeDtypeStruct(v.shape, v.dtype) for v in values],
        in_specs=[pl.BlockSpec(memory_space=pl.ANY)] * len(values),
        out_specs=[pl.BlockSpec(memory_space=pl.ANY)] * len(values),
        scratch_shapes=[pltpu.VMEM(v.shape, v.dtype) for v in values] + sems + sems,
        compiler_params=pltpu.CompilerParams(vmem_limit_bytes=VMEM_LIMIT),
        name='publish',
    )(*values)


def ring_buffers(block_rows, hidden):
    return [
        pltpu.VMEM((SLOTS, BLOCKS, block_rows, hidden), BF16),
        pltpu.VMEM((SLOTS, HALF, block_rows, hidden), BF16),
        pltpu.VMEM((SLOTS, 2, block_rows, hidden), BF16),
        pltpu.VMEM((SLOTS, 2, PIECE, block_rows, hidden), BF16),
        pltpu.VMEM((SLOTS, BLOCKS, block_rows, hidden), BF16),
    ]


def ring_sems():
    return [pltpu.SemaphoreType.DMA((SLOTS, COPIES)), pltpu.SemaphoreType.DMA((SLOTS, COPIES))]


def run_kernel(kernel, ident, outs, out_vmem, args, in_vmem, scratch):
    def spec(in_vmem):
        return pl.BlockSpec(memory_space=pltpu.VMEM if in_vmem else pl.ANY)
    return pl.pallas_call(
        kernel,
        out_shape=[jax.ShapeDtypeStruct(s, t) for s, t in outs],
        in_specs=[spec(v) for v in in_vmem],
        out_specs=[spec(v) for v in out_vmem],
        scratch_shapes=scratch,
        compiler_params=pltpu.CompilerParams(collective_id=ident, has_side_effects=True, vmem_limit_bytes=VMEM_LIMIT),
        name=f'layer_part_{ident}',
    )(*args)


def solution(mesh):
    size = mesh.shape['model']
    dma = pltpu.SemaphoreType.DMA

    def device_step(tokens, seg_ids, d_out, gain_attn, gain_mlp, w_qkv, w_out, w_up, w_down):
        count, seq_len, hidden = tokens.shape
        heads, head_dim = w_qkv.shape[1], w_qkv.shape[3]
        width = heads * head_dim
        inner = w_up.shape[1]
        block_rows = seq_len // BLOCKS
        act = (count, BLOCKS, block_rows, hidden)
        one = (BLOCKS, block_rows, hidden)
        x = tokens.reshape(act)
        d = d_out.reshape(act)
        gains = jnp.stack([gain_attn, gain_mlp]).astype(F32)
        wqkv = w_qkv.transpose(1, 2, 3, 0)
        wout = w_out.reshape(width, hidden)
        plan = Plan()

        outs = [(act, BF16), (act, BF16), (wqkv.shape, BF16), ((width, hidden), BF16),
                ((hidden, inner), BF16), ((inner, hidden), BF16), ((2, hidden), F32)]
        scratch = [pltpu.VMEM(shape, kind) for shape, kind in (
            ((plan.x_slots,) + one, BF16), ((plan.d_slots,) + one, BF16), ((plan.x1_slots,) + one, BF16),
            ((plan.a_slots,) + one, BF16), ((plan.a_slots, seq_len, 4 * width), BF16),
            ((plan.head_slots, seq_len, size * width), BF16), ((3 * width, hidden), BF16), ((size * width, hidden), BF16),
            (one, BF16), ((seq_len, inner), F32), ((seq_len, inner), BF16),
            ((seq_len, inner), BF16), ((seq_len, inner), BF16), ((seq_len, width), BF16),
            ((seq_len, seq_len), BF16), ((seq_len, seq_len), BF16), ((seq_len, 3 * width), BF16),
            ((3 * width, hidden), F32), ((width, hidden), F32), ((hidden, inner), F32), ((inner, hidden), F32),
            ((8, hidden), F32), ((8, hidden), F32), ((count, 1, seq_len), jnp.int32),
            ((plan.own_slots, PIECE, block_rows, hidden), BF16), ((size, 2, hidden), F32))]
        scratch += [dma((plan.x_slots,)), dma((plan.d_slots,)), dma((SLOTS,)), dma((SLOTS,))]
        scratch += [dma((plan.head_slots, 8))] * 2 + [dma((1, 8))] * 2 + [dma((size,))] * 2
        for _ in range(3):
            scratch += ring_buffers(block_rows, hidden) + ring_sems()
        results = run_kernel(
            functools.partial(layer_kernel, size, head_dim, plan), 1, outs, [False] * 2 + [True] * 5,
            [x, d, seg_ids, gains, wqkv, wout, w_up, w_down], [False] * 2 + [True] * 6, scratch)
        layer_out, d_tokens, dw_qkv, dw_out, d_w_up, d_w_down, dg = publish(results, 2)

        return (layer_out.reshape(tokens.shape), d_tokens.reshape(tokens.shape), dw_qkv.transpose(3, 0, 1, 2),
                dw_out.reshape(w_out.shape), d_w_up, d_w_down, dg[0], dg[1])

    in_specs = (P('data', None, None), P('data', None), P('data', None, None), P(), P(), P(None, 'model', None, None), P('model', None, None), P(None, 'model'), P('model', None))
    out_specs = (P('data', None, None), P('data', None, None), P('data', 'model', None, None), P(('data', 'model'), None, None), P('data', 'model'), P(('data', 'model'), None), P('data'), P('data'))
    return jax.shard_map(device_step, mesh=mesh, in_specs=in_specs, out_specs=out_specs, check_vma=False)
```
